8 devices in a mesh: dp: 1 (over z), tp: 8 (over x, y, core).
Axes of the slice: x: 2, y: 2, z: 1, core: 2. Of those that a mesh axis runs over, the one named last changes fastest.
Arguments:
- x: bfloat16 [2048, 8192], P('dp')
- gain: bfloat16 [8192], replicated
- wq: bfloat16 [8192, 8192], P(None, 'tp')
- wk: bfloat16 [8192, 1024], P(None, 'tp')
- wv: bfloat16 [8192, 1024], P(None, 'tp')
- wo: bfloat16 [8192, 8192], P('tp')
Outputs:
- output: bfloat16 [2048, 8192], P('dp')
All inputs are finite; a program needn't handle non-finite values.
Results may differ from the reference program's by a relative error of at most 0.012.
Values are sent between devices in bfloat16 or wider.
A program may use at most 2 GiB of HBM per device.

```python
import jax
import jax.numpy as jnp
from jax import lax

ROWS = 2048
D = 8192
HEADS = 64
KV_HEADS = 8
HEAD = 128
THETA = 10000


def setup_inputs(seed: int = 0, part: int = 0) -> dict:
    kx, kn, kq, kk, kv, ko = jax.random.split(jax.random.key(seed), 6)

    def weights(key, rows, columns):
        return jax.random.normal(key, (rows, columns), jnp.float32) * rows**-0.5

    drawn = {
        "x": jax.random.normal(jax.random.fold_in(kx, part), (ROWS, D), jnp.float32),
        "gain": 1 + 0.1 * jax.random.normal(kn, (D,), jnp.float32),
        "wq": 2 * weights(kq, D, HEADS * HEAD),
        "wk": 2 * weights(kk, D, KV_HEADS * HEAD),
        "wv": 4 * weights(kv, D, KV_HEADS * HEAD),
        "wo": weights(ko, HEADS * HEAD, D),
    }
    return {k: v.astype(jnp.bfloat16) for k, v in drawn.items()}


def normed(x, gain):
    wide = x.astype(jnp.float32)
    scale = lax.rsqrt(jnp.mean(wide * wide, -1, keepdims=True) + 1e-6)
    return (wide * scale * gain.astype(jnp.float32)).astype(jnp.bfloat16)


def turned(t, place, theta):
    half = t.shape[-1] // 2
    angle = place.astype(jnp.float32)[:, None] * theta ** (-jnp.arange(half, dtype=jnp.float32) / half)
    cos, sin = jnp.cos(angle)[:, None], jnp.sin(angle)[:, None]
    a, b = t[..., :half].astype(jnp.float32), t[..., half:].astype(jnp.float32)
    return jnp.concatenate([a * cos - b * sin, b * cos + a * sin], -1).astype(jnp.bfloat16)


def matmul(a, w):
    return jnp.dot(a, w, preferred_element_type=jnp.float32).astype(jnp.bfloat16)


def einsum(form, a, b):
    return jnp.einsum(form, a.astype(jnp.float32), b.astype(jnp.float32))


def attention(q, k, v):
    scores = einsum("tgsd,ugd->gstu", q, k) * q.shape[-1] ** -0.5
    token = jnp.arange(q.shape[0])
    scores = jnp.where(token[:, None] >= token, scores, -jnp.inf)
    weights = jax.nn.softmax(scores, -1).astype(jnp.bfloat16)
    return einsum("gstu,ugd->tgsd", weights, v).astype(jnp.bfloat16)


def reference(x, gain, wq, wk, wv, wo):
    a, place = normed(x, gain), jnp.arange(ROWS)
    q = turned(matmul(a, wq).reshape(ROWS, HEADS, HEAD), place, THETA).reshape(ROWS, KV_HEADS, -1, HEAD)
    k = turned(matmul(a, wk).reshape(ROWS, KV_HEADS, HEAD), place, THETA)
    v = matmul(a, wv).reshape(ROWS, KV_HEADS, HEAD)
    seen = attention(q, k, v).reshape(ROWS, HEADS * HEAD)
    return (x.astype(jnp.float32) + jnp.dot(seen, wo, preferred_element_type=jnp.float32)).astype(jnp.bfloat16)
```

```python
import functools

import jax
import jax.numpy as jnp
import numpy as np
from jax import lax
from jax.experimental import pallas as pl
from jax.experimental.pallas import tpu as pltpu
from jax.sharding import PartitionSpec as P

MESH = pl.DeviceIdType.MESH
NEG = -1e30
HIDDEN = 2 * NEG
LOG2E = 1.4426950408889634
HEAD = 128
THETA = 10000
ROWS, D = 2048, 8192
R = 256
W = 512
CHUNKS = ROWS // R
PER = 1024 // W
U = CHUNKS * PER
HEADS = 8
COLS = HEADS * R
STRIP = 512
VROWS = 144
F32, BF16 = jnp.float32, jnp.bfloat16


def _dot(a, b, ca, cb):
    return lax.dot_general(a, b, (((ca,), (cb,)), ((), ())), preferred_element_type=F32)


def _kernel(x_ref, gain_ref, wq_ref, wk_ref, wv_ref, wo_ref, rope_ref, y_ref,
            wq_s, wkv_s, wo_s, xb, rope_s, k_s, vt_s, q_s, seen_s, mix_s, top_s,
            sbuf, own, rbuf, s1, r1, keep1, s2, r2, keep2, yb, xr,
            w_sem, wo_sem, x_sem, xr_sem, d_send, d_recv, p1_send, p1_recv, p2_send, p2_recv,
            a_send, b_send, c_send, a1_recv, a2_recv, b1_recv, sib_recv, cred_d, cred_1, cred_2):
    me = lax.axis_index("tp")
    a = lax.rem(me, 2)
    yc = lax.rem(me // 2, 2)
    xc = me // 4
    sib = me + 1 - 2 * a
    xn, yn = me + 4 - 8 * xc, me + 2 - 4 * yc
    fnb, gnb = xn * (1 - a) + yn * a, yn * (1 - a) + xn * a
    fb, gb = xc * (1 - a) + yc * a, yc * (1 - a) + xc * a
    base = a * 4
    o_own, o_g = base + fb * 2 + gb, base + fb * 2 + 1 - gb
    o_f, o_fg = base + (1 - fb) * 2 + gb, base + (1 - fb) * 2 + 1 - gb

    def x_copy(c):
        return pltpu.make_async_copy(x_ref.at[pl.ds(c * R, R), :], xb, x_sem)

    def wq_copy(n):
        at = pl.ds(pl.multiple_of(n * 256, 256), 256)
        return pltpu.make_async_copy(wq_ref.at[:, at], wq_s.at[:, at], w_sem.at[n])

    wk_copy = pltpu.make_async_copy(wk_ref, wkv_s.at[:, pl.ds(0, HEAD)], w_sem.at[4])
    wv_copy = pltpu.make_async_copy(wv_ref, wkv_s.at[:, pl.ds(HEAD, HEAD)], w_sem.at[5])
    rope_copy = pltpu.make_async_copy(rope_ref, rope_s, w_sem.at[6])

    def columns(owner, s):
        return pl.ds(pl.multiple_of(owner * 1024 + s * W, W), W)

    def wo_copy(owner, s):
        at = columns(owner, s)
        return pltpu.make_async_copy(wo_ref.at[:, at], wo_s.at[:, at], wo_sem.at[owner * PER + s])

    x_copy(0).start()
    wk_copy.start()
    wv_copy.start()
    rope_copy.start()
    for n in range(4):
        wq_copy(n).start()

    barrier = pltpu.get_barrier_semaphore()
    for other in (sib, fnb, gnb):
        pl.semaphore_signal(barrier, inc=1, device_id={"tp": other}, device_id_type=MESH)
    pl.semaphore_wait(barrier, 3)

    for s in range(PER):
        for j in range(4):
            wo_copy((1 - a) * 4 + j, s).start()
        for j in range(4):
            wo_copy(a * 4 + j, s).start()
    vt_s[HEAD:, :] = jnp.ones((VROWS - HEAD, ROWS), BF16)

    def remote(src, dst, send, recv, to):
        return pltpu.make_async_remote_copy(src_ref=src, dst_ref=dst, send_sem=send, recv_sem=recv, device_id={"tp": to}, device_id_type=MESH)

    def block(ref, u, owner):
        return ref.at[pl.ds(pl.multiple_of((u // PER) * R, R), R), columns(owner, lax.rem(u, PER))]

    def d_copy(u):
        return remote(sbuf, rbuf, d_send, d_recv, sib)

    def p1_copy(u):
        i = lax.rem(u, 2)
        return remote(s1.at[i], r1.at[i], p1_send.at[i], p1_recv.at[i], fnb)

    def p2_copy(u):
        i = lax.rem(u, 2)
        return remote(s2.at[i], r2.at[i], p2_send.at[i], p2_recv.at[i], gnb)

    def xr_copy(u):
        i = lax.rem(u, 2)
        return pltpu.make_async_copy(block(x_ref, u, o_own), xr.at[i], xr_sem.at[i])

    def a_copies(u):
        i = lax.rem(u, 2)
        at = block(y_ref, u, o_own)
        return (remote(yb.at[i], at, a_send.at[0, i], a1_recv.at[u], gnb),
                remote(yb.at[i], at, a_send.at[1, i], a2_recv.at[u], fnb),
                remote(yb.at[i], at, a_send.at[2, i], sib_recv.at[0, u], sib),
                pltpu.make_async_copy(yb.at[i], at, a_send.at[3, i]))

    def b_copies(u):
        i = lax.rem(u, 2)
        at = block(y_ref, u, o_g)
        return (remote(at, at, b_send.at[0, i], b1_recv.at[u], fnb),
                remote(at, at, b_send.at[1, i], sib_recv.at[1, u], sib))

    def c_copies(u):
        i = lax.rem(u, 2)
        at, far = block(y_ref, u, o_f), block(y_ref, u, o_fg)
        return (remote(at, at, c_send.at[0, i], sib_recv.at[2, u], sib),
                remote(far, far, c_send.at[1, i], sib_recv.at[3, u], sib))

    def sent(copies):
        for copy in copies:
            if copy.is_remote:
                copy.wait_send()
            else:
                copy.wait()

    def reduce_pair(u):
        i = lax.rem(u, 2)
        d_copy(u).wait_recv()

        @pl.when(u >= 2)
        def _():
            p1_copy(u - 2).wait_send()

        for j in range(2):
            n = (1 - fb) * 2 + j
            s1[i, j] = (own[n] + rbuf[n].astype(F32)).astype(BF16)

        @pl.when(u >= 2)
        def _():
            pl.semaphore_wait(cred_1, 1)

        p1_copy(u).start()
        for j in range(2):
            n = fb * 2 + j
            keep1[j] = own[n] + rbuf[n].astype(F32)

        @pl.when(u + 1 < U)
        def _():
            pl.semaphore_signal(cred_d, inc=1, device_id={"tp": sib}, device_id_type=MESH)

    def reduce_f(u):
        i = lax.rem(u, 2)
        xr_copy(u).start()
        p1_copy(u).wait_recv()

        @pl.when(u >= 2)
        def _():
            p2_copy(u - 2).wait_send()

        s2[i] = (keep1[1 - gb] + r1[i, 1 - gb].astype(F32)).astype(BF16)

        @pl.when(u >= 2)
        def _():
            pl.semaphore_wait(cred_2, 1)

        p2_copy(u).start()
        keep2[...] = keep1[gb] + r1[i, gb].astype(F32)

        @pl.when(u + 2 < U)
        def _():
            pl.semaphore_signal(cred_1, inc=1, device_id={"tp": fnb}, device_id_type=MESH)

    def reduce_g(u):
        i = lax.rem(u, 2)
        xr_copy(u).wait()

        @pl.when(u >= 2)
        def _():
            sent(a_copies(u - 2))

        p2_copy(u).wait_recv()
        yb[i] = (xr[i].astype(F32) + (keep2[...] + r2[i].astype(F32))).astype(BF16)
        for copy in a_copies(u):
            copy.start()

        @pl.when(u + 2 < U)
        def _():
            pl.semaphore_signal(cred_2, inc=1, device_id={"tp": gnb}, device_id_type=MESH)

    def gather_f(u):
        @pl.when(u >= 2)
        def _():
            sent(b_copies(u - 2))

        a_copies(u)[0].wait_recv()
        for copy in b_copies(u):
            copy.start()

    def gather_pair(u):
        @pl.when(u >= 2)
        def _():
            sent(c_copies(u - 2))

        a_copies(u)[1].wait_recv()
        b_copies(u)[0].wait_recv()
        for copy in c_copies(u):
            copy.start()

    def turned(t, cosf, sinf):
        t = t.astype(BF16).astype(F32)
        return (t * cosf + pltpu.roll(t, HEAD // 2, 1) * sinf).astype(BF16)

    def project(c):
        here = pl.ds(pl.multiple_of(c * R, R), R)
        x_copy(c).wait()
        piece = 1024

        def norm_rows(r, _):
            rows = pl.ds(pl.multiple_of(r * 16, 16), 16)
            total = jnp.zeros((16, piece), F32)
            for n in range(D // piece):
                wide = xb[rows, n * piece : (n + 1) * piece].astype(F32)
                total = total + wide * wide
            scale = lax.rsqrt(jnp.sum(total, -1, keepdims=True) * (1 / D) + 1e-6)
            for n in range(D // piece):
                at = slice(n * piece, (n + 1) * piece)
                xb[rows, at] = (xb[rows, at].astype(F32) * scale * gain_ref[:, at].astype(F32)).astype(BF16)
            return 0

        lax.fori_loop(0, R // 16, norm_rows, 0)

        @pl.when(c == 0)
        def _():
            rope_copy.wait()
            wk_copy.wait()
            wv_copy.wait()

        cs = rope_s[here, :]
        sc = pltpu.roll(cs, HEAD // 2, 1)
        low = lax.broadcasted_iota(jnp.int32, (R, HEAD), 1) < HEAD // 2
        cosf, sinf = jnp.where(low, cs, sc), jnp.where(low, -sc, cs)
        kv = _dot(xb[...], wkv_s[...], 1, 0)
        k_s[here, :] = turned(kv[:, :HEAD], cosf, sinf)
        vt_s[:HEAD, here] = kv[:, HEAD:].T.astype(BF16)

        def queries(n, _):
            @pl.when(c == 0)
            def _():
                wq_copy(n).wait()

            q = _dot(xb[...], wq_s[:, pl.ds(pl.multiple_of(n * 256, 256), 256)], 1, 0)
            for h in range(2):
                q_s[pl.ds(pl.multiple_of((2 * n + h) * R, R), R), :] = turned(q[:, h * HEAD : (h + 1) * HEAD], cosf, sinf)
            return 0

        lax.fori_loop(0, 4, queries, 0)

        @pl.when(c + 1 < CHUNKS)
        def _():
            x_copy(c + 1).start()

    def attention(c):
        e = HEAD**-0.5 * LOG2E
        pieces = range(0, COLS, STRIP)
        top_s[...] = jnp.full((8, COLS), NEG, F32)
        mix_s[...] = jnp.zeros((VROWS, COLS), F32)

        def keys(j, masked):
            here = pl.ds(pl.multiple_of(j * R, R), R)
            scores = [_dot(k_s[here, :], q_s[at : at + STRIP, :], 1, 1) for at in pieces]
            if masked:
                ok = lax.rem(lax.broadcasted_iota(jnp.int32, (R, STRIP), 1), R) >= lax.broadcasted_iota(jnp.int32, (R, STRIP), 0)
            weights, keeps = [], []
            for at, s in zip(pieces, scores):
                if masked:
                    s = jnp.where(ok, s, HIDDEN)
                old = top_s[0:1, at : at + STRIP]
                top = jnp.maximum(old, s.max(axis=0, keepdims=True))
                top_s[0:1, at : at + STRIP] = top
                weights.append(jnp.exp2((s - top) * e).astype(BF16))
                keeps.append(jnp.exp2((old - top) * e))
            for at, p, keep in zip(pieces, weights, keeps):
                mix_s[:, at : at + STRIP] = mix_s[:, at : at + STRIP] * keep + _dot(vt_s[:, here], p, 1, 0)

        def whole(j, _):
            keys(j, False)
            return 0

        lax.fori_loop(0, c, whole, 0)
        keys(c, True)
        for h in range(HEADS):
            at = slice(h * R, (h + 1) * R)
            seen_s[:, h * HEAD : (h + 1) * HEAD] = (mix_s[:HEAD, at] * (1 / mix_s[HEAD : HEAD + 1, at])).T.astype(BF16)

    def output(u):
        s = lax.rem(u, PER)

        def tile(owner):
            @pl.when(u < PER)
            def _():
                wo_copy(owner, s).wait()

            return _dot(seen_s[...], wo_s[:, columns(owner, s)], 1, 0)

        @pl.when(u >= 1)
        def _():
            d_copy(u - 1).wait_send()

        def theirs(j, _):
            sbuf[j] = tile((1 - a) * 4 + j).astype(BF16)
            return 0

        lax.fori_loop(0, 4, theirs, 0)

        @pl.when(u >= 1)
        def _():
            pl.semaphore_wait(cred_d, 1)

        d_copy(u).start()

        def ours(j, _):
            own[j] = tile(a * 4 + j)
            return 0

        lax.fori_loop(0, 4, ours, 0)

    def iteration(t, _):
        u = t - 1
        for stage, lag in ((gather_pair, 5), (gather_f, 4), (reduce_g, 3), (reduce_f, 2), (reduce_pair, 1)):
            @pl.when((u >= lag) & (u < U + lag))
            def _(stage=stage, lag=lag):
                stage(u - lag)

        @pl.when((u >= 0) & (u < U) & (lax.rem(t, PER) == 1))
        def _():
            attention(u // PER)

        @pl.when((u >= 0) & (u < U))
        def _():
            output(u)

        @pl.when((u < U - 1) & (lax.rem(t, PER) == 0))
        def _():
            project(t // PER)

        return 0

    lax.fori_loop(0, U + 6, iteration, 0)

    d_copy(U - 1).wait_send()
    for u in (U - 2, U - 1):
        p1_copy(u).wait_send()
        p2_copy(u).wait_send()
        sent(a_copies(u))
        sent(b_copies(u))
        sent(c_copies(u))

    def arrivals(u, _):
        a_copies(u)[2].wait_recv()
        b_copies(u)[1].wait_recv()
        for copy in c_copies(u):
            copy.wait_recv()
        return 0

    lax.fori_loop(0, U, arrivals, 0)


def _tables():
    half = HEAD // 2
    angle = np.arange(ROWS, dtype=np.float64)[:, None] * np.float64(THETA) ** (-np.arange(half, dtype=np.float64) / half)
    return np.concatenate([np.cos(angle), np.sin(angle)], 1).astype(np.float32)


def solution(mesh):
    def step(x, gain, wq, wk, wv, wo):
        any_ = pl.BlockSpec(memory_space=pl.ANY)
        dma = pltpu.SemaphoreType.DMA
        return pl.pallas_call(
            _kernel,
            name="layer",
            out_shape=jax.ShapeDtypeStruct((ROWS, D), BF16),
            in_specs=[any_, pl.BlockSpec(memory_space=pltpu.VMEM)] + [any_] * 5,
            out_specs=any_,
            scratch_shapes=[
                pltpu.VMEM((D, 1024), BF16), pltpu.VMEM((D, 2 * HEAD), BF16), pltpu.VMEM((1024, D), BF16),
                pltpu.VMEM((R, D), BF16), pltpu.VMEM((ROWS, HEAD), F32),
                pltpu.VMEM((ROWS, HEAD), BF16), pltpu.VMEM((VROWS, ROWS), BF16), pltpu.VMEM((COLS, HEAD), BF16),
                pltpu.VMEM((R, 1024), BF16), pltpu.VMEM((VROWS, COLS), F32), pltpu.VMEM((8, COLS), F32),
                pltpu.VMEM((4, R, W), BF16), pltpu.VMEM((4, R, W), F32), pltpu.VMEM((4, R, W), BF16),
                pltpu.VMEM((2, 2, R, W), BF16), pltpu.VMEM((2, 2, R, W), BF16), pltpu.VMEM((2, R, W), F32),
                pltpu.VMEM((2, R, W), BF16), pltpu.VMEM((2, R, W), BF16), pltpu.VMEM((R, W), F32),
                pltpu.VMEM((2, R, W), BF16), pltpu.VMEM((2, R, W), BF16),
                dma((7,)), dma((8 * PER,)), dma, dma((2,)), dma, dma, dma((2,)), dma((2,)), dma((2,)), dma((2,)),
                dma((4, 2)), dma((2, 2)), dma((2, 2)), dma((U,)), dma((U,)), dma((U,)), dma((4, U)),
                pltpu.SemaphoreType.REGULAR, pltpu.SemaphoreType.REGULAR, pltpu.SemaphoreType.REGULAR,
            ],
            compiler_params=pltpu.CompilerParams(collective_id=0, has_side_effects=True, vmem_limit_bytes=67043328),
            cost_estimate=pl.CostEstimate(flops=95_000_000_000, bytes_accessed=200_000_000, transcendentals=20_000_000),
        )(x, gain.reshape(1, D), wq, wk, wv, wo, jnp.asarray(_tables()))

    tokens, columns = P("dp", None), P(None, "tp")
    return jax.shard_map(
        step,
        mesh=mesh,
        in_specs=(tokens, P(None), columns, columns, columns, P("tp", None)),
        out_specs=tokens,
        check_vma=False,
    )
```

```python
import functools

import jax
import jax.numpy as jnp
import numpy as np
from jax import lax
from jax.experimental import pallas as pl
from jax.experimental.pallas import tpu as pltpu
from jax.sharding import PartitionSpec as P

MESH = pl.DeviceIdType.MESH
NEG = -1e30
HIDDEN = 2 * NEG
LOG2E = 1.4426950408889634
HEAD = 128
THETA = 10000
ROWS, D = 2048, 8192
R = 256
W = 512
CHUNKS = ROWS // R
PER = 1024 // W
U = CHUNKS * PER
HEADS = 8
COLS = HEADS * R
STRIP = 512
VROWS = 144
F32, BF16 = jnp.float32, jnp.bfloat16
SLOTS = 5


def STAGES(stages):
    return [(stage, i, i + 1) for i, stage in enumerate(stages)]


def _dot(a, b, ca, cb):
    return lax.dot_general(a, b, (((ca,), (cb,)), ((), ())), preferred_element_type=F32)


def _kernel(x_ref, gain_ref, wq_ref, wk_ref, wv_ref, wo_ref, rope_ref, y_ref,
            gain_s, wq_s, wkv_s, wo_s, xb, rope_s, k_s, vt_s, q_s, seen_s, mix_s, top_s,
            sbuf, own, rbuf, s1, r1, keep1, s2, r2, keep2, yb, xr,
            w_sem, wo_sem, x_sem, xr_sem, d_send, d_recv, p1_send, p1_recv, p2_send, p2_recv,
            a_send, b_send, c_send, a1_recv, a2_recv, b1_recv, sib_recv, cred_d, cred_1, cred_2):
    me = lax.axis_index("tp")
    a = lax.rem(me, 2)
    yc = lax.rem(me // 2, 2)
    xc = me // 4
    sib = me + 1 - 2 * a
    xn, yn = me + 4 - 8 * xc, me + 2 - 4 * yc
    fnb, gnb = xn * (1 - a) + yn * a, yn * (1 - a) + xn * a
    fb, gb = xc * (1 - a) + yc * a, yc * (1 - a) + xc * a
    base = a * 4
    o_own, o_g = base + fb * 2 + gb, base + fb * 2 + 1 - gb
    o_f, o_fg = base + (1 - fb) * 2 + gb, base + (1 - fb) * 2 + 1 - gb

    def x_copies(c):
        n = R // 4
        return [pltpu.make_async_copy(x_ref.at[pl.ds(pl.multiple_of(c * R + i * n, n), n), :], xb.at[pl.ds(i * n, n), :], x_sem.at[i]) for i in range(4)]

    def wq_copy(n):
        at = pl.ds(pl.multiple_of(n * 256, 256), 256)
        return pltpu.make_async_copy(wq_ref.at[:, at], wq_s.at[:, at], w_sem.at[n])

    wk_copy = pltpu.make_async_copy(wk_ref, wkv_s.at[:, pl.ds(0, HEAD)], w_sem.at[4])
    wv_copy = pltpu.make_async_copy(wv_ref, wkv_s.at[:, pl.ds(HEAD, HEAD)], w_sem.at[5])
    rope_copy = pltpu.make_async_copy(rope_ref, rope_s, w_sem.at[6])

    def columns(owner, s):
        return pl.ds(pl.multiple_of(owner * 1024 + s * W, W), W)

    def wo_copy(owner, s):
        at = columns(owner, s)
        return pltpu.make_async_copy(wo_ref.at[:, at], wo_s.at[:, at], wo_sem.at[owner * PER + s])

    for copy in x_copies(0):
        copy.start()
    barrier = pltpu.get_barrier_semaphore()
    for other in (sib, fnb, gnb):
        pl.semaphore_signal(barrier, inc=1, device_id={"tp": other}, device_id_type=MESH)
    rope_copy.start()
    wk_copy.start()
    wv_copy.start()
    for n in range(4):
        wq_copy(n).start()
    gain = gain_ref[...].astype(F32)
    for n in range(D // 128):
        gain_s[:, n * 128 : (n + 1) * 128] = gain[n : n + 1, :]
    vt_s[HEAD:, :] = jnp.ones((VROWS - HEAD, ROWS), BF16)
    pl.semaphore_wait(barrier, 3)

    def remote(src, dst, send, recv, to):
        return pltpu.make_async_remote_copy(src_ref=src, dst_ref=dst, send_sem=send, recv_sem=recv, device_id={"tp": to}, device_id_type=MESH)

    def block(ref, u, owner):
        return ref.at[pl.ds(pl.multiple_of((u // PER) * R, R), R), columns(owner, lax.rem(u, PER))]

    def d_copy(u):
        return remote(sbuf, rbuf, d_send, d_recv, sib)

    def p1_copy(u):
        i = lax.rem(u, 2)
        return remote(s1.at[i], r1.at[i], p1_send.at[i], p1_recv.at[i], fnb)

    def p2_copy(u):
        i = lax.rem(u, 2)
        return remote(s2.at[i], r2.at[i], p2_send.at[i], p2_recv.at[i], gnb)

    def xr_copy(u):
        i = lax.rem(u, 2)
        return pltpu.make_async_copy(block(x_ref, u, o_own), xr.at[i], xr_sem.at[i])

    def a_copies(u):
        i = lax.rem(u, 2)
        at = block(y_ref, u, o_own)
        return (remote(yb.at[i], at, a_send.at[0, i], a1_recv.at[u], gnb),
                remote(yb.at[i], at, a_send.at[1, i], a2_recv.at[u], fnb),
                remote(yb.at[i], at, a_send.at[2, i], sib_recv.at[0, u], sib),
                pltpu.make_async_copy(yb.at[i], at, a_send.at[3, i]))

    def b_copies(u):
        i = lax.rem(u, 2)
        at = block(y_ref, u, o_g)
        return (remote(at, at, b_send.at[0, i], b1_recv.at[u], fnb),
                remote(at, at, b_send.at[1, i], sib_recv.at[1, u], sib))

    def c_copies(u):
        i = lax.rem(u, 2)
        at, far = block(y_ref, u, o_f), block(y_ref, u, o_fg)
        return (remote(at, at, c_send.at[0, i], sib_recv.at[2, u], sib),
                remote(far, far, c_send.at[1, i], sib_recv.at[3, u], sib))

    def sent(copies):
        for copy in copies:
            if copy.is_remote:
                copy.wait_send()
            else:
                copy.wait()

    def reduce_pair(u):
        i = lax.rem(u, 2)
        d_copy(u).wait_recv()

        @pl.when(u >= 2)
        def _():
            p1_copy(u - 2).wait_send()

        for j in range(2):
            n = (1 - fb) * 2 + j
            s1[i, j] = (own[n] + rbuf[n].astype(F32)).astype(BF16)

        @pl.when(u >= 2)
        def _():
            pl.semaphore_wait(cred_1, 1)

        p1_copy(u).start()
        for j in range(2):
            n = fb * 2 + j
            keep1[i, j] = own[n] + rbuf[n].astype(F32)

        @pl.when(u + 1 < U)
        def _():
            pl.semaphore_signal(cred_d, inc=1, device_id={"tp": sib}, device_id_type=MESH)

    def reduce_f(u):
        i = lax.rem(u, 2)
        xr_copy(u).start()
        p1_copy(u).wait_recv()

        @pl.when(u >= 2)
        def _():
            p2_copy(u - 2).wait_send()

        s2[i] = (keep1[i, 1 - gb] + r1[i, 1 - gb].astype(F32)).astype(BF16)

        @pl.when(u >= 2)
        def _():
            pl.semaphore_wait(cred_2, 1)

        p2_copy(u).start()
        keep2[i] = keep1[i, gb] + r1[i, gb].astype(F32)

        @pl.when(u + 2 < U)
        def _():
            pl.semaphore_signal(cred_1, inc=1, device_id={"tp": fnb}, device_id_type=MESH)

    def reduce_g(u):
        i = lax.rem(u, 2)
        xr_copy(u).wait()

        @pl.when(u >= 2)
        def _():
            sent(a_copies(u - 2))

        p2_copy(u).wait_recv()
        yb[i] = (xr[i].astype(F32) + (keep2[i] + r2[i].astype(F32))).astype(BF16)
        for copy in a_copies(u):
            copy.start()

        @pl.when(u + 2 < U)
        def _():
            pl.semaphore_signal(cred_2, inc=1, device_id={"tp": gnb}, device_id_type=MESH)

    def gather_f(u):
        @pl.when(u >= 2)
        def _():
            sent(b_copies(u - 2))

        a_copies(u)[0].wait_recv()
        for copy in b_copies(u):
            copy.start()

    def gather_pair(u):
        @pl.when(u >= 2)
        def _():
            sent(c_copies(u - 2))

        a_copies(u)[1].wait_recv()
        b_copies(u)[0].wait_recv()
        for copy in c_copies(u):
            copy.start()

    def turned(t, cosf, sinf):
        t = t.astype(BF16).astype(F32)
        return (t * cosf + pltpu.roll(t, HEAD // 2, 1) * sinf).astype(BF16)

    def normalize(c):
        for copy in x_copies(c):
            copy.wait()
        piece = 1024

        def norm_rows(r, _):
            rows = pl.ds(pl.multiple_of(r * 16, 16), 16)
            total = jnp.zeros((16, piece), F32)
            for n in range(D // piece):
                wide = xb[rows, n * piece : (n + 1) * piece].astype(F32)
                total = total + wide * wide
            scale = lax.rsqrt(jnp.sum(total, -1, keepdims=True) * (1 / D) + 1e-6)
            for n in range(D // piece):
                at = slice(n * piece, (n + 1) * piece)
                xb[rows, at] = (xb[rows, at].astype(F32) * scale * gain_s[:, at]).astype(BF16)
            return 0

        lax.fori_loop(0, R // 16, norm_rows, 0)

    def turns(c):
        cs = rope_s[pl.ds(pl.multiple_of(c * R, R), R), :]
        sc = pltpu.roll(cs, HEAD // 2, 1)
        low = lax.broadcasted_iota(jnp.int32, (R, HEAD), 1) < HEAD // 2
        return jnp.where(low, cs, sc), jnp.where(low, -sc, cs)

    def keys_values(c):
        @pl.when(c == 0)
        def _():
            rope_copy.wait()
            wk_copy.wait()
            wv_copy.wait()

        here = pl.ds(pl.multiple_of(c * R, R), R)
        kv = _dot(xb[...], wkv_s[...], 1, 0)
        k_s[here, :] = turned(kv[:, :HEAD], *turns(c))
        vt_s[:HEAD, here] = kv[:, HEAD:].T.astype(BF16)

    def queries(c, first, last):
        def tile(n, _):
            @pl.when(c == 0)
            def _():
                wq_copy(n).wait()

            @pl.when((c == 0) & (n == 1))
            def _():
                for s in range(PER):
                    for j in range(4):
                        wo_copy((1 - a) * 4 + j, s).start()
                    for j in range(4):
                        wo_copy(a * 4 + j, s).start()

            q = _dot(xb[...], wq_s[:, pl.ds(pl.multiple_of(n * 256, 256), 256)], 1, 0)
            cosf, sinf = turns(c)
            for h in range(2):
                q_s[pl.ds(pl.multiple_of((2 * n + h) * R, R), R), :] = turned(q[:, h * HEAD : (h + 1) * HEAD], cosf, sinf)
            return 0

        lax.fori_loop(first, last, tile, 0)

        @pl.when((last == 4) & (c + 1 < CHUNKS))
        def _():
            for copy in x_copies(c + 1):
                copy.start()

    def attention(c, part):
        e = HEAD**-0.5 * LOG2E
        pieces = range(0, COLS, STRIP)

        def keys(j, masked):
            here = pl.ds(pl.multiple_of(j * R, R), R)
            scores = [_dot(k_s[here, :], q_s[at : at + STRIP, :], 1, 1) for at in pieces]
            if masked:
                ok = lax.rem(lax.broadcasted_iota(jnp.int32, (R, STRIP), 1), R) >= lax.broadcasted_iota(jnp.int32, (R, STRIP), 0)
            weights, keeps = [], []
            for at, s in zip(pieces, scores):
                if masked:
                    s = jnp.where(ok, s, HIDDEN)
                old = top_s[0:1, at : at + STRIP]
                top = jnp.maximum(old, s.max(axis=0, keepdims=True))
                top_s[0:1, at : at + STRIP] = top
                weights.append(jnp.exp2((s - top) * e).astype(BF16))
                keeps.append(jnp.exp2((old - top) * e))
            for at, p, keep in zip(pieces, weights, keeps):
                mix_s[:, at : at + STRIP] = mix_s[:, at : at + STRIP] * keep + _dot(vt_s[:, here], p, 1, 0)

        def whole(j, _):
            keys(j, False)
            return 0

        @pl.when(part == 0)
        def _():
            top_s[...] = jnp.full((8, COLS), NEG, F32)
            mix_s[...] = jnp.zeros((VROWS, COLS), F32)

        lax.fori_loop(jnp.where(part == 0, 0, c // 2), jnp.where(part == 0, c // 2, c), whole, 0)

        @pl.when(part == 1)
        def _():
            keys(c, True)
            for h in range(HEADS):
                at = slice(h * R, (h + 1) * R)
                seen_s[:, h * HEAD : (h + 1) * HEAD] = (mix_s[:HEAD, at] * (1 / mix_s[HEAD : HEAD + 1, at])).T.astype(BF16)

    def tile(u, owner):
        s = lax.rem(u, PER)

        @pl.when(u < PER)
        def _():
            wo_copy(owner, s).wait()

        return _dot(seen_s[...], wo_s[:, columns(owner, s)], 1, 0)

    def output_theirs(u):
        @pl.when(u >= 1)
        def _():
            d_copy(u - 1).wait_send()

        def theirs(j, _):
            sbuf[j] = tile(u, (1 - a) * 4 + j).astype(BF16)
            return 0

        lax.fori_loop(0, 4, theirs, 0)

        @pl.when(u >= 1)
        def _():
            pl.semaphore_wait(cred_d, 1)

        d_copy(u).start()

    def output_ours(u):
        def ours(j, _):
            own[j] = tile(u, a * 4 + j)
            return 0

        lax.fori_loop(0, 4, ours, 0)

    def slot(g, _):
        u = g // SLOTS - 1
        k = lax.rem(g, SLOTS)
        c = (u + PER) // PER - 1
        odd = lax.rem(u + PER, PER) == 1
        for stage, at, lag in STAGES((reduce_pair, reduce_f, reduce_g, gather_f, gather_pair)):
            @pl.when((k == at) & (u >= lag) & (u < U + lag))
            def _(stage=stage, lag=lag):
                stage(u - lag)

        live = (u >= 0) & (u < U)

        @pl.when(live & ~odd & (k < 2))
        def _():
            attention(c, k)

        @pl.when(live & ((~odd & (k == 3)) | (odd & (k == 0))))
        def _():
            output_theirs(u)

        @pl.when(live & ((~odd & (k == 4)) | (odd & (k == 1))))
        def _():
            output_ours(u)

        more = odd & (u < U - 1)

        @pl.when(more & (k == 2))
        def _():
            normalize(c + 1)

        @pl.when(more & (k == 3))
        def _():
            keys_values(c + 1)

        @pl.when(more & (k >= 3))
        def _():
            queries(c + 1, 2 * k - 6, 2 * k - 4)

        return 0

    lax.fori_loop(2, (U + 6) * SLOTS, slot, 0)

    d_copy(U - 1).wait_send()
    for u in (U - 2, U - 1):
        p1_copy(u).wait_send()
        p2_copy(u).wait_send()
        sent(a_copies(u))
        sent(b_copies(u))
        sent(c_copies(u))

    def arrivals(u, _):
        a_copies(u)[2].wait_recv()
        b_copies(u)[1].wait_recv()
        for copy in c_copies(u):
            copy.wait_recv()
        return 0

    lax.fori_loop(0, U, arrivals, 0)


def _tables():
    half = HEAD // 2
    angle = np.arange(ROWS, dtype=np.float64)[:, None] * np.float64(THETA) ** (-np.arange(half, dtype=np.float64) / half)
    return np.concatenate([np.cos(angle), np.sin(angle)], 1).astype(np.float32)


def solution(mesh):
    def step(x, gain, wq, wk, wv, wo):
        any_ = pl.BlockSpec(memory_space=pl.ANY)
        dma = pltpu.SemaphoreType.DMA
        return pl.pallas_call(
            _kernel,
            name="layer",
            out_shape=jax.ShapeDtypeStruct((ROWS, D), BF16),
            in_specs=[any_, pl.BlockSpec(memory_space=pltpu.VMEM)] + [any_] * 5,
            out_specs=any_,
            scratch_shapes=[
                pltpu.VMEM((1, D), F32),
                pltpu.VMEM((D, 1024), BF16), pltpu.VMEM((D, 2 * HEAD), BF16), pltpu.VMEM((1024, D), BF16),
                pltpu.VMEM((R, D), BF16), pltpu.VMEM((ROWS, HEAD), F32),
                pltpu.VMEM((ROWS, HEAD), BF16), pltpu.VMEM((VROWS, ROWS), BF16), pltpu.VMEM((COLS, HEAD), BF16),
                pltpu.VMEM((R, 1024), BF16), pltpu.VMEM((VROWS, COLS), F32), pltpu.VMEM((8, COLS), F32),
                pltpu.VMEM((4, R, W), BF16), pltpu.VMEM((4, R, W), F32), pltpu.VMEM((4, R, W), BF16),
                pltpu.VMEM((2, 2, R, W), BF16), pltpu.VMEM((2, 2, R, W), BF16), pltpu.VMEM((2, 2, R, W), F32),
                pltpu.VMEM((2, R, W), BF16), pltpu.VMEM((2, R, W), BF16), pltpu.VMEM((2, R, W), F32),
                pltpu.VMEM((2, R, W), BF16), pltpu.VMEM((2, R, W), BF16),
                dma((7,)), dma((8 * PER,)), dma((4,)), dma((2,)), dma, dma, dma((2,)), dma((2,)), dma((2,)), dma((2,)),
                dma((4, 2)), dma((2, 2)), dma((2, 2)), dma((U,)), dma((U,)), dma((U,)), dma((4, U)),
                pltpu.SemaphoreType.REGULAR, pltpu.SemaphoreType.REGULAR, pltpu.SemaphoreType.REGULAR,
            ],
            compiler_params=pltpu.CompilerParams(collective_id=0, has_side_effects=True, vmem_limit_bytes=67043328),
            cost_estimate=pl.CostEstimate(flops=95_000_000_000, bytes_accessed=200_000_000, transcendentals=20_000_000),
        )(x, gain.reshape(D // 128, 128), wq, wk, wv, wo, jnp.asarray(_tables()))

    tokens, columns = P("dp", None), P(None, "tp")
    return jax.shard_map(
        step,
        mesh=mesh,
        in_specs=(tokens, P(None), columns, columns, columns, P("tp", None)),
        out_specs=tokens,
        check_vma=False,
    )
```

```python
import functools

import jax
import jax.numpy as jnp
import numpy as np
from jax import lax
from jax.experimental import pallas as pl
from jax.experimental.pallas import tpu as pltpu
from jax.sharding import PartitionSpec as P

MESH = pl.DeviceIdType.MESH
NEG = -1e30
HIDDEN = 2 * NEG
LOG2E = 1.4426950408889634
HEAD = 128
THETA = 10000
ROWS, D = 2048, 8192
R = 256
W = 512
CHUNKS = ROWS // R
PER = 1024 // W
U = CHUNKS * PER
HEADS = 8
COLS = HEADS * R
STRIP = 512
VROWS = 144
F32, BF16 = jnp.float32, jnp.bfloat16
SLOTS = 10
WHEN = {"reduce_pair": (4, 7), "reduce_f": (9, 10), "reduce_g": (11, 12), "gather_f": (19, 20), "gather_pair": (21, 25)}


def _dot(a, b, ca, cb):
    return lax.dot_general(a, b, (((ca,), (cb,)), ((), ())), preferred_element_type=F32)


def _kernel(x_ref, gain_ref, wq_ref, wk_ref, wv_ref, wo_ref, rope_ref, y_ref,
            gain_s, wq_s, wkv_s, wo_s, xb, rope_s, k_s, vt_s, q_s, seen_s, mix_s, top_s,
            sbuf, own, rbuf, s1, r1, keep1, s2, r2, keep2, yb, xr,
            w_sem, wo_sem, x_sem, xr_sem, d_send, d_recv, p1_send, p1_recv, p2_send, p2_recv,
            a_send, b_send, c_send, a1_recv, a2_recv, b1_recv, sib_recv, cred_d, cred_1, cred_2):
    me = lax.axis_index("tp")
    a = lax.rem(me, 2)
    yc = lax.rem(me // 2, 2)
    xc = me // 4
    sib = me + 1 - 2 * a
    xn, yn = me + 4 - 8 * xc, me + 2 - 4 * yc
    fnb, gnb = xn * (1 - a) + yn * a, yn * (1 - a) + xn * a
    fb, gb = xc * (1 - a) + yc * a, yc * (1 - a) + xc * a
    base = a * 4
    o_own, o_g = base + fb * 2 + gb, base + fb * 2 + 1 - gb
    o_f, o_fg = base + (1 - fb) * 2 + gb, base + (1 - fb) * 2 + 1 - gb

    def x_copies(c):
        n = R // 4
        return [pltpu.make_async_copy(x_ref.at[pl.ds(pl.multiple_of(c * R + i * n, n), n), :], xb.at[pl.ds(i * n, n), :], x_sem.at[i]) for i in range(4)]

    def wq_copy(n):
        at = pl.ds(pl.multiple_of(n * 256, 256), 256)
        return pltpu.make_async_copy(wq_ref.at[:, at], wq_s.at[:, at], w_sem.at[n])

    wk_copy = pltpu.make_async_copy(wk_ref, wkv_s.at[:, pl.ds(0, HEAD)], w_sem.at[4])
    wv_copy = pltpu.make_async_copy(wv_ref, wkv_s.at[:, pl.ds(HEAD, HEAD)], w_sem.at[5])
    rope_copy = pltpu.make_async_copy(rope_ref, rope_s, w_sem.at[6])

    def columns(owner, s):
        return pl.ds(pl.multiple_of(owner * 1024 + s * W, W), W)

    def wo_copy(owner, s):
        at = columns(owner, s)
        return pltpu.make_async_copy(wo_ref.at[:, at], wo_s.at[:, at], wo_sem.at[owner * PER + s])

    for copy in x_copies(0):
        copy.start()
    barrier = pltpu.get_barrier_semaphore()
    for other in (sib, fnb, gnb):
        pl.semaphore_signal(barrier, inc=1, device_id={"tp": other}, device_id_type=MESH)
    gain = gain_ref[...].astype(F32)
    for n in range(D // 128):
        gain_s[:, n * 128 : (n + 1) * 128] = gain[n : n + 1, :]
    vt_s[HEAD:, :] = jnp.ones((VROWS - HEAD, ROWS), BF16)
    pl.semaphore_wait(barrier, 3)
    for copy in (wk_copy, wv_copy, rope_copy, wq_copy(0), wq_copy(1)):
        copy.start()

    def remote(src, dst, send, recv, to):
        return pltpu.make_async_remote_copy(src_ref=src, dst_ref=dst, send_sem=send, recv_sem=recv, device_id={"tp": to}, device_id_type=MESH)

    def block(ref, u, owner):
        return ref.at[pl.ds(pl.multiple_of((u // PER) * R, R), R), columns(owner, lax.rem(u, PER))]

    def d_copy(j):
        return remote(sbuf.at[j], rbuf.at[j], d_send.at[j], d_recv.at[j], sib)

    def d_copies(u):
        return [d_copy(j) for j in range(4)]

    def p1_copy(u):
        i = lax.rem(u, 2)
        return remote(s1.at[i], r1.at[i], p1_send.at[i], p1_recv.at[i], fnb)

    def p2_copy(u):
        i = lax.rem(u, 2)
        return remote(s2.at[i], r2.at[i], p2_send.at[i], p2_recv.at[i], gnb)

    def xr_copy(u):
        i = lax.rem(u, 2)
        return pltpu.make_async_copy(block(x_ref, u, o_own), xr.at[i], xr_sem.at[i])

    def a_copies(u):
        i = lax.rem(u, 2)
        at = block(y_ref, u, o_own)
        return (remote(yb.at[i], at, a_send.at[0, i], a1_recv.at[u], gnb),
                remote(yb.at[i], at, a_send.at[1, i], a2_recv.at[u], fnb),
                remote(yb.at[i], at, a_send.at[2, i], sib_recv.at[0, u], sib),
                pltpu.make_async_copy(yb.at[i], at, a_send.at[3, i]))

    def b_copies(u):
        i = lax.rem(u, 2)
        at = block(y_ref, u, o_g)
        return (remote(at, at, b_send.at[0, i], b1_recv.at[u], fnb),
                remote(at, at, b_send.at[1, i], sib_recv.at[1, u], sib))

    def c_copies(u):
        i = lax.rem(u, 2)
        at, far = block(y_ref, u, o_f), block(y_ref, u, o_fg)
        return (remote(at, at, c_send.at[0, i], sib_recv.at[2, u], sib),
                remote(far, far, c_send.at[1, i], sib_recv.at[3, u], sib))

    def sent(copies):
        for copy in copies:
            if copy.is_remote:
                copy.wait_send()
            else:
                copy.wait()

    def reduce_pair(u):
        i = lax.rem(u, 2)
        for copy in d_copies(u):
            copy.wait_recv()

        @pl.when(u >= 2)
        def _():
            p1_copy(u - 2).wait_send()

        for j in range(2):
            n = (1 - fb) * 2 + j
            s1[i, j] = (own[n] + rbuf[n].astype(F32)).astype(BF16)

        @pl.when(u >= 2)
        def _():
            pl.semaphore_wait(cred_1, 1)

        p1_copy(u).start()
        for j in range(2):
            n = fb * 2 + j
            keep1[i, j] = own[n] + rbuf[n].astype(F32)

        @pl.when(u + 1 < U)
        def _():
            pl.semaphore_signal(cred_d, inc=1, device_id={"tp": sib}, device_id_type=MESH)

    def reduce_f(u):
        i = lax.rem(u, 2)
        xr_copy(u).start()
        p1_copy(u).wait_recv()

        @pl.when(u >= 2)
        def _():
            p2_copy(u - 2).wait_send()

        s2[i] = (keep1[i, 1 - gb] + r1[i, 1 - gb].astype(F32)).astype(BF16)

        @pl.when(u >= 2)
        def _():
            pl.semaphore_wait(cred_2, 1)

        p2_copy(u).start()
        keep2[i] = keep1[i, gb] + r1[i, gb].astype(F32)

        @pl.when(u + 2 < U)
        def _():
            pl.semaphore_signal(cred_1, inc=1, device_id={"tp": fnb}, device_id_type=MESH)

    def reduce_g(u):
        i = lax.rem(u, 2)
        xr_copy(u).wait()

        @pl.when(u >= 2)
        def _():
            sent(a_copies(u - 2))

        p2_copy(u).wait_recv()
        yb[i] = (xr[i].astype(F32) + (keep2[i] + r2[i].astype(F32))).astype(BF16)
        for copy in a_copies(u):
            copy.start()

        @pl.when(u + 2 < U)
        def _():
            pl.semaphore_signal(cred_2, inc=1, device_id={"tp": gnb}, device_id_type=MESH)

    def gather_f(u):
        @pl.when(u >= 2)
        def _():
            sent(b_copies(u - 2))

        a_copies(u)[0].wait_recv()
        for copy in b_copies(u):
            copy.start()

    def gather_pair(u):
        @pl.when(u >= 2)
        def _():
            sent(c_copies(u - 2))

        a_copies(u)[1].wait_recv()
        b_copies(u)[0].wait_recv()
        for copy in c_copies(u):
            copy.start()

    def turned(t, cosf, sinf):
        t = t.astype(BF16).astype(F32)
        return (t * cosf + pltpu.roll(t, HEAD // 2, 1) * sinf).astype(BF16)

    def normalize(c):
        for copy in x_copies(c):
            copy.wait()
        piece = 1024

        def norm_rows(r, _):
            rows = pl.ds(pl.multiple_of(r * 16, 16), 16)
            total = jnp.zeros((16, piece), F32)
            for n in range(D // piece):
                wide = xb[rows, n * piece : (n + 1) * piece].astype(F32)
                total = total + wide * wide
            scale = lax.rsqrt(jnp.sum(total, -1, keepdims=True) * (1 / D) + 1e-6)
            for n in range(D // piece):
                at = slice(n * piece, (n + 1) * piece)
                xb[rows, at] = (xb[rows, at].astype(F32) * scale * gain_s[:, at]).astype(BF16)
            return 0

        lax.fori_loop(0, R // 16, norm_rows, 0)

    def turns(c):
        cs = rope_s[pl.ds(pl.multiple_of(c * R, R), R), :]
        sc = pltpu.roll(cs, HEAD // 2, 1)
        low = lax.broadcasted_iota(jnp.int32, (R, HEAD), 1) < HEAD // 2
        return jnp.where(low, cs, sc), jnp.where(low, -sc, cs)

    def keys_values(c):
        @pl.when(c == 0)
        def _():
            rope_copy.wait()
            wk_copy.wait()
            wv_copy.wait()

            for n in (2, 3):
                wq_copy(n).start()

        here = pl.ds(pl.multiple_of(c * R, R), R)
        kv = _dot(xb[...], wkv_s[...], 1, 0)
        k_s[here, :] = turned(kv[:, :HEAD], *turns(c))
        vt_s[:HEAD, here] = kv[:, HEAD:].T.astype(BF16)

    def queries(c, first, last):
        def tile(n, _):
            @pl.when(c == 0)
            def _():
                wq_copy(n).wait()

            @pl.when((c == 0) & (n == 1))
            def _():
                for s in range(PER):
                    for j in range(4):
                        wo_copy((1 - a) * 4 + j, s).start()
                    for j in range(4):
                        wo_copy(a * 4 + j, s).start()

            q = _dot(xb[...], wq_s[:, pl.ds(pl.multiple_of(n * 256, 256), 256)], 1, 0)
            cosf, sinf = turns(c)
            for h in range(2):
                q_s[pl.ds(pl.multiple_of((2 * n + h) * R, R), R), :] = turned(q[:, h * HEAD : (h + 1) * HEAD], cosf, sinf)
            return 0

        lax.fori_loop(first, last, tile, 0)

        @pl.when((last == 4) & (c + 1 < CHUNKS))
        def _():
            for copy in x_copies(c + 1):
                copy.start()

    def attention(c, part):
        e = HEAD**-0.5 * LOG2E
        pieces = range(0, COLS, STRIP)

        def keys(j, masked):
            here = pl.ds(pl.multiple_of(j * R, R), R)
            scores = [_dot(k_s[here, :], q_s[at : at + STRIP, :], 1, 1) for at in pieces]
            if masked:
                ok = lax.rem(lax.broadcasted_iota(jnp.int32, (R, STRIP), 1), R) >= lax.broadcasted_iota(jnp.int32, (R, STRIP), 0)
            weights, keeps = [], []
            for at, s in zip(pieces, scores):
                if masked:
                    s = jnp.where(ok, s, HIDDEN)
                old = top_s[0:1, at : at + STRIP]
                top = jnp.maximum(old, s.max(axis=0, keepdims=True))
                top_s[0:1, at : at + STRIP] = top
                weights.append(jnp.exp2((s - top) * e).astype(BF16))
                keeps.append(jnp.exp2((old - top) * e))
            for at, p, keep in zip(pieces, weights, keeps):
                mix_s[:, at : at + STRIP] = mix_s[:, at : at + STRIP] * keep + _dot(vt_s[:, here], p, 1, 0)

        def whole(j, _):
            keys(j, False)
            return 0

        @pl.when(part == 0)
        def _():
            top_s[...] = jnp.full((8, COLS), NEG, F32)
            mix_s[...] = jnp.zeros((VROWS, COLS), F32)

        lax.fori_loop(jnp.where(part == 0, 0, c // 2), jnp.where(part == 0, c // 2, c), whole, 0)

        @pl.when(part == 1)
        def _():
            keys(c, True)
            for h in range(HEADS):
                at = slice(h * R, (h + 1) * R)
                seen_s[:, h * HEAD : (h + 1) * HEAD] = (mix_s[:HEAD, at] * (1 / mix_s[HEAD : HEAD + 1, at])).T.astype(BF16)

    def tile(u, owner):
        s = lax.rem(u, PER)

        @pl.when(u < PER)
        def _():
            wo_copy(owner, s).wait()

        return _dot(seen_s[...], wo_s[:, columns(owner, s)], 1, 0)

    def output_theirs(u):
        @pl.when(u >= 1)
        def _():
            sent(d_copies(u - 1))
            pl.semaphore_wait(cred_d, 1)

        def theirs(j, _):
            sbuf[j] = tile(u, (1 - a) * 4 + j).astype(BF16)
            d_copy(j).start()
            return 0

        lax.fori_loop(0, 4, theirs, 0)

    def output_ours(u):
        def ours(j, _):
            own[j] = tile(u, a * 4 + j)
            return 0

        lax.fori_loop(0, 4, ours, 0)

    def slot(g, _):
        for stage in (reduce_pair, reduce_f, reduce_g, gather_f, gather_pair):
            first, second = (g + 99 * SLOTS - at for at in WHEN[stage.__name__])
            is_first = lax.rem(first, SLOTS) == 0
            n = jnp.where(is_first, first, second) // SLOTS - 100

            @pl.when((is_first | (lax.rem(second, SLOTS) == 0)) & (n >= 0) & (n < CHUNKS))
            def _(stage=stage, n=n, is_first=is_first):
                stage(2 * n + jnp.where(is_first, 0, 1))

        c = g // SLOTS - 1
        k = lax.rem(g, SLOTS)
        live = (c >= 0) & (c < CHUNKS)

        @pl.when(live & (k < 2))
        def _():
            attention(c, k)

        @pl.when(live & ((k == 2) | (k == 4)))
        def _():
            output_theirs(2 * c + k // 4)

        @pl.when(live & ((k == 3) | (k == 5)))
        def _():
            output_ours(2 * c + k // 4)

        more = c + 1 < CHUNKS

        @pl.when(more & (k == 7))
        def _():
            normalize(c + 1)

        @pl.when(more & (k == 8))
        def _():
            keys_values(c + 1)

        @pl.when(more & (k >= 8))
        def _():
            queries(c + 1, 2 * k - 16, 2 * k - 14)

        return 0

    lax.fori_loop(7, SLOTS * CHUNKS + max(map(max, WHEN.values())) + 1, slot, 0)

    sent(d_copies(U - 1))
    for u in (U - 2, U - 1):
        p1_copy(u).wait_send()
        p2_copy(u).wait_send()
        sent(a_copies(u))
        sent(b_copies(u))
        sent(c_copies(u))

    def arrivals(u, _):
        a_copies(u)[2].wait_recv()
        b_copies(u)[1].wait_recv()
        for copy in c_copies(u):
            copy.wait_recv()
        return 0

    lax.fori_loop(0, U, arrivals, 0)


def _tables():
    half = HEAD // 2
    angle = np.arange(ROWS, dtype=np.float64)[:, None] * np.float64(THETA) ** (-np.arange(half, dtype=np.float64) / half)
    return np.concatenate([np.cos(angle), np.sin(angle)], 1).astype(np.float32)


def solution(mesh):
    def step(x, gain, wq, wk, wv, wo):
        any_ = pl.BlockSpec(memory_space=pl.ANY)
        dma = pltpu.SemaphoreType.DMA
        return pl.pallas_call(
            _kernel,
            name="layer",
            out_shape=jax.ShapeDtypeStruct((ROWS, D), BF16),
            in_specs=[any_, pl.BlockSpec(memory_space=pltpu.VMEM)] + [any_] * 5,
            out_specs=any_,
            scratch_shapes=[
                pltpu.VMEM((1, D), F32),
                pltpu.VMEM((D, 1024), BF16), pltpu.VMEM((D, 2 * HEAD), BF16), pltpu.VMEM((1024, D), BF16),
                pltpu.VMEM((R, D), BF16), pltpu.VMEM((ROWS, HEAD), F32),
                pltpu.VMEM((ROWS, HEAD), BF16), pltpu.VMEM((VROWS, ROWS), BF16), pltpu.VMEM((COLS, HEAD), BF16),
                pltpu.VMEM((R, 1024), BF16), pltpu.VMEM((VROWS, COLS), F32), pltpu.VMEM((8, COLS), F32),
                pltpu.VMEM((4, R, W), BF16), pltpu.VMEM((4, R, W), F32), pltpu.VMEM((4, R, W), BF16),
                pltpu.VMEM((2, 2, R, W), BF16), pltpu.VMEM((2, 2, R, W), BF16), pltpu.VMEM((2, 2, R, W), F32),
                pltpu.VMEM((2, R, W), BF16), pltpu.VMEM((2, R, W), BF16), pltpu.VMEM((2, R, W), F32),
                pltpu.VMEM((2, R, W), BF16), pltpu.VMEM((2, R, W), BF16),
                dma((7,)), dma((8 * PER,)), dma((4,)), dma((2,)), dma((4,)), dma((4,)), dma((2,)), dma((2,)), dma((2,)), dma((2,)),
                dma((4, 2)), dma((2, 2)), dma((2, 2)), dma((U,)), dma((U,)), dma((U,)), dma((4, U)),
                pltpu.SemaphoreType.REGULAR, pltpu.SemaphoreType.REGULAR, pltpu.SemaphoreType.REGULAR,
            ],
            compiler_params=pltpu.CompilerParams(collective_id=0, has_side_effects=True, vmem_limit_bytes=67043328),
            cost_estimate=pl.CostEstimate(flops=95_000_000_000, bytes_accessed=200_000_000, transcendentals=20_000_000),
        )(x, gain.reshape(D // 128, 128), wq, wk, wv, wo, jnp.asarray(_tables()))

    tokens, columns = P("dp", None), P(None, "tp")
    return jax.shard_map(
        step,
        mesh=mesh,
        in_specs=(tokens, P(None), columns, columns, columns, P("tp", None)),
        out_specs=tokens,
        check_vma=False,
    )
```

```python
import functools

import jax
import jax.numpy as jnp
import numpy as np
from jax import lax
from jax.experimental import pallas as pl
from jax.experimental.pallas import tpu as pltpu
from jax.sharding import PartitionSpec as P

MESH = pl.DeviceIdType.MESH
NEG = -1e30
HIDDEN = 2 * NEG
LOG2E = 1.4426950408889634
HEAD = 128
THETA = 10000
ROWS, D = 2048, 8192
R = 256
W = 512
CHUNKS = ROWS // R
PER = 1024 // W
LOW = 2
NO = 4
U = CHUNKS * PER
HEADS = 8
COLS = HEADS * R
STRIP = 512
VROWS = 144
F32, BF16 = jnp.float32, jnp.bfloat16
SLOTS = 10
WHEN = {"reduce_pair": (4, 7), "reduce_f": (9, 10), "reduce_g": (11, 12), "gather_f": (19, 20), "gather_pair": (21, 25)}


def _dot(a, b, ca, cb):
    return lax.dot_general(a, b, (((ca,), (cb,)), ((), ())), preferred_element_type=F32)


def _kernel(x_ref, gain_ref, wq_ref, wk_ref, wv_ref, wo_ref, rope_ref, zh_ref, zv_ref,
            gain_s, wq_s, wkv_s, wo_s, xb, rope_s, k_s, vt_s, q_s, seen_s, mix_s, top_s,
            sbuf, own, rbuf, s1, r1, keep1, s2, r2, keep2, yb, xr,
            w_sem, wq_sem, wo_sem, x_sem, xr_sem, d_send, d_recv, p1_send, p1_recv, p2_send, p2_recv,
            a_send, b_send, c_send, a1_recv, a2_recv, b1_recv, sib_recv, cred_d, cred_1, cred_2):
    me = lax.axis_index("tp")
    a = lax.rem(me, 2)
    yc = lax.rem(me // 2, 2)
    xc = me // 4
    sib = me + 1 - 2 * a
    xn, yn = me + 4 - 8 * xc, me + 2 - 4 * yc
    fnb, gnb = xn * (1 - a) + yn * a, yn * (1 - a) + xn * a
    fb, gb = xc * (1 - a) + yc * a, yc * (1 - a) + xc * a
    base = a * 4
    o_own, o_g = base + fb * 2 + gb, base + fb * 2 + 1 - gb
    o_f, o_fg = base + (1 - fb) * 2 + gb, base + (1 - fb) * 2 + 1 - gb

    def x_copies(c):
        n = R // 4
        return [pltpu.make_async_copy(x_ref.at[pl.ds(pl.multiple_of(c * R + i * n, n), n), :], xb.at[pl.ds(i * n, n), :], x_sem.at[i]) for i in range(4)]

    def wq_copy(m):
        i = lax.rem(m, 2)
        at = pl.ds(pl.multiple_of(lax.rem(m, 4) * 256, 256), 256)
        return pltpu.make_async_copy(wq_ref.at[:, at], wq_s.at[i], wq_sem.at[i])

    wk_copy = pltpu.make_async_copy(wk_ref, wkv_s.at[:, pl.ds(0, HEAD)], w_sem.at[0])
    wv_copy = pltpu.make_async_copy(wv_ref, wkv_s.at[:, pl.ds(HEAD, HEAD)], w_sem.at[1])
    rope_copy = pltpu.make_async_copy(rope_ref, rope_s, w_sem.at[2])

    def columns(owner, s):
        return pl.ds(pl.multiple_of(owner * 1024 + s * W, W), W)

    def wo_copy(m):
        i = lax.rem(m, NO)
        n = lax.rem(m, 8)
        at = columns(jnp.where(n < 4, (1 - a) * 4 + n, a * 4 + n - 4), lax.rem(m // 8, PER))
        return pltpu.make_async_copy(wo_ref.at[:, at], wo_s.at[i], wo_sem.at[i])

    for copy in x_copies(0):
        copy.start()
    barrier = pltpu.get_barrier_semaphore()
    for other in (sib, fnb, gnb):
        pl.semaphore_signal(barrier, inc=1, device_id={"tp": other}, device_id_type=MESH)
    gain = gain_ref[...].astype(F32)
    for n in range(D // 128):
        gain_s[:, n * 128 : (n + 1) * 128] = gain[n : n + 1, :]
    vt_s[HEAD:, :] = jnp.ones((VROWS - HEAD, ROWS), BF16)
    pl.semaphore_wait(barrier, 3)
    for copy in (wk_copy, wv_copy, rope_copy, wq_copy(0), wq_copy(1)):
        copy.start()

    def remote(src, dst, send, recv, to):
        return pltpu.make_async_remote_copy(src_ref=src, dst_ref=dst, send_sem=send, recv_sem=recv, device_id={"tp": to}, device_id_type=MESH)

    def rows(u, chunk=0):
        return pl.ds(pl.multiple_of((u // PER - chunk) * R, R), R)

    def block(u, owner, low):
        at = columns(owner, lax.rem(u, PER))
        if low is None:
            return zv_ref.at[pl.ds(0, R), at]
        return zh_ref.at[rows(u), at] if low else zv_ref.at[rows(u, LOW), at]

    def d_copy(j):
        return remote(sbuf.at[j], rbuf.at[j], d_send.at[j], d_recv.at[j], sib)

    def d_copies(u):
        return [d_copy(j) for j in range(4)]

    def p1_copy(u):
        i = lax.rem(u, 2)
        return remote(s1.at[i], r1.at[i], p1_send.at[i], p1_recv.at[i], fnb)

    def p2_copy(u):
        i = lax.rem(u, 2)
        return remote(s2.at[i], r2.at[i], p2_send.at[i], p2_recv.at[i], gnb)

    def xr_copy(u):
        i = lax.rem(u, 2)
        return pltpu.make_async_copy(x_ref.at[rows(u), columns(o_own, lax.rem(u, PER))], xr.at[i], xr_sem.at[i])

    def a_copies(u, low=None):
        i = lax.rem(u, 2)
        at = block(u, o_own, low)
        return (remote(yb.at[i], at, a_send.at[0, i], a1_recv.at[u], gnb),
                remote(yb.at[i], at, a_send.at[1, i], a2_recv.at[u], fnb),
                remote(yb.at[i], at, a_send.at[2, i], sib_recv.at[0, u], sib))

    def keep_copy(u):
        i = lax.rem(u, 2)
        return pltpu.make_async_copy(yb.at[i], block(u, o_own, True), a_send.at[3, i])

    def b_copies(u, low=None):
        i = lax.rem(u, 2)
        at = block(u, o_g, low)
        return (remote(at, at, b_send.at[0, i], b1_recv.at[u], fnb),
                remote(at, at, b_send.at[1, i], sib_recv.at[1, u], sib))

    def c_copies(u, low=None):
        i = lax.rem(u, 2)
        at, far = block(u, o_f, low), block(u, o_fg, low)
        return (remote(at, at, c_send.at[0, i], sib_recv.at[2, u], sib),
                remote(far, far, c_send.at[1, i], sib_recv.at[3, u], sib))

    def sent(copies):
        for copy in copies:
            copy.wait_send()

    def start(copies, u):
        @pl.when(u < LOW * PER)
        def _():
            for copy in copies(u, True):
                copy.start()

        @pl.when(u >= LOW * PER)
        def _():
            for copy in copies(u, False):
                copy.start()

    def reduce_pair(u):
        i = lax.rem(u, 2)
        for copy in d_copies(u):
            copy.wait_recv()

        @pl.when(u >= 2)
        def _():
            p1_copy(u - 2).wait_send()

        for j in range(2):
            n = (1 - fb) * 2 + j
            s1[i, j] = (own[n] + rbuf[n].astype(F32)).astype(BF16)

        @pl.when(u >= 2)
        def _():
            pl.semaphore_wait(cred_1, 1)

        p1_copy(u).start()
        for j in range(2):
            n = fb * 2 + j
            keep1[i, j] = own[n] + rbuf[n].astype(F32)

        @pl.when(u + 1 < U)
        def _():
            pl.semaphore_signal(cred_d, inc=1, device_id={"tp": sib}, device_id_type=MESH)

    def reduce_f(u):
        i = lax.rem(u, 2)
        xr_copy(u).start()
        p1_copy(u).wait_recv()

        @pl.when(u >= 2)
        def _():
            p2_copy(u - 2).wait_send()

        s2[i] = (keep1[i, 1 - gb] + r1[i, 1 - gb].astype(F32)).astype(BF16)

        @pl.when(u >= 2)
        def _():
            pl.semaphore_wait(cred_2, 1)

        p2_copy(u).start()
        keep2[i] = keep1[i, gb] + r1[i, gb].astype(F32)

        @pl.when(u + 2 < U)
        def _():
            pl.semaphore_signal(cred_1, inc=1, device_id={"tp": fnb}, device_id_type=MESH)

    def reduce_g(u):
        i = lax.rem(u, 2)
        xr_copy(u).wait()

        @pl.when(u >= 2)
        def _():
            sent(a_copies(u - 2))

        @pl.when((u >= 2) & (u < LOW * PER + 2))
        def _():
            keep_copy(jnp.minimum(u - 2, LOW * PER - 1)).wait()

        p2_copy(u).wait_recv()
        yb[i] = (xr[i].astype(F32) + (keep2[i] + r2[i].astype(F32))).astype(BF16)
        start(a_copies, u)

        @pl.when(u < LOW * PER)
        def _():
            keep_copy(u).start()

        @pl.when(u >= LOW * PER)
        def _():
            zv_ref[rows(u, LOW), columns(o_own, lax.rem(u, PER))] = yb[i]

        @pl.when(u + 2 < U)
        def _():
            pl.semaphore_signal(cred_2, inc=1, device_id={"tp": gnb}, device_id_type=MESH)

    def gather_f(u):
        @pl.when(u >= 2)
        def _():
            sent(b_copies(u - 2))

        a_copies(u)[0].wait_recv()
        start(b_copies, u)

    def gather_pair(u):
        @pl.when(u >= 2)
        def _():
            sent(c_copies(u - 2))

        a_copies(u)[1].wait_recv()
        b_copies(u)[0].wait_recv()
        start(c_copies, u)

    def turned(t, cosf, sinf):
        t = t.astype(BF16).astype(F32)
        return (t * cosf + pltpu.roll(t, HEAD // 2, 1) * sinf).astype(BF16)

    def normalize(c):
        for copy in x_copies(c):
            copy.wait()
        piece = 1024

        def norm_rows(r, _):
            rows = pl.ds(pl.multiple_of(r * 16, 16), 16)
            total = jnp.zeros((16, piece), F32)
            for n in range(D // piece):
                wide = xb[rows, n * piece : (n + 1) * piece].astype(F32)
                total = total + wide * wide
            scale = lax.rsqrt(jnp.sum(total, -1, keepdims=True) * (1 / D) + 1e-6)
            for n in range(D // piece):
                at = slice(n * piece, (n + 1) * piece)
                xb[rows, at] = (xb[rows, at].astype(F32) * scale * gain_s[:, at]).astype(BF16)
            return 0

        lax.fori_loop(0, R // 16, norm_rows, 0)

    def turns(c):
        cs = rope_s[pl.ds(pl.multiple_of(c * R, R), R), :]
        sc = pltpu.roll(cs, HEAD // 2, 1)
        low = lax.broadcasted_iota(jnp.int32, (R, HEAD), 1) < HEAD // 2
        return jnp.where(low, cs, sc), jnp.where(low, -sc, cs)

    def keys_values(c):
        @pl.when(c == 0)
        def _():
            rope_copy.wait()
            wk_copy.wait()
            wv_copy.wait()


        here = pl.ds(pl.multiple_of(c * R, R), R)
        kv = _dot(xb[...], wkv_s[...], 1, 0)
        k_s[here, :] = turned(kv[:, :HEAD], *turns(c))
        vt_s[:HEAD, here] = kv[:, HEAD:].T.astype(BF16)

    def queries(c, first, last):
        def tile(n, _):
            m = 4 * c + n
            wq_copy(m).wait()

            @pl.when(m == 1)
            def _():
                for i in range(NO):
                    wo_copy(i).start()

            q = _dot(xb[...], wq_s[lax.rem(m, 2)], 1, 0)

            @pl.when(m + 2 < 4 * CHUNKS)
            def _():
                wq_copy(m + 2).start()

            cosf, sinf = turns(c)
            for h in range(2):
                q_s[pl.ds(pl.multiple_of((2 * n + h) * R, R), R), :] = turned(q[:, h * HEAD : (h + 1) * HEAD], cosf, sinf)
            return 0

        lax.fori_loop(first, last, tile, 0)

        @pl.when((last == 4) & (c + 1 < CHUNKS))
        def _():
            for copy in x_copies(c + 1):
                copy.start()

    def attention(c, part):
        e = HEAD**-0.5 * LOG2E
        pieces = range(0, COLS, STRIP)

        def keys(j, masked):
            here = pl.ds(pl.multiple_of(j * R, R), R)
            scores = [_dot(k_s[here, :], q_s[at : at + STRIP, :], 1, 1) for at in pieces]
            if masked:
                ok = lax.rem(lax.broadcasted_iota(jnp.int32, (R, STRIP), 1), R) >= lax.broadcasted_iota(jnp.int32, (R, STRIP), 0)
            weights, keeps = [], []
            for at, s in zip(pieces, scores):
                if masked:
                    s = jnp.where(ok, s, HIDDEN)
                old = top_s[0:1, at : at + STRIP]
                top = jnp.maximum(old, s.max(axis=0, keepdims=True))
                top_s[0:1, at : at + STRIP] = top
                weights.append(jnp.exp2((s - top) * e).astype(BF16))
                keeps.append(jnp.exp2((old - top) * e))
            for at, p, keep in zip(pieces, weights, keeps):
                mix_s[:, at : at + STRIP] = mix_s[:, at : at + STRIP] * keep + _dot(vt_s[:, here], p, 1, 0)

        def whole(j, _):
            keys(j, False)
            return 0

        @pl.when(part == 0)
        def _():
            top_s[...] = jnp.full((8, COLS), NEG, F32)
            mix_s[...] = jnp.zeros((VROWS, COLS), F32)

        lax.fori_loop(jnp.where(part == 0, 0, c // 2), jnp.where(part == 0, c // 2, c), whole, 0)

        @pl.when(part == 1)
        def _():
            keys(c, True)
            for h in range(HEADS):
                at = slice(h * R, (h + 1) * R)
                seen_s[:, h * HEAD : (h + 1) * HEAD] = (mix_s[:HEAD, at] * (1 / mix_s[HEAD : HEAD + 1, at])).T.astype(BF16)

    def tile(u, n):
        m = 8 * u + n
        wo_copy(m).wait()
        term = _dot(seen_s[...], wo_s[lax.rem(m, NO)], 1, 0)

        @pl.when(m + NO < 8 * U)
        def _():
            wo_copy(m + NO).start()

        return term

    def output_theirs(u):
        @pl.when(u >= 1)
        def _():
            sent(d_copies(u - 1))
            pl.semaphore_wait(cred_d, 1)

        def theirs(j, _):
            sbuf[j] = tile(u, j).astype(BF16)
            d_copy(j).start()
            return 0

        lax.fori_loop(0, 4, theirs, 0)

    def output_ours(u):
        def ours(j, _):
            own[j] = tile(u, 4 + j)
            return 0

        lax.fori_loop(0, 4, ours, 0)

    def slot(g, _):
        for stage in (reduce_pair, reduce_f, reduce_g, gather_f, gather_pair):
            first, second = (g + 99 * SLOTS - at for at in WHEN[stage.__name__])
            is_first = lax.rem(first, SLOTS) == 0
            n = jnp.where(is_first, first, second) // SLOTS - 100

            @pl.when((is_first | (lax.rem(second, SLOTS) == 0)) & (n >= 0) & (n < CHUNKS))
            def _(stage=stage, n=n, is_first=is_first):
                stage(2 * n + jnp.where(is_first, 0, 1))

        c = g // SLOTS - 1
        k = lax.rem(g, SLOTS)
        live = (c >= 0) & (c < CHUNKS)

        @pl.when(live & (k < 2))
        def _():
            attention(c, k)

        @pl.when(live & ((k == 2) | (k == 4)))
        def _():
            output_theirs(2 * c + k // 4)

        @pl.when(live & ((k == 3) | (k == 5)))
        def _():
            output_ours(2 * c + k // 4)

        more = c + 1 < CHUNKS

        @pl.when(more & (k == 7))
        def _():
            normalize(c + 1)

        @pl.when(more & (k == 8))
        def _():
            keys_values(c + 1)

        @pl.when(more & (k >= 8))
        def _():
            queries(c + 1, 2 * k - 16, 2 * k - 14)

        return 0

    lax.fori_loop(7, SLOTS * CHUNKS + max(map(max, WHEN.values())) + 1, slot, 0)

    sent(d_copies(U - 1))
    for u in (U - 2, U - 1):
        p1_copy(u).wait_send()
        p2_copy(u).wait_send()
        sent(a_copies(u))
        sent(b_copies(u))
        sent(c_copies(u))

    def arrivals(u, _):
        a_copies(u)[2].wait_recv()
        b_copies(u)[1].wait_recv()
        for copy in c_copies(u):
            copy.wait_recv()
        return 0

    lax.fori_loop(0, U, arrivals, 0)


def _place(zh_ref, zv_ref, y_ref, sem):
    n = 128
    copies = [pltpu.make_async_copy(zh_ref.at[pl.ds(at, n), :], y_ref.at[pl.ds(at, n), :], sem.at[at // n]) for at in range(0, LOW * R, n)]
    copies += [pltpu.make_async_copy(zv_ref.at[pl.ds(at - LOW * R, n), :], y_ref.at[pl.ds(at, n), :], sem.at[at // n]) for at in range(LOW * R, ROWS, n)]
    for copy in copies:
        copy.start()
    for copy in copies:
        copy.wait()


def _tables():
    half = HEAD // 2
    angle = np.arange(ROWS, dtype=np.float64)[:, None] * np.float64(THETA) ** (-np.arange(half, dtype=np.float64) / half)
    return np.concatenate([np.cos(angle), np.sin(angle)], 1).astype(np.float32)


def solution(mesh):
    def step(x, gain, wq, wk, wv, wo):
        any_ = pl.BlockSpec(memory_space=pl.ANY)
        dma = pltpu.SemaphoreType.DMA
        zh, zv = pl.pallas_call(
            _kernel,
            name="layer",
            out_shape=[jax.ShapeDtypeStruct((LOW * R, D), BF16), pltpu.VMEM((ROWS - LOW * R, D), BF16)],
            in_specs=[any_, pl.BlockSpec(memory_space=pltpu.VMEM)] + [any_] * 5,
            out_specs=[any_, pl.BlockSpec(memory_space=pltpu.VMEM)],
            scratch_shapes=[
                pltpu.VMEM((1, D), F32),
                pltpu.VMEM((2, D, 256), BF16), pltpu.VMEM((D, 2 * HEAD), BF16), pltpu.VMEM((NO, 1024, W), BF16),
                pltpu.VMEM((R, D), BF16), pltpu.VMEM((ROWS, HEAD), F32),
                pltpu.VMEM((ROWS, HEAD), BF16), pltpu.VMEM((VROWS, ROWS), BF16), pltpu.VMEM((COLS, HEAD), BF16),
                pltpu.VMEM((R, 1024), BF16), pltpu.VMEM((VROWS, COLS), F32), pltpu.VMEM((8, COLS), F32),
                pltpu.VMEM((4, R, W), BF16), pltpu.VMEM((4, R, W), F32), pltpu.VMEM((4, R, W), BF16),
                pltpu.VMEM((2, 2, R, W), BF16), pltpu.VMEM((2, 2, R, W), BF16), pltpu.VMEM((2, 2, R, W), F32),
                pltpu.VMEM((2, R, W), BF16), pltpu.VMEM((2, R, W), BF16), pltpu.VMEM((2, R, W), F32),
                pltpu.VMEM((2, R, W), BF16), pltpu.VMEM((2, R, W), BF16),
                dma((3,)), dma((2,)), dma((NO,)), dma((4,)), dma((2,)), dma((4,)), dma((4,)), dma((2,)), dma((2,)), dma((2,)), dma((2,)),
                dma((4, 2)), dma((2, 2)), dma((2, 2)), dma((U,)), dma((U,)), dma((U,)), dma((4, U)),
                pltpu.SemaphoreType.REGULAR, pltpu.SemaphoreType.REGULAR, pltpu.SemaphoreType.REGULAR,
            ],
            compiler_params=pltpu.CompilerParams(collective_id=0, has_side_effects=True, vmem_limit_bytes=67043328 - (ROWS - LOW * R) * D * 2),
            cost_estimate=pl.CostEstimate(flops=95_000_000_000, bytes_accessed=200_000_000, transcendentals=20_000_000),
        )(x, gain.reshape(D // 128, 128), wq, wk, wv, wo, jnp.asarray(_tables()))
        return pl.pallas_call(
            _place,
            name="place",
            out_shape=jax.ShapeDtypeStruct((ROWS, D), BF16),
            in_specs=[pl.BlockSpec(memory_space=pltpu.VMEM)] * 2,
            out_specs=any_,
            scratch_shapes=[dma((ROWS // 128,))],
            compiler_params=pltpu.CompilerParams(vmem_limit_bytes=2**20),
            cost_estimate=pl.CostEstimate(flops=0, bytes_accessed=42_000_000, transcendentals=0),
        )(zh, zv)

    tokens, columns = P("dp", None), P(None, "tp")
    return jax.shard_map(
        step,
        mesh=mesh,
        in_specs=(tokens, P(None), columns, columns, columns, P("tp", None)),
        out_specs=tokens,
        check_vma=False,
    )
```

```python
import functools

import jax
import jax.numpy as jnp
import numpy as np
from jax import lax
from jax.experimental import pallas as pl
from jax.experimental.pallas import tpu as pltpu
from jax.sharding import PartitionSpec as P

MESH = pl.DeviceIdType.MESH
NEG = -1e30
HIDDEN = 2 * NEG
LOG2E = 1.4426950408889634
HEAD = 128
THETA = 10000
ROWS, D = 2048, 8192
R = 256
W = 512
CHUNKS = ROWS // R
PER = 1024 // W
LOW = 4
NO = 4
U = CHUNKS * PER
HEADS = 8
COLS = HEADS * R
STRIP = 512
VROWS = 144
F32, BF16 = jnp.float32, jnp.bfloat16
SLOTS = 10
WHEN = {"reduce_pair": (4, 7), "reduce_f": (9, 10), "reduce_g": (11, 12), "gather_f": (19, 20), "gather_pair": (21, 25)}


def _dot(a, b, ca, cb):
    return lax.dot_general(a, b, (((ca,), (cb,)), ((), ())), preferred_element_type=F32)


def _kernel(x_ref, gain_ref, wq_ref, wk_ref, wv_ref, wo_ref, rope_ref, zh_ref, z_ref,
            gain_s, wkv_s, wo_s, xb, rope_s, k_s, vt_s, q_s, seen_s, mix_s, top_s,
            sbuf, own, rbuf, s1, r1, keep1, s2, r2, keep2, yb, xr,
            w_sem, wq_sem, fetch_sem, wo_sem, x_sem, xr_sem, d_send, d_recv, p1_send, p1_recv, p2_send, p2_recv,
            a_send, b_send, c_send, a1_recv, a2_recv, b1_recv, sib_recv, cred_d, cred_1, cred_2):
    me = lax.axis_index("tp")
    a = lax.rem(me, 2)
    yc = lax.rem(me // 2, 2)
    xc = me // 4
    sib = me + 1 - 2 * a
    xn, yn = me + 4 - 8 * xc, me + 2 - 4 * yc
    fnb, gnb = xn * (1 - a) + yn * a, yn * (1 - a) + xn * a
    fb, gb = xc * (1 - a) + yc * a, yc * (1 - a) + xc * a
    base = a * 4
    o_own, o_g = base + fb * 2 + gb, base + fb * 2 + 1 - gb
    o_f, o_fg = base + (1 - fb) * 2 + gb, base + (1 - fb) * 2 + 1 - gb

    def x_copies(c):
        n = R // 4
        return [pltpu.make_async_copy(x_ref.at[pl.ds(pl.multiple_of(c * R + i * n, n), n), :], xb.at[pl.ds(i * n, n), :], x_sem.at[i]) for i in range(4)]

    def heads_at(n, k):
        return pl.ds(pl.multiple_of(k * 1024 + n * 256, 256), 256)

    def wq_copies(n):
        low = pl.ds(0, LOW * R)
        return [pltpu.make_async_copy(wq_ref.at[pl.ds(k * 1024, 1024), heads_at(n, 0)], z_ref.at[low, heads_at(n, k)], wq_sem.at[n, k]) for k in range(D // 1024)]

    def load(copies):
        for copy in copies:
            copy.start()

    def fetch_copies():
        n = LOW * R // 8
        return [pltpu.make_async_copy(zh_ref.at[pl.ds(i * n, n), :], z_ref.at[pl.ds(i * n, n), :], fetch_sem.at[i]) for i in range(8)]

    wk_copy = pltpu.make_async_copy(wk_ref, wkv_s.at[:, pl.ds(0, HEAD)], w_sem.at[0])
    wv_copy = pltpu.make_async_copy(wv_ref, wkv_s.at[:, pl.ds(HEAD, HEAD)], w_sem.at[1])
    rope_copy = pltpu.make_async_copy(rope_ref, rope_s, w_sem.at[2])

    def columns(owner, s):
        return pl.ds(pl.multiple_of(owner * 1024 + s * W, W), W)

    def wo_copy(m):
        i = lax.rem(m, NO)
        n = lax.rem(m, 8)
        at = columns(jnp.where(n < 4, (1 - a) * 4 + n, a * 4 + n - 4), lax.rem(m // 8, PER))
        return pltpu.make_async_copy(wo_ref.at[:, at], wo_s.at[i], wo_sem.at[i])

    for copy in x_copies(0):
        copy.start()
    barrier = pltpu.get_barrier_semaphore()
    for other in (sib, fnb, gnb):
        pl.semaphore_signal(barrier, inc=1, device_id={"tp": other}, device_id_type=MESH)
    wk_copy.start()
    wv_copy.start()
    load(wq_copies(0))
    gain = gain_ref[...].astype(F32)
    for n in range(D // 128):
        gain_s[:, n * 128 : (n + 1) * 128] = gain[n : n + 1, :]
    vt_s[HEAD:, :] = jnp.ones((VROWS - HEAD, ROWS), BF16)
    pl.semaphore_wait(barrier, 3)
    rope_copy.start()
    load(wq_copies(1))

    def remote(src, dst, send, recv, to):
        return pltpu.make_async_remote_copy(src_ref=src, dst_ref=dst, send_sem=send, recv_sem=recv, device_id={"tp": to}, device_id_type=MESH)

    def rows(u):
        return pl.ds(pl.multiple_of(u // PER * R, R), R)

    def block(u, owner, low):
        at = columns(owner, lax.rem(u, PER))
        if low is None:
            return z_ref.at[pl.ds(LOW * R, R), at]
        return (zh_ref if low else z_ref).at[rows(u), at]

    def d_copy(j):
        return remote(sbuf.at[j], rbuf.at[j], d_send.at[j], d_recv.at[j], sib)

    def d_copies(u):
        return [d_copy(j) for j in range(4)]

    def p1_copy(u):
        i = lax.rem(u, 2)
        return remote(s1.at[i], r1.at[i], p1_send.at[i], p1_recv.at[i], fnb)

    def p2_copy(u):
        i = lax.rem(u, 2)
        return remote(s2.at[i], r2.at[i], p2_send.at[i], p2_recv.at[i], gnb)

    def xr_copy(u):
        i = lax.rem(u, 2)
        return pltpu.make_async_copy(x_ref.at[rows(u), columns(o_own, lax.rem(u, PER))], xr.at[i], xr_sem.at[i])

    def a_copies(u, low=None):
        i = lax.rem(u, 2)
        at = block(u, o_own, low)
        return (remote(yb.at[i], at, a_send.at[0, i], a1_recv.at[u], gnb),
                remote(yb.at[i], at, a_send.at[1, i], a2_recv.at[u], fnb),
                remote(yb.at[i], at, a_send.at[2, i], sib_recv.at[0, u], sib))

    def keep_copy(u):
        i = lax.rem(u, 2)
        return pltpu.make_async_copy(yb.at[i], block(u, o_own, True), a_send.at[3, i])

    def b_copies(u, low=None):
        i = lax.rem(u, 2)
        at = block(u, o_g, low)
        return (remote(at, at, b_send.at[0, i], b1_recv.at[u], fnb),
                remote(at, at, b_send.at[1, i], sib_recv.at[1, u], sib))

    def c_copies(u, low=None):
        i = lax.rem(u, 2)
        at, far = block(u, o_f, low), block(u, o_fg, low)
        return (remote(at, at, c_send.at[0, i], sib_recv.at[2, u], sib),
                remote(far, far, c_send.at[1, i], sib_recv.at[3, u], sib))

    def sent(copies):
        for copy in copies:
            copy.wait_send()

    def start(copies, u):
        @pl.when(u < LOW * PER)
        def _():
            for copy in copies(u, True):
                copy.start()

        @pl.when(u >= LOW * PER)
        def _():
            for copy in copies(u, False):
                copy.start()

    def reduce_pair(u):
        i = lax.rem(u, 2)
        for copy in d_copies(u):
            copy.wait_recv()

        @pl.when(u >= 2)
        def _():
            p1_copy(u - 2).wait_send()

        for j in range(2):
            n = (1 - fb) * 2 + j
            s1[i, j] = (own[n] + rbuf[n].astype(F32)).astype(BF16)

        @pl.when(u >= 2)
        def _():
            pl.semaphore_wait(cred_1, 1)

        p1_copy(u).start()
        for j in range(2):
            n = fb * 2 + j
            keep1[i, j] = own[n] + rbuf[n].astype(F32)

        @pl.when(u + 1 < U)
        def _():
            pl.semaphore_signal(cred_d, inc=1, device_id={"tp": sib}, device_id_type=MESH)

    def reduce_f(u):
        i = lax.rem(u, 2)
        xr_copy(u).start()
        p1_copy(u).wait_recv()

        @pl.when(u >= 2)
        def _():
            p2_copy(u - 2).wait_send()

        s2[i] = (keep1[i, 1 - gb] + r1[i, 1 - gb].astype(F32)).astype(BF16)

        @pl.when(u >= 2)
        def _():
            pl.semaphore_wait(cred_2, 1)

        p2_copy(u).start()
        keep2[i] = keep1[i, gb] + r1[i, gb].astype(F32)

        @pl.when(u + 2 < U)
        def _():
            pl.semaphore_signal(cred_1, inc=1, device_id={"tp": fnb}, device_id_type=MESH)

    def reduce_g(u):
        i = lax.rem(u, 2)
        xr_copy(u).wait()

        @pl.when(u >= 2)
        def _():
            sent(a_copies(u - 2))

        @pl.when((u >= 2) & (u < LOW * PER + 2))
        def _():
            keep_copy(jnp.minimum(u - 2, LOW * PER - 1)).wait()

        p2_copy(u).wait_recv()
        yb[i] = (xr[i].astype(F32) + (keep2[i] + r2[i].astype(F32))).astype(BF16)
        start(a_copies, u)

        @pl.when(u < LOW * PER)
        def _():
            keep_copy(u).start()

        @pl.when(u >= LOW * PER)
        def _():
            z_ref[rows(u), columns(o_own, lax.rem(u, PER))] = yb[i]

        @pl.when(u + 2 < U)
        def _():
            pl.semaphore_signal(cred_2, inc=1, device_id={"tp": gnb}, device_id_type=MESH)

    def gather_f(u):
        @pl.when(u >= 2)
        def _():
            sent(b_copies(u - 2))

        a_copies(u)[0].wait_recv()
        start(b_copies, u)

    def gather_pair(u):
        @pl.when(u >= 2)
        def _():
            sent(c_copies(u - 2))

        a_copies(u)[1].wait_recv()
        b_copies(u)[0].wait_recv()
        start(c_copies, u)

    def turned(t, cosf, sinf):
        t = t.astype(BF16).astype(F32)
        return (t * cosf + pltpu.roll(t, HEAD // 2, 1) * sinf).astype(BF16)

    def normalize(c):
        piece = 1024

        def norm_rows(r, _):
            rows = pl.ds(pl.multiple_of(r * 16, 16), 16)
            total = jnp.zeros((16, piece), F32)
            for n in range(D // piece):
                wide = xb[rows, n * piece : (n + 1) * piece].astype(F32)
                total = total + wide * wide
            scale = lax.rsqrt(jnp.sum(total, -1, keepdims=True) * (1 / D) + 1e-6)
            for n in range(D // piece):
                at = slice(n * piece, (n + 1) * piece)
                xb[rows, at] = (xb[rows, at].astype(F32) * scale * gain_s[:, at]).astype(BF16)
            return 0

        def quarter(i, _):
            n = R // 4
            at = pl.multiple_of(i * n, n)
            pltpu.make_async_copy(x_ref.at[pl.ds(pl.multiple_of(c * R + at, n), n), :], xb.at[pl.ds(at, n), :], x_sem.at[i]).wait()
            lax.fori_loop(i * (n // 16), (i + 1) * (n // 16), norm_rows, 0)
            return 0

        lax.fori_loop(0, 4, quarter, 0)

    def turns(c):
        cs = rope_s[pl.ds(pl.multiple_of(c * R, R), R), :]
        sc = pltpu.roll(cs, HEAD // 2, 1)
        low = lax.broadcasted_iota(jnp.int32, (R, HEAD), 1) < HEAD // 2
        return jnp.where(low, cs, sc), jnp.where(low, -sc, cs)

    def keys_values(c):
        @pl.when(c == 0)
        def _():
            rope_copy.wait()
            wk_copy.wait()
            wv_copy.wait()
            for n in (2, 3):
                load(wq_copies(n))


        here = pl.ds(pl.multiple_of(c * R, R), R)
        kv = _dot(xb[...], wkv_s[...], 1, 0)
        k_s[here, :] = turned(kv[:, :HEAD], *turns(c))
        vt_s[:HEAD, here] = kv[:, HEAD:].T.astype(BF16)

    def queries(c, first, last):
        def tile(n, _):
            @pl.when(c == 0)
            def _():
                for copy in wq_copies(n):
                    copy.wait()

            @pl.when((c == 0) & (n == 1))
            def _():
                for i in range(NO):
                    wo_copy(i).start()

            q = 0
            for k in range(D // 1024):
                q += _dot(xb[:, k * 1024 : (k + 1) * 1024], z_ref[pl.ds(0, LOW * R), heads_at(n, k)], 1, 0)
            cosf, sinf = turns(c)
            for h in range(2):
                q_s[pl.ds(pl.multiple_of((2 * n + h) * R, R), R), :] = turned(q[:, h * HEAD : (h + 1) * HEAD], cosf, sinf)
            return 0

        lax.fori_loop(first, last, tile, 0)

        @pl.when((last == 4) & (c + 1 < CHUNKS))
        def _():
            for copy in x_copies(c + 1):
                copy.start()

    def attention(c, part):
        e = HEAD**-0.5 * LOG2E
        pieces = range(0, COLS, STRIP)

        def keys(j, masked):
            here = pl.ds(pl.multiple_of(j * R, R), R)
            scores = [_dot(k_s[here, :], q_s[at : at + STRIP, :], 1, 1) for at in pieces]
            if masked:
                ok = lax.rem(lax.broadcasted_iota(jnp.int32, (R, STRIP), 1), R) >= lax.broadcasted_iota(jnp.int32, (R, STRIP), 0)
            weights, keeps = [], []
            for at, s in zip(pieces, scores):
                if masked:
                    s = jnp.where(ok, s, HIDDEN)
                old = top_s[0:1, at : at + STRIP]
                top = jnp.maximum(old, s.max(axis=0, keepdims=True))
                top_s[0:1, at : at + STRIP] = top
                weights.append(jnp.exp2((s - top) * e).astype(BF16))
                keeps.append(jnp.exp2((old - top) * e))
            for at, p, keep in zip(pieces, weights, keeps):
                mix_s[:, at : at + STRIP] = mix_s[:, at : at + STRIP] * keep + _dot(vt_s[:, here], p, 1, 0)

        def whole(j, _):
            keys(j, False)
            return 0

        @pl.when(part == 0)
        def _():
            top_s[...] = jnp.full((8, COLS), NEG, F32)
            mix_s[...] = jnp.zeros((VROWS, COLS), F32)

        lax.fori_loop(jnp.where(part == 0, 0, c // 2), jnp.where(part == 0, c // 2, c), whole, 0)

        @pl.when(part == 1)
        def _():
            keys(c, True)
            for h in range(HEADS):
                at = slice(h * R, (h + 1) * R)
                seen_s[:, h * HEAD : (h + 1) * HEAD] = (mix_s[:HEAD, at] * (1 / mix_s[HEAD : HEAD + 1, at])).T.astype(BF16)

    def tile(u, n):
        m = 8 * u + n
        wo_copy(m).wait()
        term = _dot(seen_s[...], wo_s[lax.rem(m, NO)], 1, 0)

        @pl.when(m + NO < 8 * U)
        def _():
            wo_copy(m + NO).start()

        return term

    def output_theirs(u):
        @pl.when(u >= 1)
        def _():
            sent(d_copies(u - 1))
            pl.semaphore_wait(cred_d, 1)

        def theirs(j, _):
            sbuf[j] = tile(u, j).astype(BF16)
            d_copy(j).start()
            return 0

        lax.fori_loop(0, 4, theirs, 0)

    def output_ours(u):
        def ours(j, _):
            own[j] = tile(u, 4 + j)
            return 0

        lax.fori_loop(0, 4, ours, 0)

    def arrivals(u, _):
        a_copies(u)[2].wait_recv()
        b_copies(u)[1].wait_recv()
        for copy in c_copies(u):
            copy.wait_recv()
        return 0

    def slot(g, _):
        for stage in (reduce_pair, reduce_f, reduce_g, gather_f, gather_pair):
            first, second = (g + 99 * SLOTS - at for at in WHEN[stage.__name__])
            is_first = lax.rem(first, SLOTS) == 0
            n = jnp.where(is_first, first, second) // SLOTS - 100

            @pl.when((is_first | (lax.rem(second, SLOTS) == 0)) & (n >= 0) & (n < CHUNKS))
            def _(stage=stage, n=n, is_first=is_first):
                stage(2 * n + jnp.where(is_first, 0, 1))

        c = g // SLOTS - 1
        k = lax.rem(g, SLOTS)
        live = (c >= 0) & (c < CHUNKS)

        @pl.when(live & (k < 2))
        def _():
            attention(c, k)

        @pl.when(live & ((k == 2) | (k == 4)))
        def _():
            output_theirs(2 * c + k // 4)

        @pl.when(live & ((k == 3) | (k == 5)))
        def _():
            output_ours(2 * c + k // 4)

        @pl.when((c == CHUNKS - 1) & (k == 6))
        def _():
            lax.fori_loop(0, LOW * PER, arrivals, 0)
            for copy in fetch_copies():
                copy.start()

        more = c + 1 < CHUNKS

        @pl.when(more & (k == 7))
        def _():
            normalize(c + 1)

        @pl.when(more & (k == 8))
        def _():
            keys_values(c + 1)

        @pl.when(more & (k >= 8))
        def _():
            queries(c + 1, 2 * k - 16, 2 * k - 14)

        return 0

    lax.fori_loop(7, SLOTS * CHUNKS + max(map(max, WHEN.values())) + 1, slot, 0)

    sent(d_copies(U - 1))
    for u in (U - 2, U - 1):
        p1_copy(u).wait_send()
        p2_copy(u).wait_send()
        sent(a_copies(u))
        sent(b_copies(u))
        sent(c_copies(u))

    lax.fori_loop(LOW * PER, U, arrivals, 0)
    for copy in fetch_copies():
        copy.wait()


def _place(z_ref, y_ref, sem):
    n = ROWS // 32
    copies = [pltpu.make_async_copy(z_ref.at[pl.ds(i * n, n), :], y_ref.at[pl.ds(i * n, n), :], sem.at[i]) for i in range(32)]
    for copy in copies:
        copy.start()
    for copy in copies:
        copy.wait()


def _tables():
    half = HEAD // 2
    angle = np.arange(ROWS, dtype=np.float64)[:, None] * np.float64(THETA) ** (-np.arange(half, dtype=np.float64) / half)
    return np.concatenate([np.cos(angle), np.sin(angle)], 1).astype(np.float32)


def solution(mesh):
    def step(x, gain, wq, wk, wv, wo):
        any_ = pl.BlockSpec(memory_space=pl.ANY)
        dma = pltpu.SemaphoreType.DMA
        _, z = pl.pallas_call(
            _kernel,
            name="layer",
            out_shape=[jax.ShapeDtypeStruct((LOW * R, D), BF16), pltpu.VMEM((ROWS, D), BF16)],
            in_specs=[any_, pl.BlockSpec(memory_space=pltpu.VMEM)] + [any_] * 5,
            out_specs=[any_, pl.BlockSpec(memory_space=pltpu.VMEM)],
            scratch_shapes=[
                pltpu.VMEM((1, D), F32),
                pltpu.VMEM((D, 2 * HEAD), BF16), pltpu.VMEM((NO, 1024, W), BF16),
                pltpu.VMEM((R, D), BF16), pltpu.VMEM((ROWS, HEAD), F32),
                pltpu.VMEM((ROWS, HEAD), BF16), pltpu.VMEM((VROWS, ROWS), BF16), pltpu.VMEM((COLS, HEAD), BF16),
                pltpu.VMEM((R, 1024), BF16), pltpu.VMEM((VROWS, COLS), F32), pltpu.VMEM((8, COLS), F32),
                pltpu.VMEM((4, R, W), BF16), pltpu.VMEM((4, R, W), F32), pltpu.VMEM((4, R, W), BF16),
                pltpu.VMEM((2, 2, R, W), BF16), pltpu.VMEM((2, 2, R, W), BF16), pltpu.VMEM((2, 2, R, W), F32),
                pltpu.VMEM((2, R, W), BF16), pltpu.VMEM((2, R, W), BF16), pltpu.VMEM((2, R, W), F32),
                pltpu.VMEM((2, R, W), BF16), pltpu.VMEM((2, R, W), BF16),
                dma((3,)), dma((4, D // 1024)), dma((8,)), dma((NO,)), dma((4,)), dma((2,)), dma((4,)), dma((4,)), dma((2,)), dma((2,)), dma((2,)), dma((2,)),
                dma((4, 2)), dma((2, 2)), dma((2, 2)), dma((U,)), dma((U,)), dma((U,)), dma((4, U)),
                pltpu.SemaphoreType.REGULAR, pltpu.SemaphoreType.REGULAR, pltpu.SemaphoreType.REGULAR,
            ],
            compiler_params=pltpu.CompilerParams(collective_id=0, has_side_effects=True, vmem_limit_bytes=67043328 - ROWS * D * 2),
            cost_estimate=pl.CostEstimate(flops=95_000_000_000, bytes_accessed=200_000_000, transcendentals=20_000_000),
        )(x, gain.reshape(D // 128, 128), wq, wk, wv, wo, jnp.asarray(_tables()))
        return pl.pallas_call(
            _place,
            name="place",
            out_shape=jax.ShapeDtypeStruct((ROWS, D), BF16),
            in_specs=[pl.BlockSpec(memory_space=pltpu.VMEM)],
            out_specs=any_,
            scratch_shapes=[dma((32,))],
            compiler_params=pltpu.CompilerParams(vmem_limit_bytes=2**20),
            cost_estimate=pl.CostEstimate(flops=0, bytes_accessed=42_000_000, transcendentals=0),
        )(z)

    tokens, columns = P("dp", None), P(None, "tp")
    return jax.shard_map(
        step,
        mesh=mesh,
        in_specs=(tokens, P(None), columns, columns, columns, P("tp", None)),
        out_specs=tokens,
        check_vma=False,
    )
```

```python
import functools

import jax
import jax.numpy as jnp
import numpy as np
from jax import lax
from jax.experimental import pallas as pl
from jax.experimental.pallas import tpu as pltpu
from jax.sharding import PartitionSpec as P

MESH = pl.DeviceIdType.MESH
NEG = -1e30
HIDDEN = 2 * NEG
LOG2E = 1.4426950408889634
HEAD = 128
THETA = 10000
ROWS, D = 2048, 8192
R = 256
W = 512
CHUNKS = ROWS // R
PER = 1024 // W
LOW = 4
NO = 4
U = CHUNKS * PER
HEADS = 8
COLS = HEADS * R
STRIP = 512
VROWS = 144
F32, BF16 = jnp.float32, jnp.bfloat16
SLOTS = 10
WHEN = {"pair_send": (3, 5), "pair_keep": (4, 6), "reduce_f": (9, 10), "reduce_g": (11, 12), "gather_f": (19, 20), "gather_pair": (21, 25)}


def _dot(a, b, ca, cb):
    return lax.dot_general(a, b, (((ca,), (cb,)), ((), ())), preferred_element_type=F32)


def _kernel(x_ref, gain_ref, wq_ref, wk_ref, wv_ref, wo_ref, rope_ref, zh_ref, z_ref,
            gain_s, wkv_s, wo_s, xb, rope_s, k_s, vt_s, q_s, seen_s, mix_s, top_s,
            sbuf, own, rbuf, s1, r1, keep1, s2, r2, keep2, yb, xr,
            w_sem, wq_sem, fetch_sem, wo_sem, x_sem, xr_sem, d_send, d_recv, p1_send, p1_recv, p2_send, p2_recv,
            a_send, b_send, c_send, a1_recv, a2_recv, b1_recv, sib_recv, cred_d, cred_1, cred_2):
    me = lax.axis_index("tp")
    a = lax.rem(me, 2)
    yc = lax.rem(me // 2, 2)
    xc = me // 4
    sib = me + 1 - 2 * a
    xn, yn = me + 4 - 8 * xc, me + 2 - 4 * yc
    fnb, gnb = xn * (1 - a) + yn * a, yn * (1 - a) + xn * a
    fb, gb = xc * (1 - a) + yc * a, yc * (1 - a) + xc * a
    base = a * 4
    o_own, o_g = base + fb * 2 + gb, base + fb * 2 + 1 - gb
    o_f, o_fg = base + (1 - fb) * 2 + gb, base + (1 - fb) * 2 + 1 - gb


    def theirs_of(part):
        return jnp.where(part == 0, 1 - gb, gb) * 2

    def ours_of(part):
        return jnp.where(part == 0, 1 - fb, fb) * 2

    def x_copies(c):
        n = R // 4
        return [pltpu.make_async_copy(x_ref.at[pl.ds(pl.multiple_of(c * R + i * n, n), n), :], xb.at[pl.ds(i * n, n), :], x_sem.at[i]) for i in range(4)]

    def heads_at(n, k):
        return pl.ds(pl.multiple_of(k * 1024 + n * 256, 256), 256)

    def wq_copies(n):
        low = pl.ds(0, LOW * R)
        return [pltpu.make_async_copy(wq_ref.at[pl.ds(k * 1024, 1024), heads_at(n, 0)], z_ref.at[low, heads_at(n, k)], wq_sem.at[n, k]) for k in range(D // 1024)]

    def load(copies):
        for copy in copies:
            copy.start()

    def fetch_copies():
        n = LOW * R // 8
        return [pltpu.make_async_copy(zh_ref.at[pl.ds(i * n, n), :], z_ref.at[pl.ds(i * n, n), :], fetch_sem.at[i]) for i in range(8)]

    wk_copy = pltpu.make_async_copy(wk_ref, wkv_s.at[:, pl.ds(0, HEAD)], w_sem.at[0])
    wv_copy = pltpu.make_async_copy(wv_ref, wkv_s.at[:, pl.ds(HEAD, HEAD)], w_sem.at[1])
    rope_copy = pltpu.make_async_copy(rope_ref, rope_s, w_sem.at[2])

    def columns(owner, s):
        return pl.ds(pl.multiple_of(owner * 1024 + s * W, W), W)

    def wo_copy(m):
        i = lax.rem(m, NO)
        part, n = lax.rem(m, 8) // 4, lax.rem(m, 4)
        owner = jnp.where(n < 2, (1 - a) * 4 + theirs_of(part) + n, base + ours_of(part) + n - 2)
        at = columns(owner, lax.rem(m // 8, PER))
        return pltpu.make_async_copy(wo_ref.at[:, at], wo_s.at[i], wo_sem.at[i])

    for copy in x_copies(0):
        copy.start()
    barrier = pltpu.get_barrier_semaphore()
    for other in (sib, fnb, gnb):
        pl.semaphore_signal(barrier, inc=1, device_id={"tp": other}, device_id_type=MESH)
    wk_copy.start()
    wv_copy.start()
    load(wq_copies(0))
    gain = gain_ref[...].astype(F32)
    for n in range(D // 128):
        gain_s[:, n * 128 : (n + 1) * 128] = gain[n : n + 1, :]
    vt_s[HEAD:, :] = jnp.ones((VROWS - HEAD, ROWS), BF16)
    pl.semaphore_wait(barrier, 3)
    rope_copy.start()
    load(wq_copies(1))

    def remote(src, dst, send, recv, to):
        return pltpu.make_async_remote_copy(src_ref=src, dst_ref=dst, send_sem=send, recv_sem=recv, device_id={"tp": to}, device_id_type=MESH)

    def rows(u):
        return pl.ds(pl.multiple_of(u // PER * R, R), R)

    def block(u, owner, low):
        at = columns(owner, lax.rem(u, PER))
        if low is None:
            return z_ref.at[pl.ds(LOW * R, R), at]
        return (zh_ref if low else z_ref).at[rows(u), at]

    def d_copy(j):
        return remote(sbuf.at[j], rbuf.at[j], d_send.at[j], d_recv.at[j], sib)

    def d_copies(u):
        return [d_copy(j) for j in range(4)]

    def p1_copy(u):
        i = lax.rem(u, 2)
        return remote(s1.at[i], r1.at[i], p1_send.at[i], p1_recv.at[i], fnb)

    def p2_copy(u):
        i = lax.rem(u, 2)
        return remote(s2.at[i], r2.at[i], p2_send.at[i], p2_recv.at[i], gnb)

    def xr_copy(u):
        i = lax.rem(u, 2)
        return pltpu.make_async_copy(x_ref.at[rows(u), columns(o_own, lax.rem(u, PER))], xr.at[i], xr_sem.at[i])

    def a_copies(u, low=None):
        i = lax.rem(u, 2)
        at = block(u, o_own, low)
        return (remote(yb.at[i], at, a_send.at[0, i], a1_recv.at[u], gnb),
                remote(yb.at[i], at, a_send.at[1, i], a2_recv.at[u], fnb),
                remote(yb.at[i], at, a_send.at[2, i], sib_recv.at[0, u], sib))

    def keep_copy(u):
        i = lax.rem(u, 2)
        return pltpu.make_async_copy(yb.at[i], block(u, o_own, True), a_send.at[3, i])

    def b_copies(u, low=None):
        i = lax.rem(u, 2)
        at = block(u, o_g, low)
        return (remote(at, at, b_send.at[0, i], b1_recv.at[u], fnb),
                remote(at, at, b_send.at[1, i], sib_recv.at[1, u], sib))

    def c_copies(u, low=None):
        i = lax.rem(u, 2)
        at, far = block(u, o_f, low), block(u, o_fg, low)
        return (remote(at, at, c_send.at[0, i], sib_recv.at[2, u], sib),
                remote(far, far, c_send.at[1, i], sib_recv.at[3, u], sib))

    def sent(copies):
        for copy in copies:
            copy.wait_send()

    def start(copies, u):
        @pl.when(u < LOW * PER)
        def _():
            for copy in copies(u, True):
                copy.start()

        @pl.when(u >= LOW * PER)
        def _():
            for copy in copies(u, False):
                copy.start()

    def pair_send(u):
        i = lax.rem(u, 2)
        for j in range(2):
            d_copy((1 - fb) * 2 + j).wait_recv()

        @pl.when(u >= 2)
        def _():
            p1_copy(u - 2).wait_send()

        for j in range(2):
            n = (1 - fb) * 2 + j
            s1[i, j] = (own[n] + rbuf[n].astype(F32)).astype(BF16)

        @pl.when(u >= 2)
        def _():
            pl.semaphore_wait(cred_1, 1)

        p1_copy(u).start()

    def pair_keep(u):
        i = lax.rem(u, 2)
        for j in range(2):
            n = fb * 2 + j
            d_copy(n).wait_recv()
            keep1[i, j] = own[n] + rbuf[n].astype(F32)

        @pl.when(u + 1 < U)
        def _():
            pl.semaphore_signal(cred_d, inc=1, device_id={"tp": sib}, device_id_type=MESH)

    def reduce_f(u):
        i = lax.rem(u, 2)
        xr_copy(u).start()
        p1_copy(u).wait_recv()

        @pl.when(u >= 2)
        def _():
            p2_copy(u - 2).wait_send()

        s2[i] = (keep1[i, 1 - gb] + r1[i, 1 - gb].astype(F32)).astype(BF16)

        @pl.when(u >= 2)
        def _():
            pl.semaphore_wait(cred_2, 1)

        p2_copy(u).start()
        keep2[i] = keep1[i, gb] + r1[i, gb].astype(F32)

        @pl.when(u + 2 < U)
        def _():
            pl.semaphore_signal(cred_1, inc=1, device_id={"tp": fnb}, device_id_type=MESH)

    def reduce_g(u):
        i = lax.rem(u, 2)
        xr_copy(u).wait()

        @pl.when(u >= 2)
        def _():
            sent(a_copies(u - 2))

        @pl.when((u >= 2) & (u < LOW * PER + 2))
        def _():
            keep_copy(jnp.minimum(u - 2, LOW * PER - 1)).wait()

        p2_copy(u).wait_recv()
        yb[i] = (xr[i].astype(F32) + (keep2[i] + r2[i].astype(F32))).astype(BF16)
        start(a_copies, u)

        @pl.when(u < LOW * PER)
        def _():
            keep_copy(u).start()

        @pl.when(u >= LOW * PER)
        def _():
            z_ref[rows(u), columns(o_own, lax.rem(u, PER))] = yb[i]

        @pl.when(u + 2 < U)
        def _():
            pl.semaphore_signal(cred_2, inc=1, device_id={"tp": gnb}, device_id_type=MESH)

    def gather_f(u):
        @pl.when(u >= 2)
        def _():
            sent(b_copies(u - 2))

        a_copies(u)[0].wait_recv()
        start(b_copies, u)

    def gather_pair(u):
        @pl.when(u >= 2)
        def _():
            sent(c_copies(u - 2))

        a_copies(u)[1].wait_recv()
        b_copies(u)[0].wait_recv()
        start(c_copies, u)

    def turned(t, cosf, sinf):
        t = t.astype(BF16).astype(F32)
        return (t * cosf + pltpu.roll(t, HEAD // 2, 1) * sinf).astype(BF16)

    def normalize(c):
        piece = 1024

        def norm_rows(r, _):
            rows = pl.ds(pl.multiple_of(r * 16, 16), 16)
            total = jnp.zeros((16, piece), F32)
            for n in range(D // piece):
                wide = xb[rows, n * piece : (n + 1) * piece].astype(F32)
                total = total + wide * wide
            scale = lax.rsqrt(jnp.sum(total, -1, keepdims=True) * (1 / D) + 1e-6)
            for n in range(D // piece):
                at = slice(n * piece, (n + 1) * piece)
                xb[rows, at] = (xb[rows, at].astype(F32) * scale * gain_s[:, at]).astype(BF16)
            return 0

        def quarter(i, _):
            n = R // 4
            at = pl.multiple_of(i * n, n)
            pltpu.make_async_copy(x_ref.at[pl.ds(pl.multiple_of(c * R + at, n), n), :], xb.at[pl.ds(at, n), :], x_sem.at[i]).wait()
            lax.fori_loop(i * (n // 16), (i + 1) * (n // 16), norm_rows, 0)
            return 0

        lax.fori_loop(0, 4, quarter, 0)

    def turns(c):
        cs = rope_s[pl.ds(pl.multiple_of(c * R, R), R), :]
        sc = pltpu.roll(cs, HEAD // 2, 1)
        low = lax.broadcasted_iota(jnp.int32, (R, HEAD), 1) < HEAD // 2
        return jnp.where(low, cs, sc), jnp.where(low, -sc, cs)

    def keys_values(c):
        @pl.when(c == 0)
        def _():
            rope_copy.wait()
            wk_copy.wait()
            wv_copy.wait()
            for n in (2, 3):
                load(wq_copies(n))


        here = pl.ds(pl.multiple_of(c * R, R), R)
        kv = _dot(xb[...], wkv_s[...], 1, 0)
        k_s[here, :] = turned(kv[:, :HEAD], *turns(c))
        vt_s[:HEAD, here] = kv[:, HEAD:].T.astype(BF16)

    def queries(c, first, last):
        def tile(n, _):
            @pl.when(c == 0)
            def _():
                for copy in wq_copies(n):
                    copy.wait()

            @pl.when((c == 0) & (n == 1))
            def _():
                for i in range(NO):
                    wo_copy(i).start()

            q = 0
            for k in range(D // 1024):
                q += _dot(xb[:, k * 1024 : (k + 1) * 1024], z_ref[pl.ds(0, LOW * R), heads_at(n, k)], 1, 0)
            cosf, sinf = turns(c)
            for h in range(2):
                q_s[pl.ds(pl.multiple_of((2 * n + h) * R, R), R), :] = turned(q[:, h * HEAD : (h + 1) * HEAD], cosf, sinf)
            return 0

        lax.fori_loop(first, last, tile, 0)

        @pl.when((last == 4) & (c + 1 < CHUNKS))
        def _():
            for copy in x_copies(c + 1):
                copy.start()

    def attention(c, part):
        e = HEAD**-0.5 * LOG2E
        pieces = range(0, COLS, STRIP)

        def keys(j, masked):
            here = pl.ds(pl.multiple_of(j * R, R), R)
            scores = [_dot(k_s[here, :], q_s[at : at + STRIP, :], 1, 1) for at in pieces]
            if masked:
                ok = lax.rem(lax.broadcasted_iota(jnp.int32, (R, STRIP), 1), R) >= lax.broadcasted_iota(jnp.int32, (R, STRIP), 0)
            weights, keeps = [], []
            for at, s in zip(pieces, scores):
                if masked:
                    s = jnp.where(ok, s, HIDDEN)
                old = top_s[0:1, at : at + STRIP]
                top = jnp.maximum(old, s.max(axis=0, keepdims=True))
                top_s[0:1, at : at + STRIP] = top
                weights.append(jnp.exp2((s - top) * e).astype(BF16))
                keeps.append(jnp.exp2((old - top) * e))
            for at, p, keep in zip(pieces, weights, keeps):
                mix_s[:, at : at + STRIP] = mix_s[:, at : at + STRIP] * keep + _dot(vt_s[:, here], p, 1, 0)

        def whole(j, _):
            keys(j, False)
            return 0

        @pl.when(part == 0)
        def _():
            top_s[...] = jnp.full((8, COLS), NEG, F32)
            mix_s[...] = jnp.zeros((VROWS, COLS), F32)

        lax.fori_loop(jnp.where(part == 0, 0, c // 2), jnp.where(part == 0, c // 2, c), whole, 0)

        @pl.when(part == 1)
        def _():
            keys(c, True)
            for h in range(HEADS):
                at = slice(h * R, (h + 1) * R)
                seen_s[:, h * HEAD : (h + 1) * HEAD] = (mix_s[:HEAD, at] * (1 / mix_s[HEAD : HEAD + 1, at])).T.astype(BF16)

    def tile(u, n):
        m = 8 * u + n
        wo_copy(m).wait()
        term = _dot(seen_s[...], wo_s[lax.rem(m, NO)], 1, 0)

        @pl.when(m + NO < 8 * U)
        def _():
            wo_copy(m + NO).start()

        return term

    def output(u, part):
        @pl.when((u >= 1) & (part == 0))
        def _():
            sent(d_copies(u - 1))
            pl.semaphore_wait(cred_d, 1)

        def theirs(n, _):
            j = theirs_of(part) + n
            sbuf[j] = tile(u, 4 * part + n).astype(BF16)
            d_copy(j).start()
            return 0

        def ours(n, _):
            own[ours_of(part) + n] = tile(u, 4 * part + 2 + n)
            return 0

        lax.fori_loop(0, 2, theirs, 0)
        lax.fori_loop(0, 2, ours, 0)

    def arrivals(u, _):
        a_copies(u)[2].wait_recv()
        b_copies(u)[1].wait_recv()
        for copy in c_copies(u):
            copy.wait_recv()
        return 0

    def slot(g, _):
        for stage in (pair_send, pair_keep, reduce_f, reduce_g, gather_f, gather_pair):
            first, second = (g + 99 * SLOTS - at for at in WHEN[stage.__name__])
            is_first = lax.rem(first, SLOTS) == 0
            n = jnp.where(is_first, first, second) // SLOTS - 100

            @pl.when((is_first | (lax.rem(second, SLOTS) == 0)) & (n >= 0) & (n < CHUNKS))
            def _(stage=stage, n=n, is_first=is_first):
                stage(2 * n + jnp.where(is_first, 0, 1))

        c = g // SLOTS - 1
        k = lax.rem(g, SLOTS)
        live = (c >= 0) & (c < CHUNKS)

        @pl.when(live & (k < 2))
        def _():
            attention(c, k)

        @pl.when(live & (k >= 2) & (k < 6))
        def _():
            output(2 * c + (k - 2) // 2, lax.rem(k, 2))

        @pl.when((c == CHUNKS - 1) & (k == 6))
        def _():
            lax.fori_loop(0, LOW * PER, arrivals, 0)
            for copy in fetch_copies():
                copy.start()

        more = c + 1 < CHUNKS

        @pl.when(more & (k == 7))
        def _():
            normalize(c + 1)

        @pl.when(more & (k == 8))
        def _():
            keys_values(c + 1)

        @pl.when(more & (k >= 8))
        def _():
            queries(c + 1, 2 * k - 16, 2 * k - 14)

        return 0

    lax.fori_loop(7, SLOTS * CHUNKS + max(map(max, WHEN.values())) + 1, slot, 0)

    sent(d_copies(U - 1))
    for u in (U - 2, U - 1):
        p1_copy(u).wait_send()
        p2_copy(u).wait_send()
        sent(a_copies(u))
        sent(b_copies(u))
        sent(c_copies(u))

    lax.fori_loop(LOW * PER, U, arrivals, 0)
    for copy in fetch_copies():
        copy.wait()


def _place(z_ref, y_ref, sem):
    n = ROWS // 16
    copies = [pltpu.make_async_copy(z_ref.at[pl.ds(i * n, n), :], y_ref.at[pl.ds(i * n, n), :], sem.at[i]) for i in range(16)]
    for copy in copies:
        copy.start()
    for copy in copies:
        copy.wait()


def _tables():
    half = HEAD // 2
    angle = np.arange(ROWS, dtype=np.float64)[:, None] * np.float64(THETA) ** (-np.arange(half, dtype=np.float64) / half)
    return np.concatenate([np.cos(angle), np.sin(angle)], 1).astype(np.float32)


def solution(mesh):
    def step(x, gain, wq, wk, wv, wo):
        any_ = pl.BlockSpec(memory_space=pl.ANY)
        dma = pltpu.SemaphoreType.DMA
        _, z = pl.pallas_call(
            _kernel,
            name="layer",
            out_shape=[jax.ShapeDtypeStruct((LOW * R, D), BF16), pltpu.VMEM((ROWS, D), BF16)],
            in_specs=[any_, pl.BlockSpec(memory_space=pltpu.VMEM)] + [any_] * 5,
            out_specs=[any_, pl.BlockSpec(memory_space=pltpu.VMEM)],
            scratch_shapes=[
                pltpu.VMEM((1, D), F32),
                pltpu.VMEM((D, 2 * HEAD), BF16), pltpu.VMEM((NO, 1024, W), BF16),
                pltpu.VMEM((R, D), BF16), pltpu.VMEM((ROWS, HEAD), F32),
                pltpu.VMEM((ROWS, HEAD), BF16), pltpu.VMEM((VROWS, ROWS), BF16), pltpu.VMEM((COLS, HEAD), BF16),
                pltpu.VMEM((R, 1024), BF16), pltpu.VMEM((VROWS, COLS), F32), pltpu.VMEM((8, COLS), F32),
                pltpu.VMEM((4, R, W), BF16), pltpu.VMEM((4, R, W), F32), pltpu.VMEM((4, R, W), BF16),
                pltpu.VMEM((2, 2, R, W), BF16), pltpu.VMEM((2, 2, R, W), BF16), pltpu.VMEM((2, 2, R, W), F32),
                pltpu.VMEM((2, R, W), BF16), pltpu.VMEM((2, R, W), BF16), pltpu.VMEM((2, R, W), F32),
                pltpu.VMEM((2, R, W), BF16), pltpu.VMEM((2, R, W), BF16),
                dma((3,)), dma((4, D // 1024)), dma((8,)), dma((NO,)), dma((4,)), dma((2,)), dma((4,)), dma((4,)), dma((2,)), dma((2,)), dma((2,)), dma((2,)),
                dma((4, 2)), dma((2, 2)), dma((2, 2)), dma((U,)), dma((U,)), dma((U,)), dma((4, U)),
                pltpu.SemaphoreType.REGULAR, pltpu.SemaphoreType.REGULAR, pltpu.SemaphoreType.REGULAR,
            ],
            compiler_params=pltpu.CompilerParams(collective_id=0, has_side_effects=True, vmem_limit_bytes=67043328 - ROWS * D * 2),
            cost_estimate=pl.CostEstimate(flops=95_000_000_000, bytes_accessed=200_000_000, transcendentals=20_000_000),
        )(x, gain.reshape(D // 128, 128), wq, wk, wv, wo, jnp.asarray(_tables()))
        return pl.pallas_call(
            _place,
            name="place",
            out_shape=jax.ShapeDtypeStruct((ROWS, D), BF16),
            in_specs=[pl.BlockSpec(memory_space=pltpu.VMEM)],
            out_specs=any_,
            scratch_shapes=[dma((16,))],
            compiler_params=pltpu.CompilerParams(vmem_limit_bytes=2**20),
            cost_estimate=pl.CostEstimate(flops=0, bytes_accessed=42_000_000, transcendentals=0),
        )(z)

    tokens, columns = P("dp", None), P(None, "tp")
    return jax.shard_map(
        step,
        mesh=mesh,
        in_specs=(tokens, P(None), columns, columns, columns, P("tp", None)),
        out_specs=tokens,
        check_vma=False,
    )
```

```python
import functools

import jax
import jax.numpy as jnp
import numpy as np
from jax import lax
from jax.experimental import pallas as pl
from jax.experimental.pallas import tpu as pltpu
from jax.sharding import PartitionSpec as P

MESH = pl.DeviceIdType.MESH
NEG = -1e30
HIDDEN = 2 * NEG
LOG2E = 1.4426950408889634
HEAD = 128
THETA = 10000
ROWS, D = 2048, 8192
R = 256
W = 512
CHUNKS = ROWS // R
PER = 1024 // W
LOW = 4
NO = 6
U = CHUNKS * PER
HEADS = 8
COLS = HEADS * R
STRIP = 512
VROWS = 144
F32, BF16 = jnp.float32, jnp.bfloat16
SLOTS = 10
WHEN = {"reduce_pair": (4, 7), "reduce_f": (9, 10), "reduce_g": (11, 12), "gather_f": (19, 20), "gather_pair": (21, 25)}


def _dot(a, b, ca, cb):
    return lax.dot_general(a, b, (((ca,), (cb,)), ((), ())), preferred_element_type=F32)


def _kernel(x_ref, gain_ref, wq_ref, wk_ref, wv_ref, wo_ref, rope_ref, zh_ref, z_ref,
            gain_s, wkv_s, wo_s, xb, rope_s, k_s, vt_s, q_s, seen_s, mix_s, top_s,
            sbuf, own, rbuf, s1, r1, keep1, s2, r2, keep2, yb, xr,
            w_sem, wq_sem, fetch_sem, wo_sem, x_sem, xr_sem, d_send, d_recv, p1_send, p1_recv, p2_send, p2_recv,
            a_send, b_send, c_send, a1_recv, a2_recv, b1_recv, sib_recv, cred_d, cred_1, cred_2):
    me = lax.axis_index("tp")
    a = lax.rem(me, 2)
    yc = lax.rem(me // 2, 2)
    xc = me // 4
    sib = me + 1 - 2 * a
    xn, yn = me + 4 - 8 * xc, me + 2 - 4 * yc
    fnb, gnb = xn * (1 - a) + yn * a, yn * (1 - a) + xn * a
    fb, gb = xc * (1 - a) + yc * a, yc * (1 - a) + xc * a
    base = a * 4
    o_own, o_g = base + fb * 2 + gb, base + fb * 2 + 1 - gb
    o_f, o_fg = base + (1 - fb) * 2 + gb, base + (1 - fb) * 2 + 1 - gb

    def x_copies(c):
        n = R // 4
        return [pltpu.make_async_copy(x_ref.at[pl.ds(pl.multiple_of(c * R + i * n, n), n), :], xb.at[pl.ds(i * n, n), :], x_sem.at[i]) for i in range(4)]

    def heads_at(n, k):
        return pl.ds(pl.multiple_of(k * 1024 + n * 256, 256), 256)

    def wq_copies(n):
        low = pl.ds(0, LOW * R)
        return [pltpu.make_async_copy(wq_ref.at[pl.ds(k * 1024, 1024), heads_at(n, 0)], z_ref.at[low, heads_at(n, k)], wq_sem.at[n, k]) for k in range(D // 1024)]

    def load(copies):
        for copy in copies:
            copy.start()

    def fetch_copies():
        n = LOW * R // 8
        return [pltpu.make_async_copy(zh_ref.at[pl.ds(i * n, n), :], z_ref.at[pl.ds(i * n, n), :], fetch_sem.at[i]) for i in range(8)]

    wk_copy = pltpu.make_async_copy(wk_ref, wkv_s.at[:, pl.ds(0, HEAD)], w_sem.at[0])
    wv_copy = pltpu.make_async_copy(wv_ref, wkv_s.at[:, pl.ds(HEAD, HEAD)], w_sem.at[1])
    rope_copy = pltpu.make_async_copy(rope_ref, rope_s, w_sem.at[2])

    def columns(owner, s):
        return pl.ds(pl.multiple_of(owner * 1024 + s * W, W), W)

    def wo_copy(m):
        i = lax.rem(m, NO)
        n = lax.rem(m, 8)
        at = columns(jnp.where(n < 4, (1 - a) * 4 + n, a * 4 + n - 4), lax.rem(m // 8, PER))
        return pltpu.make_async_copy(wo_ref.at[:, at], wo_s.at[i], wo_sem.at[i])

    for copy in x_copies(0):
        copy.start()
    barrier = pltpu.get_barrier_semaphore()
    for other in (sib, fnb, gnb):
        pl.semaphore_signal(barrier, inc=1, device_id={"tp": other}, device_id_type=MESH)
    wk_copy.start()
    wv_copy.start()
    load(wq_copies(0))
    gain = gain_ref[...].astype(F32)
    for n in range(D // 128):
        gain_s[:, n * 128 : (n + 1) * 128] = gain[n : n + 1, :]
    vt_s[HEAD:, :] = jnp.ones((VROWS - HEAD, ROWS), BF16)
    pl.semaphore_wait(barrier, 3)
    rope_copy.start()
    load(wq_copies(1))

    def remote(src, dst, send, recv, to):
        return pltpu.make_async_remote_copy(src_ref=src, dst_ref=dst, send_sem=send, recv_sem=recv, device_id={"tp": to}, device_id_type=MESH)

    def rows(u):
        return pl.ds(pl.multiple_of(u // PER * R, R), R)

    def block(u, owner, low):
        at = columns(owner, lax.rem(u, PER))
        if low is None:
            return z_ref.at[pl.ds(LOW * R, R), at]
        return (zh_ref if low else z_ref).at[rows(u), at]

    def d_copy(j):
        return remote(sbuf.at[j], rbuf.at[j], d_send.at[j], d_recv.at[j], sib)

    def d_copies(u):
        return [d_copy(j) for j in range(4)]

    def p1_copy(u):
        i = lax.rem(u, 2)
        return remote(s1.at[i], r1.at[i], p1_send.at[i], p1_recv.at[i], fnb)

    def p2_copy(u):
        i = lax.rem(u, 2)
        return remote(s2.at[i], r2.at[i], p2_send.at[i], p2_recv.at[i], gnb)

    def xr_copy(u):
        i = lax.rem(u, 2)
        return pltpu.make_async_copy(x_ref.at[rows(u), columns(o_own, lax.rem(u, PER))], xr.at[i], xr_sem.at[i])

    def a_copies(u, low=None):
        i = lax.rem(u, 2)
        at = block(u, o_own, low)
        return (remote(yb.at[i], at, a_send.at[0, i], a1_recv.at[u], gnb),
                remote(yb.at[i], at, a_send.at[1, i], a2_recv.at[u], fnb),
                remote(yb.at[i], at, a_send.at[2, i], sib_recv.at[0, u], sib))

    def keep_copy(u):
        i = lax.rem(u, 2)
        return pltpu.make_async_copy(yb.at[i], block(u, o_own, True), a_send.at[3, i])

    def b_copies(u, low=None):
        i = lax.rem(u, 2)
        at = block(u, o_g, low)
        return (remote(at, at, b_send.at[0, i], b1_recv.at[u], fnb),
                remote(at, at, b_send.at[1, i], sib_recv.at[1, u], sib))

    def c_copies(u, low=None):
        i = lax.rem(u, 2)
        at, far = block(u, o_f, low), block(u, o_fg, low)
        return (remote(at, at, c_send.at[0, i], sib_recv.at[2, u], sib),
                remote(far, far, c_send.at[1, i], sib_recv.at[3, u], sib))

    def sent(copies):
        for copy in copies:
            copy.wait_send()

    def start(copies, u):
        @pl.when(u < LOW * PER)
        def _():
            for copy in copies(u, True):
                copy.start()

        @pl.when(u >= LOW * PER)
        def _():
            for copy in copies(u, False):
                copy.start()

    def reduce_pair(u):
        i = lax.rem(u, 2)
        for copy in d_copies(u):
            copy.wait_recv()

        @pl.when(u >= 2)
        def _():
            p1_copy(u - 2).wait_send()

        for j in range(2):
            n = (1 - fb) * 2 + j
            s1[i, j] = (own[n] + rbuf[n].astype(F32)).astype(BF16)

        @pl.when(u >= 2)
        def _():
            pl.semaphore_wait(cred_1, 1)

        p1_copy(u).start()
        for j in range(2):
            n = fb * 2 + j
            keep1[i, j] = own[n] + rbuf[n].astype(F32)

        @pl.when(u + 1 < U)
        def _():
            pl.semaphore_signal(cred_d, inc=1, device_id={"tp": sib}, device_id_type=MESH)

    def reduce_f(u):
        i = lax.rem(u, 2)
        xr_copy(u).start()
        p1_copy(u).wait_recv()

        @pl.when(u >= 2)
        def _():
            p2_copy(u - 2).wait_send()

        s2[i] = (keep1[i, 1 - gb] + r1[i, 1 - gb].astype(F32)).astype(BF16)

        @pl.when(u >= 2)
        def _():
            pl.semaphore_wait(cred_2, 1)

        p2_copy(u).start()
        keep2[i] = keep1[i, gb] + r1[i, gb].astype(F32)

        @pl.when(u + 2 < U)
        def _():
            pl.semaphore_signal(cred_1, inc=1, device_id={"tp": fnb}, device_id_type=MESH)

    def reduce_g(u):
        i = lax.rem(u, 2)
        xr_copy(u).wait()

        @pl.when(u >= 2)
        def _():
            sent(a_copies(u - 2))

        @pl.when((u >= 2) & (u < LOW * PER + 2))
        def _():
            keep_copy(jnp.minimum(u - 2, LOW * PER - 1)).wait()

        p2_copy(u).wait_recv()
        yb[i] = (xr[i].astype(F32) + (keep2[i] + r2[i].astype(F32))).astype(BF16)
        start(a_copies, u)

        @pl.when(u < LOW * PER)
        def _():
            keep_copy(u).start()

        @pl.when(u >= LOW * PER)
        def _():
            z_ref[rows(u), columns(o_own, lax.rem(u, PER))] = yb[i]

        @pl.when(u + 2 < U)
        def _():
            pl.semaphore_signal(cred_2, inc=1, device_id={"tp": gnb}, device_id_type=MESH)

    def gather_f(u):
        @pl.when(u >= 2)
        def _():
            sent(b_copies(u - 2))

        a_copies(u)[0].wait_recv()
        start(b_copies, u)

    def gather_pair(u):
        @pl.when(u >= 2)
        def _():
            sent(c_copies(u - 2))

        a_copies(u)[1].wait_recv()
        b_copies(u)[0].wait_recv()
        start(c_copies, u)

    def turned(t, cosf, sinf):
        t = t.astype(BF16).astype(F32)
        return (t * cosf + pltpu.roll(t, HEAD // 2, 1) * sinf).astype(BF16)

    def normalize(c):
        piece = 1024

        def norm_rows(r, _):
            rows = pl.ds(pl.multiple_of(r * 16, 16), 16)
            total = jnp.zeros((16, piece), F32)
            for n in range(D // piece):
                wide = xb[rows, n * piece : (n + 1) * piece].astype(F32)
                total = total + wide * wide
            scale = lax.rsqrt(jnp.sum(total, -1, keepdims=True) * (1 / D) + 1e-6)
            for n in range(D // piece):
                at = slice(n * piece, (n + 1) * piece)
                xb[rows, at] = (xb[rows, at].astype(F32) * scale * gain_s[:, at]).astype(BF16)
            return 0

        def quarter(i, _):
            n = R // 4
            at = pl.multiple_of(i * n, n)
            pltpu.make_async_copy(x_ref.at[pl.ds(pl.multiple_of(c * R + at, n), n), :], xb.at[pl.ds(at, n), :], x_sem.at[i]).wait()
            lax.fori_loop(i * (n // 16), (i + 1) * (n // 16), norm_rows, 0)
            return 0

        lax.fori_loop(0, 4, quarter, 0)

    def turns(c):
        cs = rope_s[pl.ds(pl.multiple_of(c * R, R), R), :]
        sc = pltpu.roll(cs, HEAD // 2, 1)
        low = lax.broadcasted_iota(jnp.int32, (R, HEAD), 1) < HEAD // 2
        return jnp.where(low, cs, sc), jnp.where(low, -sc, cs)

    def keys_values(c):
        @pl.when(c == 0)
        def _():
            rope_copy.wait()
            wk_copy.wait()
            wv_copy.wait()
            for n in (2, 3):
                load(wq_copies(n))


        here = pl.ds(pl.multiple_of(c * R, R), R)
        kv = _dot(xb[...], wkv_s[...], 1, 0)
        k_s[here, :] = turned(kv[:, :HEAD], *turns(c))
        vt_s[:HEAD, here] = kv[:, HEAD:].T.astype(BF16)

    def queries(c, first, last):
        def tile(n, _):
            @pl.when(c == 0)
            def _():
                for copy in wq_copies(n):
                    copy.wait()

            @pl.when((c == 0) & (n == 1))
            def _():
                for i in range(NO):
                    wo_copy(i).start()

            q = 0
            for k in range(D // 1024):
                q += _dot(xb[:, k * 1024 : (k + 1) * 1024], z_ref[pl.ds(0, LOW * R), heads_at(n, k)], 1, 0)
            cosf, sinf = turns(c)
            for h in range(2):
                q_s[pl.ds(pl.multiple_of((2 * n + h) * R, R), R), :] = turned(q[:, h * HEAD : (h + 1) * HEAD], cosf, sinf)
            return 0

        lax.fori_loop(first, last, tile, 0)

        @pl.when((last == 4) & (c + 1 < CHUNKS))
        def _():
            for copy in x_copies(c + 1):
                copy.start()

    def attention(c, part):
        e = HEAD**-0.5 * LOG2E
        pieces = range(0, COLS, STRIP)

        def keys(j, masked):
            here = pl.ds(pl.multiple_of(j * R, R), R)
            scores = [_dot(k_s[here, :], q_s[at : at + STRIP, :], 1, 1) for at in pieces]
            if masked:
                ok = lax.rem(lax.broadcasted_iota(jnp.int32, (R, STRIP), 1), R) >= lax.broadcasted_iota(jnp.int32, (R, STRIP), 0)
            weights, keeps = [], []
            for at, s in zip(pieces, scores):
                if masked:
                    s = jnp.where(ok, s, HIDDEN)
                old = top_s[0:1, at : at + STRIP]
                top = jnp.maximum(old, s.max(axis=0, keepdims=True))
                top_s[0:1, at : at + STRIP] = top
                weights.append(jnp.exp2((s - top) * e).astype(BF16))
                keeps.append(jnp.exp2((old - top) * e))
            for at, p, keep in zip(pieces, weights, keeps):
                mix_s[:, at : at + STRIP] = mix_s[:, at : at + STRIP] * keep + _dot(vt_s[:, here], p, 1, 0)

        def whole(j, _):
            keys(j, False)
            return 0

        @pl.when(part == 0)
        def _():
            top_s[...] = jnp.full((8, COLS), NEG, F32)
            mix_s[...] = jnp.zeros((VROWS, COLS), F32)

        lax.fori_loop(jnp.where(part == 0, 0, c // 2), jnp.where(part == 0, c // 2, c), whole, 0)

        @pl.when(part == 1)
        def _():
            keys(c, True)
            for h in range(HEADS):
                at = slice(h * R, (h + 1) * R)
                seen_s[:, h * HEAD : (h + 1) * HEAD] = (mix_s[:HEAD, at] * (1 / mix_s[HEAD : HEAD + 1, at])).T.astype(BF16)

    def tile(u, n):
        m = 8 * u + n
        wo_copy(m).wait()
        term = _dot(seen_s[...], wo_s[lax.rem(m, NO)], 1, 0)

        @pl.when(m + NO < 8 * U)
        def _():
            wo_copy(m + NO).start()

        return term

    def output_theirs(u):
        @pl.when(u >= 1)
        def _():
            sent(d_copies(u - 1))
            pl.semaphore_wait(cred_d, 1)

        def theirs(j, _):
            sbuf[j] = tile(u, j).astype(BF16)
            d_copy(j).start()
            return 0

        lax.fori_loop(0, 4, theirs, 0)

    def output_ours(u):
        def ours(j, _):
            own[j] = tile(u, 4 + j)
            return 0

        lax.fori_loop(0, 4, ours, 0)

    def arrivals(u, _):
        a_copies(u)[2].wait_recv()
        b_copies(u)[1].wait_recv()
        for copy in c_copies(u):
            copy.wait_recv()
        return 0

    def slot(g, _):
        for stage in (reduce_pair, reduce_f, reduce_g, gather_f, gather_pair):
            first, second = (g + 99 * SLOTS - at for at in WHEN[stage.__name__])
            is_first = lax.rem(first, SLOTS) == 0
            n = jnp.where(is_first, first, second) // SLOTS - 100

            @pl.when((is_first | (lax.rem(second, SLOTS) == 0)) & (n >= 0) & (n < CHUNKS))
            def _(stage=stage, n=n, is_first=is_first):
                stage(2 * n + jnp.where(is_first, 0, 1))

        c = g // SLOTS - 1
        k = lax.rem(g, SLOTS)
        live = (c >= 0) & (c < CHUNKS)

        @pl.when(live & (k < 2))
        def _():
            attention(c, k)

        @pl.when(live & ((k == 2) | (k == 4)))
        def _():
            output_theirs(2 * c + k // 4)

        @pl.when(live & ((k == 3) | (k == 5)))
        def _():
            output_ours(2 * c + k // 4)

        @pl.when((c == CHUNKS - 1) & (k == 6))
        def _():
            lax.fori_loop(0, LOW * PER, arrivals, 0)
            for copy in fetch_copies():
                copy.start()

        more = c + 1 < CHUNKS

        @pl.when(more & (k == 7))
        def _():
            normalize(c + 1)

        @pl.when(more & (k == 8))
        def _():
            keys_values(c + 1)

        @pl.when(more & (k >= 8))
        def _():
            queries(c + 1, 2 * k - 16, 2 * k - 14)

        return 0

    lax.fori_loop(7, SLOTS * CHUNKS + max(map(max, WHEN.values())) + 1, slot, 0)

    sent(d_copies(U - 1))
    for u in (U - 2, U - 1):
        p1_copy(u).wait_send()
        p2_copy(u).wait_send()
        sent(a_copies(u))
        sent(b_copies(u))
        sent(c_copies(u))

    lax.fori_loop(LOW * PER, U, arrivals, 0)
    for copy in fetch_copies():
        copy.wait()


def _place(z_ref, y_ref, sem):
    n = ROWS // 16
    copies = [pltpu.make_async_copy(z_ref.at[pl.ds(i * n, n), :], y_ref.at[pl.ds(i * n, n), :], sem.at[i]) for i in range(16)]
    for copy in copies:
        copy.start()
    for copy in copies:
        copy.wait()


def _tables():
    half = HEAD // 2
    angle = np.arange(ROWS, dtype=np.float64)[:, None] * np.float64(THETA) ** (-np.arange(half, dtype=np.float64) / half)
    return np.concatenate([np.cos(angle), np.sin(angle)], 1).astype(np.float32)


def solution(mesh):
    def step(x, gain, wq, wk, wv, wo):
        any_ = pl.BlockSpec(memory_space=pl.ANY)
        dma = pltpu.SemaphoreType.DMA
        _, z = pl.pallas_call(
            _kernel,
            name="layer",
            out_shape=[jax.ShapeDtypeStruct((LOW * R, D), BF16), pltpu.VMEM((ROWS, D), BF16)],
            in_specs=[any_, pl.BlockSpec(memory_space=pltpu.VMEM)] + [any_] * 5,
            out_specs=[any_, pl.BlockSpec(memory_space=pltpu.VMEM)],
            scratch_shapes=[
                pltpu.VMEM((1, D), F32),
                pltpu.VMEM((D, 2 * HEAD), BF16), pltpu.VMEM((NO, 1024, W), BF16),
                pltpu.VMEM((R, D), BF16), pltpu.VMEM((ROWS, HEAD), F32),
                pltpu.VMEM((ROWS, HEAD), BF16), pltpu.VMEM((VROWS, ROWS), BF16), pltpu.VMEM((COLS, HEAD), BF16),
                pltpu.VMEM((R, 1024), BF16), pltpu.VMEM((VROWS, COLS), F32), pltpu.VMEM((8, COLS), F32),
                pltpu.VMEM((4, R, W), BF16), pltpu.VMEM((4, R, W), F32), pltpu.VMEM((4, R, W), BF16),
                pltpu.VMEM((2, 2, R, W), BF16), pltpu.VMEM((2, 2, R, W), BF16), pltpu.VMEM((2, 2, R, W), F32),
                pltpu.VMEM((2, R, W), BF16), pltpu.VMEM((2, R, W), BF16), pltpu.VMEM((2, R, W), F32),
                pltpu.VMEM((2, R, W), BF16), pltpu.VMEM((2, R, W), BF16),
                dma((3,)), dma((4, D // 1024)), dma((8,)), dma((NO,)), dma((4,)), dma((2,)), dma((4,)), dma((4,)), dma((2,)), dma((2,)), dma((2,)), dma((2,)),
                dma((4, 2)), dma((2, 2)), dma((2, 2)), dma((U,)), dma((U,)), dma((U,)), dma((4, U)),
                pltpu.SemaphoreType.REGULAR, pltpu.SemaphoreType.REGULAR, pltpu.SemaphoreType.REGULAR,
            ],
            compiler_params=pltpu.CompilerParams(collective_id=0, has_side_effects=True, vmem_limit_bytes=67043328 - ROWS * D * 2),
            cost_estimate=pl.CostEstimate(flops=95_000_000_000, bytes_accessed=200_000_000, transcendentals=20_000_000),
        )(x, gain.reshape(D // 128, 128), wq, wk, wv, wo, jnp.asarray(_tables()))
        return pl.pallas_call(
            _place,
            name="place",
            out_shape=jax.ShapeDtypeStruct((ROWS, D), BF16),
            in_specs=[pl.BlockSpec(memory_space=pltpu.VMEM)],
            out_specs=any_,
            scratch_shapes=[dma((16,))],
            compiler_params=pltpu.CompilerParams(vmem_limit_bytes=2**20),
            cost_estimate=pl.CostEstimate(flops=0, bytes_accessed=42_000_000, transcendentals=0),
        )(z)

    tokens, columns = P("dp", None), P(None, "tp")
    return jax.shard_map(
        step,
        mesh=mesh,
        in_specs=(tokens, P(None), columns, columns, columns, P("tp", None)),
        out_specs=tokens,
        check_vma=False,
    )
```

```python
import functools

import jax
import jax.numpy as jnp
import numpy as np
from jax import lax
from jax.experimental import pallas as pl
from jax.experimental.pallas import tpu as pltpu
from jax.sharding import PartitionSpec as P

MESH = pl.DeviceIdType.MESH
NEG = -1e30
HIDDEN = 2 * NEG
LOG2E = 1.4426950408889634
HEAD = 128
THETA = 10000
ROWS, D = 2048, 8192
R = 256
W = 512
CHUNKS = ROWS // R
PER = 1024 // W
LOW = 4
NO = 6
U = CHUNKS * PER
HEADS = 8
COLS = HEADS * R
STRIP = 512
VROWS = 144
F32, BF16 = jnp.float32, jnp.bfloat16
SLOTS = 10
WHEN = {"reduce_pair": (4, 7), "reduce_f": (9, 10), "reduce_g": (11, 12), "gather_f": (19, 20), "gather_pair": (21, 25)}


def _dot(a, b, ca, cb):
    return lax.dot_general(a, b, (((ca,), (cb,)), ((), ())), preferred_element_type=F32)


def _kernel(x_ref, gain_ref, wq_ref, wk_ref, wv_ref, wo_ref, rope_ref, zh_ref, z_ref,
            gain_s, wkv_s, wo_s, xb, rope_s, k_s, vt_s, q_s, seen_s, mix_s, top_s,
            sbuf, own, rbuf, s1, r1, keep1, s2, r2, keep2, yb, xr,
            w_sem, wq_sem, fetch_sem, wo_sem, x_sem, xr_sem, d_send, d_recv, p1_send, p1_recv, p2_send, p2_recv,
            a_send, b_send, c_send, a1_recv, a2_recv, b1_recv, sib_recv, cred_d, cred_1, cred_2):
    me = lax.axis_index("tp")
    a = lax.rem(me, 2)
    yc = lax.rem(me // 2, 2)
    xc = me // 4
    sib = me + 1 - 2 * a
    xn, yn = me + 4 - 8 * xc, me + 2 - 4 * yc
    fnb, gnb = xn * (1 - a) + yn * a, yn * (1 - a) + xn * a
    fb, gb = xc * (1 - a) + yc * a, yc * (1 - a) + xc * a
    base = a * 4
    o_own, o_g = base + fb * 2 + gb, base + fb * 2 + 1 - gb
    o_f, o_fg = base + (1 - fb) * 2 + gb, base + (1 - fb) * 2 + 1 - gb

    def x_copies(c):
        n = R // 4
        return [pltpu.make_async_copy(x_ref.at[pl.ds(pl.multiple_of(c * R + i * n, n), n), :], xb.at[pl.ds(i * n, n), :], x_sem.at[i]) for i in range(4)]

    def heads_at(n, k):
        return pl.ds(pl.multiple_of(k * 1024 + n * 256, 256), 256)

    def wq_copies(n):
        low = pl.ds(0, LOW * R)
        return [pltpu.make_async_copy(wq_ref.at[pl.ds(k * 1024, 1024), heads_at(n, 0)], z_ref.at[low, heads_at(n, k)], wq_sem.at[n, k]) for k in range(D // 1024)]

    def load(copies):
        for copy in copies:
            copy.start()

    def fetch_copies():
        n = LOW * R // 8
        return [pltpu.make_async_copy(zh_ref.at[pl.ds(i * n, n), :], z_ref.at[pl.ds(i * n, n), :], fetch_sem.at[i]) for i in range(8)]

    wk_copy = pltpu.make_async_copy(wk_ref, wkv_s.at[:, pl.ds(0, HEAD)], w_sem.at[0])
    wv_copy = pltpu.make_async_copy(wv_ref, wkv_s.at[:, pl.ds(HEAD, HEAD)], w_sem.at[1])
    rope_copy = pltpu.make_async_copy(rope_ref, rope_s, w_sem.at[2])

    def columns(owner, s):
        return pl.ds(pl.multiple_of(owner * 1024 + s * W, W), W)

    def wo_copy(m):
        i = lax.rem(m, NO)
        n = lax.rem(m, 8)
        at = columns(jnp.where(n < 4, (1 - a) * 4 + n, a * 4 + n - 4), lax.rem(m // 8, PER))
        return pltpu.make_async_copy(wo_ref.at[:, at], wo_s.at[i], wo_sem.at[i])

    for copy in x_copies(0):
        copy.start()
    barrier = pltpu.get_barrier_semaphore()
    for other in (sib, fnb, gnb):
        pl.semaphore_signal(barrier, inc=1, device_id={"tp": other}, device_id_type=MESH)
    gain = gain_ref[...].astype(F32)
    for n in range(D // 128):
        gain_s[:, n * 128 : (n + 1) * 128] = gain[n : n + 1, :]
    vt_s[HEAD:, :] = jnp.ones((VROWS - HEAD, ROWS), BF16)
    pl.semaphore_wait(barrier, 3)

    def remote(src, dst, send, recv, to):
        return pltpu.make_async_remote_copy(src_ref=src, dst_ref=dst, send_sem=send, recv_sem=recv, device_id={"tp": to}, device_id_type=MESH)

    def rows(u):
        return pl.ds(pl.multiple_of(u // PER * R, R), R)

    def block(u, owner, low):
        at = columns(owner, lax.rem(u, PER))
        if low is None:
            return z_ref.at[pl.ds(LOW * R, R), at]
        return (zh_ref if low else z_ref).at[rows(u), at]

    def d_copy(j):
        return remote(sbuf.at[j], rbuf.at[j], d_send.at[j], d_recv.at[j], sib)

    def d_copies(u):
        return [d_copy(j) for j in range(4)]

    def p1_copy(u):
        i = lax.rem(u, 2)
        return remote(s1.at[i], r1.at[i], p1_send.at[i], p1_recv.at[i], fnb)

    def p2_copy(u):
        i = lax.rem(u, 2)
        return remote(s2.at[i], r2.at[i], p2_send.at[i], p2_recv.at[i], gnb)

    def xr_copy(u):
        i = lax.rem(u, 2)
        return pltpu.make_async_copy(x_ref.at[rows(u), columns(o_own, lax.rem(u, PER))], xr.at[i], xr_sem.at[i])

    def a_copies(u, low=None):
        i = lax.rem(u, 2)
        at = block(u, o_own, low)
        return (remote(yb.at[i], at, a_send.at[0, i], a1_recv.at[u], gnb),
                remote(yb.at[i], at, a_send.at[1, i], a2_recv.at[u], fnb),
                remote(yb.at[i], at, a_send.at[2, i], sib_recv.at[0, u], sib))

    def keep_copy(u):
        i = lax.rem(u, 2)
        return pltpu.make_async_copy(yb.at[i], block(u, o_own, True), a_send.at[3, i])

    def b_copies(u, low=None):
        i = lax.rem(u, 2)
        at = block(u, o_g, low)
        return (remote(at, at, b_send.at[0, i], b1_recv.at[u], fnb),
                remote(at, at, b_send.at[1, i], sib_recv.at[1, u], sib))

    def c_copies(u, low=None):
        i = lax.rem(u, 2)
        at, far = block(u, o_f, low), block(u, o_fg, low)
        return (remote(at, at, c_send.at[0, i], sib_recv.at[2, u], sib),
                remote(far, far, c_send.at[1, i], sib_recv.at[3, u], sib))

    def sent(copies):
        for copy in copies:
            copy.wait_send()

    def start(copies, u):
        @pl.when(u < LOW * PER)
        def _():
            for copy in copies(u, True):
                copy.start()

        @pl.when(u >= LOW * PER)
        def _():
            for copy in copies(u, False):
                copy.start()

    def reduce_pair(u):
        i = lax.rem(u, 2)
        for copy in d_copies(u):
            copy.wait_recv()

        @pl.when(u >= 2)
        def _():
            p1_copy(u - 2).wait_send()

        for j in range(2):
            n = (1 - fb) * 2 + j
            s1[i, j] = (own[n] + rbuf[n].astype(F32)).astype(BF16)

        @pl.when(u >= 2)
        def _():
            pl.semaphore_wait(cred_1, 1)

        p1_copy(u).start()
        for j in range(2):
            n = fb * 2 + j
            keep1[i, j] = own[n] + rbuf[n].astype(F32)

        @pl.when(u + 1 < U)
        def _():
            pl.semaphore_signal(cred_d, inc=1, device_id={"tp": sib}, device_id_type=MESH)

    def reduce_f(u):
        i = lax.rem(u, 2)
        xr_copy(u).start()
        p1_copy(u).wait_recv()

        @pl.when(u >= 2)
        def _():
            p2_copy(u - 2).wait_send()

        s2[i] = (keep1[i, 1 - gb] + r1[i, 1 - gb].astype(F32)).astype(BF16)

        @pl.when(u >= 2)
        def _():
            pl.semaphore_wait(cred_2, 1)

        p2_copy(u).start()
        keep2[i] = keep1[i, gb] + r1[i, gb].astype(F32)

        @pl.when(u + 2 < U)
        def _():
            pl.semaphore_signal(cred_1, inc=1, device_id={"tp": fnb}, device_id_type=MESH)

    def reduce_g(u):
        i = lax.rem(u, 2)
        xr_copy(u).wait()

        @pl.when(u >= 2)
        def _():
            sent(a_copies(u - 2))

        @pl.when((u >= 2) & (u < LOW * PER + 2))
        def _():
            keep_copy(jnp.minimum(u - 2, LOW * PER - 1)).wait()

        p2_copy(u).wait_recv()
        yb[i] = (xr[i].astype(F32) + (keep2[i] + r2[i].astype(F32))).astype(BF16)
        start(a_copies, u)

        @pl.when(u < LOW * PER)
        def _():
            keep_copy(u).start()

        @pl.when(u >= LOW * PER)
        def _():
            z_ref[rows(u), columns(o_own, lax.rem(u, PER))] = yb[i]

        @pl.when(u + 2 < U)
        def _():
            pl.semaphore_signal(cred_2, inc=1, device_id={"tp": gnb}, device_id_type=MESH)

    def gather_f(u):
        @pl.when(u >= 2)
        def _():
            sent(b_copies(u - 2))

        a_copies(u)[0].wait_recv()
        start(b_copies, u)

    def gather_pair(u):
        @pl.when(u >= 2)
        def _():
            sent(c_copies(u - 2))

        a_copies(u)[1].wait_recv()
        b_copies(u)[0].wait_recv()
        start(c_copies, u)

    def turned(t, cosf, sinf):
        t = t.astype(BF16).astype(F32)
        return (t * cosf + pltpu.roll(t, HEAD // 2, 1) * sinf).astype(BF16)

    def normalize(c):
        piece = 1024

        def norm_rows(r, _):
            rows = pl.ds(pl.multiple_of(r * 16, 16), 16)
            total = jnp.zeros((16, piece), F32)
            for n in range(D // piece):
                wide = xb[rows, n * piece : (n + 1) * piece].astype(F32)
                total = total + wide * wide
            scale = lax.rsqrt(jnp.sum(total, -1, keepdims=True) * (1 / D) + 1e-6)
            for n in range(D // piece):
                at = slice(n * piece, (n + 1) * piece)
                xb[rows, at] = (xb[rows, at].astype(F32) * scale * gain_s[:, at]).astype(BF16)
            return 0

        def quarter(i, _):
            n = R // 4
            at = pl.multiple_of(i * n, n)
            pltpu.make_async_copy(x_ref.at[pl.ds(pl.multiple_of(c * R + at, n), n), :], xb.at[pl.ds(at, n), :], x_sem.at[i]).wait()

            @pl.when((c == 0) & (i == 0))
            def _():
                load([wk_copy, wv_copy, rope_copy])
                load(wq_copies(0))

            @pl.when((c == 0) & (i == 3))
            def _():
                load(wq_copies(1))

            lax.fori_loop(i * (n // 16), (i + 1) * (n // 16), norm_rows, 0)
            return 0

        lax.fori_loop(0, 4, quarter, 0)

    def turns(c):
        cs = rope_s[pl.ds(pl.multiple_of(c * R, R), R), :]
        sc = pltpu.roll(cs, HEAD // 2, 1)
        low = lax.broadcasted_iota(jnp.int32, (R, HEAD), 1) < HEAD // 2
        return jnp.where(low, cs, sc), jnp.where(low, -sc, cs)

    def keys_values(c):
        @pl.when(c == 0)
        def _():
            rope_copy.wait()
            wk_copy.wait()
            wv_copy.wait()
            for n in (2, 3):
                load(wq_copies(n))


        here = pl.ds(pl.multiple_of(c * R, R), R)
        kv = _dot(xb[...], wkv_s[...], 1, 0)
        k_s[here, :] = turned(kv[:, :HEAD], *turns(c))
        vt_s[:HEAD, here] = kv[:, HEAD:].T.astype(BF16)

    def queries(c, first, last):
        def tile(n, _):
            @pl.when(c == 0)
            def _():
                for copy in wq_copies(n):
                    copy.wait()

            @pl.when((c == 0) & (n == 1))
            def _():
                for i in range(NO):
                    wo_copy(i).start()

            q = 0
            for k in range(D // 1024):
                q += _dot(xb[:, k * 1024 : (k + 1) * 1024], z_ref[pl.ds(0, LOW * R), heads_at(n, k)], 1, 0)
            cosf, sinf = turns(c)
            for h in range(2):
                q_s[pl.ds(pl.multiple_of((2 * n + h) * R, R), R), :] = turned(q[:, h * HEAD : (h + 1) * HEAD], cosf, sinf)
            return 0

        lax.fori_loop(first, last, tile, 0)

        @pl.when((last == 4) & (c + 1 < CHUNKS))
        def _():
            for copy in x_copies(c + 1):
                copy.start()

    def attention(c, part):
        e = HEAD**-0.5 * LOG2E
        pieces = range(0, COLS, STRIP)

        def keys(j, masked):
            here = pl.ds(pl.multiple_of(j * R, R), R)
            scores = [_dot(k_s[here, :], q_s[at : at + STRIP, :], 1, 1) for at in pieces]
            if masked:
                ok = lax.rem(lax.broadcasted_iota(jnp.int32, (R, STRIP), 1), R) >= lax.broadcasted_iota(jnp.int32, (R, STRIP), 0)
            weights, keeps = [], []
            for at, s in zip(pieces, scores):
                if masked:
                    s = jnp.where(ok, s, HIDDEN)
                old = top_s[0:1, at : at + STRIP]
                top = jnp.maximum(old, s.max(axis=0, keepdims=True))
                top_s[0:1, at : at + STRIP] = top
                weights.append(jnp.exp2((s - top) * e).astype(BF16))
                keeps.append(jnp.exp2((old - top) * e))
            for at, p, keep in zip(pieces, weights, keeps):
                mix_s[:, at : at + STRIP] = mix_s[:, at : at + STRIP] * keep + _dot(vt_s[:, here], p, 1, 0)

        def whole(j, _):
            keys(j, False)
            return 0

        @pl.when(part == 0)
        def _():
            top_s[...] = jnp.full((8, COLS), NEG, F32)
            mix_s[...] = jnp.zeros((VROWS, COLS), F32)

        lax.fori_loop(jnp.where(part == 0, 0, c // 2), jnp.where(part == 0, c // 2, c), whole, 0)

        @pl.when(part == 1)
        def _():
            keys(c, True)
            for h in range(HEADS):
                at = slice(h * R, (h + 1) * R)
                seen_s[:, h * HEAD : (h + 1) * HEAD] = (mix_s[:HEAD, at] * (1 / mix_s[HEAD : HEAD + 1, at])).T.astype(BF16)

    def tile(u, n):
        m = 8 * u + n
        wo_copy(m).wait()
        term = _dot(seen_s[...], wo_s[lax.rem(m, NO)], 1, 0)

        @pl.when(m + NO < 8 * U)
        def _():
            wo_copy(m + NO).start()

        return term

    def output_theirs(u):
        @pl.when(u >= 1)
        def _():
            sent(d_copies(u - 1))
            pl.semaphore_wait(cred_d, 1)

        def theirs(j, _):
            sbuf[j] = tile(u, j).astype(BF16)
            d_copy(j).start()
            return 0

        lax.fori_loop(0, 4, theirs, 0)

    def output_ours(u):
        def ours(j, _):
            own[j] = tile(u, 4 + j)
            return 0

        lax.fori_loop(0, 4, ours, 0)

    def arrivals(u, _):
        a_copies(u)[2].wait_recv()
        b_copies(u)[1].wait_recv()
        for copy in c_copies(u):
            copy.wait_recv()
        return 0

    def slot(g, _):
        for stage in (reduce_pair, reduce_f, reduce_g, gather_f, gather_pair):
            first, second = (g + 99 * SLOTS - at for at in WHEN[stage.__name__])
            is_first = lax.rem(first, SLOTS) == 0
            n = jnp.where(is_first, first, second) // SLOTS - 100

            @pl.when((is_first | (lax.rem(second, SLOTS) == 0)) & (n >= 0) & (n < CHUNKS))
            def _(stage=stage, n=n, is_first=is_first):
                stage(2 * n + jnp.where(is_first, 0, 1))

        c = g // SLOTS - 1
        k = lax.rem(g, SLOTS)
        live = (c >= 0) & (c < CHUNKS)

        @pl.when(live & (k < 2))
        def _():
            attention(c, k)

        @pl.when(live & ((k == 2) | (k == 4)))
        def _():
            output_theirs(2 * c + k // 4)

        @pl.when(live & ((k == 3) | (k == 5)))
        def _():
            output_ours(2 * c + k // 4)

        @pl.when((c == CHUNKS - 1) & (k == 6))
        def _():
            lax.fori_loop(0, LOW * PER, arrivals, 0)
            for copy in fetch_copies():
                copy.start()

        more = c + 1 < CHUNKS

        @pl.when(more & (k == 7))
        def _():
            normalize(c + 1)

        @pl.when(more & (k == 8))
        def _():
            keys_values(c + 1)

        @pl.when(more & (k >= 8))
        def _():
            queries(c + 1, 2 * k - 16, 2 * k - 14)

        return 0

    lax.fori_loop(7, SLOTS * CHUNKS + max(map(max, WHEN.values())) + 1, slot, 0)

    sent(d_copies(U - 1))
    for u in (U - 2, U - 1):
        p1_copy(u).wait_send()
        p2_copy(u).wait_send()
        sent(a_copies(u))
        sent(b_copies(u))
        sent(c_copies(u))

    lax.fori_loop(LOW * PER, U, arrivals, 0)
    for copy in fetch_copies():
        copy.wait()


def _place(z_ref, y_ref, sem):
    n = ROWS // 16
    copies = [pltpu.make_async_copy(z_ref.at[pl.ds(i * n, n), :], y_ref.at[pl.ds(i * n, n), :], sem.at[i]) for i in range(16)]
    for copy in copies:
        copy.start()
    for copy in copies:
        copy.wait()


def _tables():
    half = HEAD // 2
    angle = np.arange(ROWS, dtype=np.float64)[:, None] * np.float64(THETA) ** (-np.arange(half, dtype=np.float64) / half)
    return np.concatenate([np.cos(angle), np.sin(angle)], 1).astype(np.float32)


def solution(mesh):
    def step(x, gain, wq, wk, wv, wo):
        any_ = pl.BlockSpec(memory_space=pl.ANY)
        dma = pltpu.SemaphoreType.DMA
        _, z = pl.pallas_call(
            _kernel,
            name="layer",
            out_shape=[jax.ShapeDtypeStruct((LOW * R, D), BF16), pltpu.VMEM((ROWS, D), BF16)],
            in_specs=[any_, pl.BlockSpec(memory_space=pltpu.VMEM)] + [any_] * 5,
            out_specs=[any_, pl.BlockSpec(memory_space=pltpu.VMEM)],
            scratch_shapes=[
                pltpu.VMEM((1, D), F32),
                pltpu.VMEM((D, 2 * HEAD), BF16), pltpu.VMEM((NO, 1024, W), BF16),
                pltpu.VMEM((R, D), BF16), pltpu.VMEM((ROWS, HEAD), F32),
                pltpu.VMEM((ROWS, HEAD), BF16), pltpu.VMEM((VROWS, ROWS), BF16), pltpu.VMEM((COLS, HEAD), BF16),
                pltpu.VMEM((R, 1024), BF16), pltpu.VMEM((VROWS, COLS), F32), pltpu.VMEM((8, COLS), F32),
                pltpu.VMEM((4, R, W), BF16), pltpu.VMEM((4, R, W), F32), pltpu.VMEM((4, R, W), BF16),
                pltpu.VMEM((2, 2, R, W), BF16), pltpu.VMEM((2, 2, R, W), BF16), pltpu.VMEM((2, 2, R, W), F32),
                pltpu.VMEM((2, R, W), BF16), pltpu.VMEM((2, R, W), BF16), pltpu.VMEM((2, R, W), F32),
                pltpu.VMEM((2, R, W), BF16), pltpu.VMEM((2, R, W), BF16),
                dma((3,)), dma((4, D // 1024)), dma((8,)), dma((NO,)), dma((4,)), dma((2,)), dma((4,)), dma((4,)), dma((2,)), dma((2,)), dma((2,)), dma((2,)),
                dma((4, 2)), dma((2, 2)), dma((2, 2)), dma((U,)), dma((U,)), dma((U,)), dma((4, U)),
                pltpu.SemaphoreType.REGULAR, pltpu.SemaphoreType.REGULAR, pltpu.SemaphoreType.REGULAR,
            ],
            compiler_params=pltpu.CompilerParams(collective_id=0, has_side_effects=True, vmem_limit_bytes=67043328 - ROWS * D * 2),
            cost_estimate=pl.CostEstimate(flops=95_000_000_000, bytes_accessed=200_000_000, transcendentals=20_000_000),
        )(x, gain.reshape(D // 128, 128), wq, wk, wv, wo, jnp.asarray(_tables()))
        return pl.pallas_call(
            _place,
            name="place",
            out_shape=jax.ShapeDtypeStruct((ROWS, D), BF16),
            in_specs=[pl.BlockSpec(memory_space=pltpu.VMEM)],
            out_specs=any_,
            scratch_shapes=[dma((16,))],
            compiler_params=pltpu.CompilerParams(vmem_limit_bytes=2**20),
            cost_estimate=pl.CostEstimate(flops=0, bytes_accessed=42_000_000, transcendentals=0),
        )(z)

    tokens, columns = P("dp", None), P(None, "tp")
    return jax.shard_map(
        step,
        mesh=mesh,
        in_specs=(tokens, P(None), columns, columns, columns, P("tp", None)),
        out_specs=tokens,
        check_vma=False,
    )
```

```python
import functools

import jax
import jax.numpy as jnp
import numpy as np
from jax import lax
from jax.experimental import pallas as pl
from jax.experimental.pallas import tpu as pltpu
from jax.sharding import PartitionSpec as P

MESH = pl.DeviceIdType.MESH
NEG = -1e30
HIDDEN = 2 * NEG
LOG2E = 1.4426950408889634
HEAD = 128
THETA = 10000
ROWS, D = 2048, 8192
R = 256
W = 512
CHUNKS = ROWS // R
PER = 1024 // W
LOW = 4
NO = 6
U = CHUNKS * PER
HEADS = 8
COLS = HEADS * R
STRIP = 512
VROWS = 144
F32, BF16 = jnp.float32, jnp.bfloat16
SLOTS = 10
WHEN = {"reduce_pair": (4, 7), "reduce_f": (10, 11), "reduce_g": (12, 13), "gather_f": (19, 22), "gather_pair": (27, 29)}


def _dot(a, b, ca, cb):
    return lax.dot_general(a, b, (((ca,), (cb,)), ((), ())), preferred_element_type=F32)


def _kernel(x_ref, gain_ref, wq_ref, wk_ref, wv_ref, wo_ref, rope_ref, zh_ref, z_ref,
            gain_s, wkv_s, wo_s, xb, rope_s, k_s, vt_s, q_s, seen_s, mix_s, top_s,
            sbuf, own, rbuf, s1, r1, keep1, s2, r2, keep2, yb, xr,
            w_sem, wq_sem, fetch_sem, wo_sem, x_sem, xr_sem, d_send, d_recv, p1_send, p1_recv, p2_send, p2_recv,
            a_send, keep_sem, b_send, c_send, a_recv, b_recv, c_recv, cred_d, cred_1, cred_2):
    me = lax.axis_index("tp")
    a = lax.rem(me, 2)
    yc = lax.rem(me // 2, 2)
    xc = me // 4
    sib = me + 1 - 2 * a
    xn, yn = me + 4 - 8 * xc, me + 2 - 4 * yc
    fnb, gnb = xn * (1 - a) + yn * a, yn * (1 - a) + xn * a
    fb, gb = xc * (1 - a) + yc * a, yc * (1 - a) + xc * a
    base = a * 4
    o_own = base + fb * 2 + gb

    def x_copies(c):
        n = R // 4
        return [pltpu.make_async_copy(x_ref.at[pl.ds(pl.multiple_of(c * R + i * n, n), n), :], xb.at[pl.ds(i * n, n), :], x_sem.at[i]) for i in range(4)]

    def heads_at(n, k):
        return pl.ds(pl.multiple_of(k * 1024 + n * 256, 256), 256)

    def wq_copies(n):
        low = pl.ds(0, LOW * R)
        return [pltpu.make_async_copy(wq_ref.at[pl.ds(k * 1024, 1024), heads_at(n, 0)], z_ref.at[low, heads_at(n, k)], wq_sem.at[n, k]) for k in range(D // 1024)]

    def load(copies):
        for copy in copies:
            copy.start()

    def fetch_copies():
        n = LOW * R // 8
        return [pltpu.make_async_copy(zh_ref.at[pl.ds(i * n, n), :], z_ref.at[pl.ds(i * n, n), :], fetch_sem.at[i]) for i in range(8)]

    wk_copy = pltpu.make_async_copy(wk_ref, wkv_s.at[:, pl.ds(0, HEAD)], w_sem.at[0])
    wv_copy = pltpu.make_async_copy(wv_ref, wkv_s.at[:, pl.ds(HEAD, HEAD)], w_sem.at[1])
    rope_copy = pltpu.make_async_copy(rope_ref, rope_s, w_sem.at[2])

    def columns(owner, s, n=1):
        return pl.ds(pl.multiple_of(s * (8 * W) + owner * W, W), n * W)

    def wo_copy(m):
        i = lax.rem(m, NO)
        n = lax.rem(m, 8)
        at = columns(jnp.where(n < 4, (1 - a) * 4 + n, a * 4 + n - 4), lax.rem(m // 8, PER))
        return pltpu.make_async_copy(wo_ref.at[:, at], wo_s.at[i], wo_sem.at[i])

    for copy in x_copies(0):
        copy.start()
    barrier = pltpu.get_barrier_semaphore()
    for other in (sib, fnb, gnb):
        pl.semaphore_signal(barrier, inc=1, device_id={"tp": other}, device_id_type=MESH)
    gain = gain_ref[...].astype(F32)
    for n in range(D // 128):
        gain_s[:, n * 128 : (n + 1) * 128] = gain[n : n + 1, :]
    vt_s[HEAD:, :] = jnp.ones((VROWS - HEAD, ROWS), BF16)
    pl.semaphore_wait(barrier, 3)

    def remote(src, dst, send, recv, to):
        return pltpu.make_async_remote_copy(src_ref=src, dst_ref=dst, send_sem=send, recv_sem=recv, device_id={"tp": to}, device_id_type=MESH)

    def rows(u):
        return pl.ds(pl.multiple_of(u // PER * R, R), R)

    def block(u, owner, low, n=1):
        at = columns(owner, lax.rem(u, PER), n)
        if low is None:
            return z_ref.at[pl.ds(LOW * R, R), at]
        return (zh_ref if low else z_ref).at[rows(u), at]

    def d_copy(j):
        return remote(sbuf.at[j], rbuf.at[j], d_send.at[j], d_recv.at[j], sib)

    def d_copies(u):
        return [d_copy(j) for j in range(4)]

    def p1_copy(u):
        i = lax.rem(u, 2)
        return remote(s1.at[i], r1.at[i], p1_send.at[i], p1_recv.at[i], fnb)

    def p2_copy(u):
        i = lax.rem(u, 2)
        return remote(s2.at[i], r2.at[i], p2_send.at[i], p2_recv.at[i], gnb)

    def xr_copy(u):
        i = lax.rem(u, 2)
        return pltpu.make_async_copy(x_ref.at[rows(u), columns(o_own, lax.rem(u, PER))], xr.at[i], xr_sem.at[i])

    def a_copies(u, low=None):
        i = lax.rem(u, 2)
        return [remote(yb.at[i], block(u, o_own, low), a_send.at[i], a_recv.at[u], gnb)]

    def keep_copy(u):
        i = lax.rem(u, 2)
        return pltpu.make_async_copy(yb.at[i], block(u, o_own, True), keep_sem.at[i])

    def b_copies(u, low=None):
        at = block(u, base + fb * 2, low, 2)
        return [remote(at, at, b_send.at[lax.rem(u, 2)], b_recv.at[u], fnb)]

    def c_copies(u, low=None):
        at = block(u, base, low, 4)
        return [remote(at, at, c_send.at[lax.rem(u, 2)], c_recv.at[u], sib)]

    def sent(copies):
        for copy in copies:
            copy.wait_send()

    def start(copies, u):
        @pl.when(u < LOW * PER)
        def _():
            for copy in copies(u, True):
                copy.start()

        @pl.when(u >= LOW * PER)
        def _():
            for copy in copies(u, False):
                copy.start()

    def reduce_pair(u):
        i = lax.rem(u, 2)
        for copy in d_copies(u):
            copy.wait_recv()

        @pl.when(u >= 2)
        def _():
            p1_copy(u - 2).wait_send()

        for j in range(2):
            n = (1 - fb) * 2 + j
            s1[i, j] = (own[n] + rbuf[n].astype(F32)).astype(BF16)

        @pl.when(u >= 2)
        def _():
            pl.semaphore_wait(cred_1, 1)

        p1_copy(u).start()
        for j in range(2):
            n = fb * 2 + j
            keep1[i, j] = own[n] + rbuf[n].astype(F32)

        @pl.when(u + 1 < U)
        def _():
            pl.semaphore_signal(cred_d, inc=1, device_id={"tp": sib}, device_id_type=MESH)

    def reduce_f(u):
        i = lax.rem(u, 2)
        xr_copy(u).start()
        p1_copy(u).wait_recv()

        @pl.when(u >= 2)
        def _():
            p2_copy(u - 2).wait_send()

        s2[i] = (keep1[i, 1 - gb] + r1[i, 1 - gb].astype(F32)).astype(BF16)

        @pl.when(u >= 2)
        def _():
            pl.semaphore_wait(cred_2, 1)

        p2_copy(u).start()
        keep2[i] = keep1[i, gb] + r1[i, gb].astype(F32)

        @pl.when(u + 2 < U)
        def _():
            pl.semaphore_signal(cred_1, inc=1, device_id={"tp": fnb}, device_id_type=MESH)

    def reduce_g(u):
        i = lax.rem(u, 2)
        xr_copy(u).wait()

        @pl.when(u >= 2)
        def _():
            sent(a_copies(u - 2))

        p2_copy(u).wait_recv()
        yb[i] = (xr[i].astype(F32) + (keep2[i] + r2[i].astype(F32))).astype(BF16)
        start(a_copies, u)

        @pl.when(u < LOW * PER)
        def _():
            keep_copy(u).start()

        @pl.when(u >= LOW * PER)
        def _():
            z_ref[rows(u), columns(o_own, lax.rem(u, PER))] = yb[i]

        @pl.when(u + 2 < U)
        def _():
            pl.semaphore_signal(cred_2, inc=1, device_id={"tp": gnb}, device_id_type=MESH)

    def gather_f(u):
        @pl.when(u >= 2)
        def _():
            sent(b_copies(u - 2))

        a_copies(u)[0].wait_recv()

        @pl.when(u < LOW * PER)
        def _():
            keep_copy(u).wait()

        start(b_copies, u)

    def gather_pair(u):
        @pl.when(u >= 2)
        def _():
            sent(c_copies(u - 2))

        b_copies(u)[0].wait_recv()
        start(c_copies, u)

    def turned(t, cosf, sinf):
        t = t.astype(BF16).astype(F32)
        return (t * cosf + pltpu.roll(t, HEAD // 2, 1) * sinf).astype(BF16)

    def normalize(c):
        piece = 1024

        def norm_rows(r, _):
            rows = pl.ds(pl.multiple_of(r * 16, 16), 16)
            total = jnp.zeros((16, piece), F32)
            for n in range(D // piece):
                wide = xb[rows, n * piece : (n + 1) * piece].astype(F32)
                total = total + wide * wide
            scale = lax.rsqrt(jnp.sum(total, -1, keepdims=True) * (1 / D) + 1e-6)
            for n in range(D // piece):
                at = slice(n * piece, (n + 1) * piece)
                xb[rows, at] = (xb[rows, at].astype(F32) * scale * gain_s[:, at]).astype(BF16)
            return 0

        def quarter(i, _):
            n = R // 4
            at = pl.multiple_of(i * n, n)
            pltpu.make_async_copy(x_ref.at[pl.ds(pl.multiple_of(c * R + at, n), n), :], xb.at[pl.ds(at, n), :], x_sem.at[i]).wait()

            @pl.when((c == 0) & (i == 0))
            def _():
                load([wk_copy, wv_copy, rope_copy])
                load(wq_copies(0))

            @pl.when((c == 0) & (i == 3))
            def _():
                load(wq_copies(1))

            lax.fori_loop(i * (n // 16), (i + 1) * (n // 16), norm_rows, 0)
            return 0

        lax.fori_loop(0, 4, quarter, 0)

    def turns(c):
        cs = rope_s[pl.ds(pl.multiple_of(c * R, R), R), :]
        sc = pltpu.roll(cs, HEAD // 2, 1)
        low = lax.broadcasted_iota(jnp.int32, (R, HEAD), 1) < HEAD // 2
        return jnp.where(low, cs, sc), jnp.where(low, -sc, cs)

    def keys_values(c):
        @pl.when(c == 0)
        def _():
            rope_copy.wait()
            wk_copy.wait()
            wv_copy.wait()
            for n in (2, 3):
                load(wq_copies(n))


        here = pl.ds(pl.multiple_of(c * R, R), R)
        kv = _dot(xb[...], wkv_s[...], 1, 0)
        k_s[here, :] = turned(kv[:, :HEAD], *turns(c))
        vt_s[:HEAD, here] = kv[:, HEAD:].T.astype(BF16)

    def queries(c, first, last):
        def tile(n, _):
            @pl.when(c == 0)
            def _():
                for copy in wq_copies(n):
                    copy.wait()

            @pl.when((c == 0) & (n == 1))
            def _():
                for i in range(NO):
                    wo_copy(i).start()

            q = 0
            for k in range(D // 1024):
                q += _dot(xb[:, k * 1024 : (k + 1) * 1024], z_ref[pl.ds(0, LOW * R), heads_at(n, k)], 1, 0)
            cosf, sinf = turns(c)
            for h in range(2):
                q_s[pl.ds(pl.multiple_of((2 * n + h) * R, R), R), :] = turned(q[:, h * HEAD : (h + 1) * HEAD], cosf, sinf)
            return 0

        lax.fori_loop(first, last, tile, 0)

        @pl.when((last == 4) & (c + 1 < CHUNKS))
        def _():
            for copy in x_copies(c + 1):
                copy.start()

    def attention(c, part):
        e = HEAD**-0.5 * LOG2E
        pieces = range(0, COLS, STRIP)

        def keys(j, masked):
            here = pl.ds(pl.multiple_of(j * R, R), R)
            scores = [_dot(k_s[here, :], q_s[at : at + STRIP, :], 1, 1) for at in pieces]
            if masked:
                ok = lax.rem(lax.broadcasted_iota(jnp.int32, (R, STRIP), 1), R) >= lax.broadcasted_iota(jnp.int32, (R, STRIP), 0)
            weights, keeps = [], []
            for at, s in zip(pieces, scores):
                if masked:
                    s = jnp.where(ok, s, HIDDEN)
                old = top_s[0:1, at : at + STRIP]
                top = jnp.maximum(old, s.max(axis=0, keepdims=True))
                top_s[0:1, at : at + STRIP] = top
                weights.append(jnp.exp2((s - top) * e).astype(BF16))
                keeps.append(jnp.exp2((old - top) * e))
            for at, p, keep in zip(pieces, weights, keeps):
                mix_s[:, at : at + STRIP] = mix_s[:, at : at + STRIP] * keep + _dot(vt_s[:, here], p, 1, 0)

        def whole(j, _):
            keys(j, False)
            return 0

        @pl.when(part == 0)
        def _():
            top_s[...] = jnp.full((8, COLS), NEG, F32)
            mix_s[...] = jnp.zeros((VROWS, COLS), F32)

        lax.fori_loop(jnp.where(part == 0, 0, c // 2), jnp.where(part == 0, c // 2, c), whole, 0)

        @pl.when(part == 1)
        def _():
            keys(c, True)
            for h in range(HEADS):
                at = slice(h * R, (h + 1) * R)
                seen_s[:, h * HEAD : (h + 1) * HEAD] = (mix_s[:HEAD, at] * (1 / mix_s[HEAD : HEAD + 1, at])).T.astype(BF16)

    def tile(u, n):
        m = 8 * u + n
        wo_copy(m).wait()
        term = _dot(seen_s[...], wo_s[lax.rem(m, NO)], 1, 0)

        @pl.when(m + NO < 8 * U)
        def _():
            wo_copy(m + NO).start()

        return term

    def output_theirs(u):
        @pl.when(u >= 1)
        def _():
            sent(d_copies(u - 1))
            pl.semaphore_wait(cred_d, 1)

        def theirs(j, _):
            sbuf[j] = tile(u, j).astype(BF16)
            d_copy(j).start()
            return 0

        lax.fori_loop(0, 4, theirs, 0)

    def output_ours(u):
        def ours(j, _):
            own[j] = tile(u, 4 + j)
            return 0

        lax.fori_loop(0, 4, ours, 0)

    def arrivals(u, _):
        c_copies(u)[0].wait_recv()
        return 0

    def slot(g, _):
        for stage in (reduce_pair, reduce_f, reduce_g, gather_f, gather_pair):
            first, second = (g + 99 * SLOTS - at for at in WHEN[stage.__name__])
            is_first = lax.rem(first, SLOTS) == 0
            n = jnp.where(is_first, first, second) // SLOTS - 100

            @pl.when((is_first | (lax.rem(second, SLOTS) == 0)) & (n >= 0) & (n < CHUNKS))
            def _(stage=stage, n=n, is_first=is_first):
                stage(2 * n + jnp.where(is_first, 0, 1))

        c = g // SLOTS - 1
        k = lax.rem(g, SLOTS)
        live = (c >= 0) & (c < CHUNKS)

        @pl.when(live & (k < 2))
        def _():
            attention(c, k)

        @pl.when(live & ((k == 2) | (k == 4)))
        def _():
            output_theirs(2 * c + k // 4)

        @pl.when(live & ((k == 3) | (k == 5)))
        def _():
            output_ours(2 * c + k // 4)

        @pl.when((c == CHUNKS - 1) & (k == 6))
        def _():
            lax.fori_loop(0, LOW * PER, arrivals, 0)
            for copy in fetch_copies():
                copy.start()

        more = c + 1 < CHUNKS

        @pl.when(more & (k == 7))
        def _():
            normalize(c + 1)

        @pl.when(more & (k == 8))
        def _():
            keys_values(c + 1)

        @pl.when(more & (k >= 8))
        def _():
            queries(c + 1, 2 * k - 16, 2 * k - 14)

        return 0

    lax.fori_loop(7, SLOTS * CHUNKS + max(map(max, WHEN.values())) + 1, slot, 0)

    sent(d_copies(U - 1))
    for u in (U - 2, U - 1):
        p1_copy(u).wait_send()
        p2_copy(u).wait_send()
        sent(a_copies(u))
        sent(b_copies(u))
        sent(c_copies(u))

    lax.fori_loop(LOW * PER, U, arrivals, 0)
    for copy in fetch_copies():
        copy.wait()


def _place(z_ref, y_ref, sem):
    n = ROWS // 8
    copies = [pltpu.make_async_copy(z_ref.at[pl.ds(i * n, n), :], y_ref.at[pl.ds(i * n, n), :], sem.at[i]) for i in range(8)]
    for copy in copies:
        copy.start()
    for copy in copies:
        copy.wait()


def _tables():
    half = HEAD // 2
    angle = np.arange(ROWS, dtype=np.float64)[:, None] * np.float64(THETA) ** (-np.arange(half, dtype=np.float64) / half)
    return np.concatenate([np.cos(angle), np.sin(angle)], 1).astype(np.float32)


def solution(mesh):
    def step(x, gain, wq, wk, wv, wo):
        any_ = pl.BlockSpec(memory_space=pl.ANY)
        dma = pltpu.SemaphoreType.DMA
        _, z = pl.pallas_call(
            _kernel,
            name="layer",
            out_shape=[jax.ShapeDtypeStruct((LOW * R, D), BF16), pltpu.VMEM((ROWS, D), BF16)],
            in_specs=[any_, pl.BlockSpec(memory_space=pltpu.VMEM)] + [any_] * 5,
            out_specs=[any_, pl.BlockSpec(memory_space=pltpu.VMEM)],
            scratch_shapes=[
                pltpu.VMEM((1, D), F32),
                pltpu.VMEM((D, 2 * HEAD), BF16), pltpu.VMEM((NO, 1024, W), BF16),
                pltpu.VMEM((R, D), BF16), pltpu.VMEM((ROWS, HEAD), F32),
                pltpu.VMEM((ROWS, HEAD), BF16), pltpu.VMEM((VROWS, ROWS), BF16), pltpu.VMEM((COLS, HEAD), BF16),
                pltpu.VMEM((R, 1024), BF16), pltpu.VMEM((VROWS, COLS), F32), pltpu.VMEM((8, COLS), F32),
                pltpu.VMEM((4, R, W), BF16), pltpu.VMEM((4, R, W), F32), pltpu.VMEM((4, R, W), BF16),
                pltpu.VMEM((2, 2, R, W), BF16), pltpu.VMEM((2, 2, R, W), BF16), pltpu.VMEM((2, 2, R, W), F32),
                pltpu.VMEM((2, R, W), BF16), pltpu.VMEM((2, R, W), BF16), pltpu.VMEM((2, R, W), F32),
                pltpu.VMEM((2, R, W), BF16), pltpu.VMEM((2, R, W), BF16),
                dma((3,)), dma((4, D // 1024)), dma((8,)), dma((NO,)), dma((4,)), dma((2,)), dma((4,)), dma((4,)), dma((2,)), dma((2,)), dma((2,)), dma((2,)),
                dma((2,)), dma((2,)), dma((2,)), dma((2,)), dma((U,)), dma((U,)), dma((U,)),
                pltpu.SemaphoreType.REGULAR, pltpu.SemaphoreType.REGULAR, pltpu.SemaphoreType.REGULAR,
            ],
            compiler_params=pltpu.CompilerParams(collective_id=0, has_side_effects=True, vmem_limit_bytes=67043328 - ROWS * D * 2),
            cost_estimate=pl.CostEstimate(flops=95_000_000_000, bytes_accessed=200_000_000, transcendentals=20_000_000),
        )(x, gain.reshape(D // 128, 128), wq, wk, wv, wo, jnp.asarray(_tables()))
        return pl.pallas_call(
            _place,
            name="place",
            out_shape=jax.ShapeDtypeStruct((ROWS, D), BF16),
            in_specs=[pl.BlockSpec(memory_space=pltpu.VMEM)],
            out_specs=any_,
            scratch_shapes=[dma((8,))],
            compiler_params=pltpu.CompilerParams(vmem_limit_bytes=2**20),
            cost_estimate=pl.CostEstimate(flops=0, bytes_accessed=42_000_000, transcendentals=0),
        )(z)

    tokens, columns = P("dp", None), P(None, "tp")
    return jax.shard_map(
        step,
        mesh=mesh,
        in_specs=(tokens, P(None), columns, columns, columns, P("tp", None)),
        out_specs=tokens,
        check_vma=False,
    )
```

```python
import functools

import jax
import jax.numpy as jnp
import numpy as np
from jax import lax
from jax.experimental import pallas as pl
from jax.experimental.pallas import tpu as pltpu
from jax.sharding import PartitionSpec as P

MESH = pl.DeviceIdType.MESH
NEG = -1e30
HIDDEN = 2 * NEG
LOG2E = 1.4426950408889634
HEAD = 128
THETA = 10000
ROWS, D = 2048, 8192
R = 256
W = 512
CHUNKS = ROWS // R
PER = 1024 // W
LOW = 4
NO = 6
U = CHUNKS * PER
HEADS = 8
COLS = HEADS * R
STRIP = 512
VROWS = 144
F32, BF16 = jnp.float32, jnp.bfloat16
SLOTS = 10
WHEN = {"reduce_pair": (4, 7), "reduce_f": (9, 10), "reduce_g": (10, 11), "gather_f": (19, 20), "gather_pair": (21, 25)}


def _dot(a, b, ca, cb):
    return lax.dot_general(a, b, (((ca,), (cb,)), ((), ())), preferred_element_type=F32)


def _kernel(x_ref, gain_ref, wq_ref, wk_ref, wv_ref, wo_ref, rope_ref, zh_ref, z_ref,
            gain_s, wkv_s, wo_s, xb, rope_s, k_s, vt_s, q_s, seen_s, mix_s, top_s,
            sbuf, own, rbuf, s1, r1, keep1, s2, r2, keep2, yb, xr,
            w_sem, wq_sem, fetch_sem, wo_sem, x_sem, xr_sem, d_send, d_recv, p1_send, p1_recv, p2_send, p2_recv,
            a_send, b_send, c_send, a1_recv, a2_recv, b1_recv, sib_recv, cred_d, cred_1, cred_2):
    me = lax.axis_index("tp")
    a = lax.rem(me, 2)
    yc = lax.rem(me // 2, 2)
    xc = me // 4
    sib = me + 1 - 2 * a
    xn, yn = me + 4 - 8 * xc, me + 2 - 4 * yc
    fnb, gnb = xn * (1 - a) + yn * a, yn * (1 - a) + xn * a
    fb, gb = xc * (1 - a) + yc * a, yc * (1 - a) + xc * a
    base = a * 4
    o_own, o_g = base + fb * 2 + gb, base + fb * 2 + 1 - gb
    o_f, o_fg = base + (1 - fb) * 2 + gb, base + (1 - fb) * 2 + 1 - gb

    def x_copies(c):
        n = R // 4
        return [pltpu.make_async_copy(x_ref.at[pl.ds(pl.multiple_of(c * R + i * n, n), n), :], xb.at[pl.ds(i * n, n), :], x_sem.at[i]) for i in range(4)]

    def heads_at(n, k):
        return pl.ds(pl.multiple_of(k * 1024 + n * 256, 256), 256)

    def wq_copies(n):
        low = pl.ds(0, LOW * R)
        return [pltpu.make_async_copy(wq_ref.at[pl.ds(k * 1024, 1024), heads_at(n, 0)], z_ref.at[low, heads_at(n, k)], wq_sem.at[n, k]) for k in range(D // 1024)]

    def load(copies):
        for copy in copies:
            copy.start()

    def fetch_copies():
        n = LOW * R // 8
        return [pltpu.make_async_copy(zh_ref.at[pl.ds(i * n, n), :], z_ref.at[pl.ds(i * n, n), :], fetch_sem.at[i]) for i in range(8)]

    wk_copy = pltpu.make_async_copy(wk_ref, wkv_s.at[:, pl.ds(0, HEAD)], w_sem.at[0])
    wv_copy = pltpu.make_async_copy(wv_ref, wkv_s.at[:, pl.ds(HEAD, HEAD)], w_sem.at[1])
    rope_copy = pltpu.make_async_copy(rope_ref, rope_s, w_sem.at[2])

    def columns(owner, s):
        return pl.ds(pl.multiple_of(owner * 1024 + s * W, W), W)

    def wo_copy(m):
        i = lax.rem(m, NO)
        n = lax.rem(m, 8)
        at = columns(jnp.where(n < 4, (1 - a) * 4 + n, a * 4 + n - 4), lax.rem(m // 8, PER))
        return pltpu.make_async_copy(wo_ref.at[:, at], wo_s.at[i], wo_sem.at[i])

    for copy in x_copies(0):
        copy.start()
    barrier = pltpu.get_barrier_semaphore()
    for other in (sib, fnb, gnb):
        pl.semaphore_signal(barrier, inc=1, device_id={"tp": other}, device_id_type=MESH)
    gain = gain_ref[...].astype(F32)
    for n in range(D // 128):
        gain_s[:, n * 128 : (n + 1) * 128] = gain[n : n + 1, :]
    vt_s[HEAD:, :] = jnp.ones((VROWS - HEAD, ROWS), BF16)
    pl.semaphore_wait(barrier, 3)

    def remote(src, dst, send, recv, to):
        return pltpu.make_async_remote_copy(src_ref=src, dst_ref=dst, send_sem=send, recv_sem=recv, device_id={"tp": to}, device_id_type=MESH)

    def rows(u):
        return pl.ds(pl.multiple_of(u // PER * R, R), R)

    def block(u, owner, low):
        at = columns(owner, lax.rem(u, PER))
        if low is None:
            return z_ref.at[pl.ds(LOW * R, R), at]
        return (zh_ref if low else z_ref).at[rows(u), at]

    def d_copy(j):
        return remote(sbuf.at[j], rbuf.at[j], d_send.at[j], d_recv.at[j], sib)

    def d_copies(u):
        return [d_copy(j) for j in range(4)]

    def p1_copy(u):
        i = lax.rem(u, 2)
        return remote(s1.at[i], r1.at[i], p1_send.at[i], p1_recv.at[i], fnb)

    def p2_copy(u):
        i = lax.rem(u, 2)
        return remote(s2.at[i], r2.at[i], p2_send.at[i], p2_recv.at[i], gnb)

    def xr_copy(u):
        i = lax.rem(u, 2)
        return pltpu.make_async_copy(x_ref.at[rows(u), columns(o_own, lax.rem(u, PER))], xr.at[i], xr_sem.at[i])

    def a_copies(u, low=None):
        i = lax.rem(u, 2)
        at = block(u, o_own, low)
        return (remote(yb.at[i], at, a_send.at[0, i], a1_recv.at[u], gnb),
                remote(yb.at[i], at, a_send.at[1, i], a2_recv.at[u], fnb),
                remote(yb.at[i], at, a_send.at[2, i], sib_recv.at[0, u], sib))

    def keep_copy(u):
        i = lax.rem(u, 2)
        return pltpu.make_async_copy(yb.at[i], block(u, o_own, True), a_send.at[3, i])

    def b_copies(u, low=None):
        i = lax.rem(u, 2)
        at = block(u, o_g, low)
        return (remote(at, at, b_send.at[0, i], b1_recv.at[u], fnb),
                remote(at, at, b_send.at[1, i], sib_recv.at[1, u], sib))

    def c_copies(u, low=None):
        i = lax.rem(u, 2)
        at, far = block(u, o_f, low), block(u, o_fg, low)
        return (remote(at, at, c_send.at[0, i], sib_recv.at[2, u], sib),
                remote(far, far, c_send.at[1, i], sib_recv.at[3, u], sib))

    def sent(copies):
        for copy in copies:
            copy.wait_send()

    def start(copies, u):
        @pl.when(u < LOW * PER)
        def _():
            for copy in copies(u, True):
                copy.start()

        @pl.when(u >= LOW * PER)
        def _():
            for copy in copies(u, False):
                copy.start()

    def reduce_pair(u):
        i = lax.rem(u, 2)
        for copy in d_copies(u):
            copy.wait_recv()

        @pl.when(u >= 2)
        def _():
            p1_copy(u - 2).wait_send()

        for j in range(2):
            n = (1 - fb) * 2 + j
            s1[i, j] = (own[n] + rbuf[n].astype(F32)).astype(BF16)

        @pl.when(u >= 2)
        def _():
            pl.semaphore_wait(cred_1, 1)

        p1_copy(u).start()
        for j in range(2):
            n = fb * 2 + j
            keep1[i, j] = own[n] + rbuf[n].astype(F32)

        @pl.when(u + 1 < U)
        def _():
            pl.semaphore_signal(cred_d, inc=1, device_id={"tp": sib}, device_id_type=MESH)

    def reduce_f(u):
        i = lax.rem(u, 2)
        xr_copy(u).start()
        p1_copy(u).wait_recv()

        @pl.when(u >= 2)
        def _():
            p2_copy(u - 2).wait_send()

        s2[i] = (keep1[i, 1 - gb] + r1[i, 1 - gb].astype(F32)).astype(BF16)

        @pl.when(u >= 2)
        def _():
            pl.semaphore_wait(cred_2, 1)

        p2_copy(u).start()
        keep2[i] = keep1[i, gb] + r1[i, gb].astype(F32)

        @pl.when(u + 2 < U)
        def _():
            pl.semaphore_signal(cred_1, inc=1, device_id={"tp": fnb}, device_id_type=MESH)

    def reduce_g(u):
        i = lax.rem(u, 2)
        xr_copy(u).wait()

        @pl.when(u >= 2)
        def _():
            sent(a_copies(u - 2))

        @pl.when((u >= 2) & (u < LOW * PER + 2))
        def _():
            keep_copy(jnp.minimum(u - 2, LOW * PER - 1)).wait()

        p2_copy(u).wait_recv()
        yb[i] = (xr[i].astype(F32) + (keep2[i] + r2[i].astype(F32))).astype(BF16)
        start(a_copies, u)

        @pl.when(u < LOW * PER)
        def _():
            keep_copy(u).start()

        @pl.when(u >= LOW * PER)
        def _():
            z_ref[rows(u), columns(o_own, lax.rem(u, PER))] = yb[i]

        @pl.when(u + 2 < U)
        def _():
            pl.semaphore_signal(cred_2, inc=1, device_id={"tp": gnb}, device_id_type=MESH)

    def gather_f(u):
        @pl.when(u >= 2)
        def _():
            sent(b_copies(u - 2))

        a_copies(u)[0].wait_recv()
        start(b_copies, u)

    def gather_pair(u):
        @pl.when(u >= 2)
        def _():
            sent(c_copies(u - 2))

        a_copies(u)[1].wait_recv()
        b_copies(u)[0].wait_recv()
        start(c_copies, u)

    def turned(t, cosf, sinf):
        t = t.astype(BF16).astype(F32)
        return (t * cosf + pltpu.roll(t, HEAD // 2, 1) * sinf).astype(BF16)

    def normalize(c):
        piece = 1024

        def norm_rows(r, _):
            rows = pl.ds(pl.multiple_of(r * 16, 16), 16)
            total = jnp.zeros((16, piece), F32)
            for n in range(D // piece):
                wide = xb[rows, n * piece : (n + 1) * piece].astype(F32)
                total = total + wide * wide
            scale = lax.rsqrt(jnp.sum(total, -1, keepdims=True) * (1 / D) + 1e-6)
            for n in range(D // piece):
                at = slice(n * piece, (n + 1) * piece)
                xb[rows, at] = (xb[rows, at].astype(F32) * scale * gain_s[:, at]).astype(BF16)
            return 0

        def quarter(i, _):
            n = R // 4
            at = pl.multiple_of(i * n, n)
            pltpu.make_async_copy(x_ref.at[pl.ds(pl.multiple_of(c * R + at, n), n), :], xb.at[pl.ds(at, n), :], x_sem.at[i]).wait()

            @pl.when((c == 0) & (i == 0))
            def _():
                load([wk_copy, wv_copy, rope_copy])
                load(wq_copies(0))

            @pl.when((c == 0) & (i == 3))
            def _():
                load(wq_copies(1))

            lax.fori_loop(i * (n // 16), (i + 1) * (n // 16), norm_rows, 0)
            return 0

        lax.fori_loop(0, 4, quarter, 0)

    def turns(c):
        cs = rope_s[pl.ds(pl.multiple_of(c * R, R), R), :]
        sc = pltpu.roll(cs, HEAD // 2, 1)
        low = lax.broadcasted_iota(jnp.int32, (R, HEAD), 1) < HEAD // 2
        return jnp.where(low, cs, sc), jnp.where(low, -sc, cs)

    def keys_values(c):
        @pl.when(c == 0)
        def _():
            rope_copy.wait()
            wk_copy.wait()
            wv_copy.wait()
            for n in (2, 3):
                load(wq_copies(n))


        here = pl.ds(pl.multiple_of(c * R, R), R)
        kv = _dot(xb[...], wkv_s[...], 1, 0)
        k_s[here, :] = turned(kv[:, :HEAD], *turns(c))
        vt_s[:HEAD, here] = kv[:, HEAD:].T.astype(BF16)

    def queries(c, first, last):
        def tile(n, _):
            @pl.when(c == 0)
            def _():
                for copy in wq_copies(n):
                    copy.wait()

            @pl.when((c == 0) & (n == 1))
            def _():
                for i in range(NO):
                    wo_copy(i).start()

            q = 0
            for k in range(D // 1024):
                q += _dot(xb[:, k * 1024 : (k + 1) * 1024], z_ref[pl.ds(0, LOW * R), heads_at(n, k)], 1, 0)
            cosf, sinf = turns(c)
            for h in range(2):
                q_s[pl.ds(pl.multiple_of((2 * n + h) * R, R), R), :] = turned(q[:, h * HEAD : (h + 1) * HEAD], cosf, sinf)
            return 0

        lax.fori_loop(first, last, tile, 0)

        @pl.when((last == 4) & (c + 1 < CHUNKS))
        def _():
            for copy in x_copies(c + 1):
                copy.start()

    def attention(c, part):
        e = HEAD**-0.5 * LOG2E
        pieces = range(0, COLS, STRIP)

        def keys(j, masked):
            here = pl.ds(pl.multiple_of(j * R, R), R)
            scores = [_dot(k_s[here, :], q_s[at : at + STRIP, :], 1, 1) for at in pieces]
            if masked:
                ok = lax.rem(lax.broadcasted_iota(jnp.int32, (R, STRIP), 1), R) >= lax.broadcasted_iota(jnp.int32, (R, STRIP), 0)
            weights, keeps = [], []
            for at, s in zip(pieces, scores):
                if masked:
                    s = jnp.where(ok, s, HIDDEN)
                old = top_s[0:1, at : at + STRIP]
                top = jnp.maximum(old, s.max(axis=0, keepdims=True))
                top_s[0:1, at : at + STRIP] = top
                weights.append(jnp.exp2((s - top) * e).astype(BF16))
                keeps.append(jnp.exp2((old - top) * e))
            for at, p, keep in zip(pieces, weights, keeps):
                mix_s[:, at : at + STRIP] = mix_s[:, at : at + STRIP] * keep + _dot(vt_s[:, here], p, 1, 0)

        def whole(j, _):
            keys(j, False)
            return 0

        @pl.when(part == 0)
        def _():
            top_s[...] = jnp.full((8, COLS), NEG, F32)
            mix_s[...] = jnp.zeros((VROWS, COLS), F32)

        lax.fori_loop(jnp.where(part == 0, 0, c // 2), jnp.where(part == 0, c // 2, c), whole, 0)

        @pl.when(part == 1)
        def _():
            keys(c, True)
            for h in range(HEADS):
                at = slice(h * R, (h + 1) * R)
                seen_s[:, h * HEAD : (h + 1) * HEAD] = (mix_s[:HEAD, at] * (1 / mix_s[HEAD : HEAD + 1, at])).T.astype(BF16)

    def tile(u, n):
        m = 8 * u + n
        wo_copy(m).wait()
        term = _dot(seen_s[...], wo_s[lax.rem(m, NO)], 1, 0)

        @pl.when(m + NO < 8 * U)
        def _():
            wo_copy(m + NO).start()

        return term

    def output_theirs(u):
        @pl.when(u >= 1)
        def _():
            sent(d_copies(u - 1))
            pl.semaphore_wait(cred_d, 1)

        def theirs(j, _):
            sbuf[j] = tile(u, j).astype(BF16)
            d_copy(j).start()
            return 0

        lax.fori_loop(0, 4, theirs, 0)

    def output_ours(u):
        def ours(j, _):
            own[j] = tile(u, 4 + j)
            return 0

        lax.fori_loop(0, 4, ours, 0)

    def arrivals(u, _):
        a_copies(u)[2].wait_recv()
        b_copies(u)[1].wait_recv()
        for copy in c_copies(u):
            copy.wait_recv()
        return 0

    def slot(g, _):
        for stage in (reduce_pair, reduce_f, reduce_g, gather_f, gather_pair):
            first, second = (g + 99 * SLOTS - at for at in WHEN[stage.__name__])
            is_first = lax.rem(first, SLOTS) == 0
            n = jnp.where(is_first, first, second) // SLOTS - 100

            @pl.when((is_first | (lax.rem(second, SLOTS) == 0)) & (n >= 0) & (n < CHUNKS))
            def _(stage=stage, n=n, is_first=is_first):
                stage(2 * n + jnp.where(is_first, 0, 1))

        c = g // SLOTS - 1
        k = lax.rem(g, SLOTS)
        live = (c >= 0) & (c < CHUNKS)

        @pl.when(live & (k < 2))
        def _():
            attention(c, k)

        @pl.when(live & ((k == 2) | (k == 4)))
        def _():
            output_theirs(2 * c + k // 4)

        @pl.when(live & ((k == 3) | (k == 5)))
        def _():
            output_ours(2 * c + k // 4)

        @pl.when((c == CHUNKS - 1) & (k == 6))
        def _():
            lax.fori_loop(0, LOW * PER, arrivals, 0)
            for copy in fetch_copies():
                copy.start()

        more = c + 1 < CHUNKS

        @pl.when(more & (k == 7))
        def _():
            normalize(c + 1)

        @pl.when(more & (k == 8))
        def _():
            keys_values(c + 1)

        @pl.when(more & (k >= 8))
        def _():
            queries(c + 1, 2 * k - 16, 2 * k - 14)

        return 0

    lax.fori_loop(7, SLOTS * CHUNKS + max(map(max, WHEN.values())) + 1, slot, 0)

    sent(d_copies(U - 1))
    for u in (U - 2, U - 1):
        p1_copy(u).wait_send()
        p2_copy(u).wait_send()
        sent(a_copies(u))
        sent(b_copies(u))
        sent(c_copies(u))

    lax.fori_loop(LOW * PER, U, arrivals, 0)
    for copy in fetch_copies():
        copy.wait()


def _place(z_ref, y_ref, sem):
    n = ROWS // 8
    copies = [pltpu.make_async_copy(z_ref.at[pl.ds(i * n, n), :], y_ref.at[pl.ds(i * n, n), :], sem.at[i]) for i in range(8)]
    for copy in copies:
        copy.start()
    for copy in copies:
        copy.wait()


def _tables():
    half = HEAD // 2
    angle = np.arange(ROWS, dtype=np.float64)[:, None] * np.float64(THETA) ** (-np.arange(half, dtype=np.float64) / half)
    return np.concatenate([np.cos(angle), np.sin(angle)], 1).astype(np.float32)


def solution(mesh):
    def step(x, gain, wq, wk, wv, wo):
        any_ = pl.BlockSpec(memory_space=pl.ANY)
        dma = pltpu.SemaphoreType.DMA
        _, z = pl.pallas_call(
            _kernel,
            name="layer",
            out_shape=[jax.ShapeDtypeStruct((LOW * R, D), BF16), pltpu.VMEM((ROWS, D), BF16)],
            in_specs=[any_, pl.BlockSpec(memory_space=pltpu.VMEM)] + [any_] * 5,
            out_specs=[any_, pl.BlockSpec(memory_space=pltpu.VMEM)],
            scratch_shapes=[
                pltpu.VMEM((1, D), F32),
                pltpu.VMEM((D, 2 * HEAD), BF16), pltpu.VMEM((NO, 1024, W), BF16),
                pltpu.VMEM((R, D), BF16), pltpu.VMEM((ROWS, HEAD), F32),
                pltpu.VMEM((ROWS, HEAD), BF16), pltpu.VMEM((VROWS, ROWS), BF16), pltpu.VMEM((COLS, HEAD), BF16),
                pltpu.VMEM((R, 1024), BF16), pltpu.VMEM((VROWS, COLS), F32), pltpu.VMEM((8, COLS), F32),
                pltpu.VMEM((4, R, W), BF16), pltpu.VMEM((4, R, W), F32), pltpu.VMEM((4, R, W), BF16),
                pltpu.VMEM((2, 2, R, W), BF16), pltpu.VMEM((2, 2, R, W), BF16), pltpu.VMEM((2, 2, R, W), F32),
                pltpu.VMEM((2, R, W), BF16), pltpu.VMEM((2, R, W), BF16), pltpu.VMEM((2, R, W), F32),
                pltpu.VMEM((2, R, W), BF16), pltpu.VMEM((2, R, W), BF16),
                dma((3,)), dma((4, D // 1024)), dma((8,)), dma((NO,)), dma((4,)), dma((2,)), dma((4,)), dma((4,)), dma((2,)), dma((2,)), dma((2,)), dma((2,)),
                dma((4, 2)), dma((2, 2)), dma((2, 2)), dma((U,)), dma((U,)), dma((U,)), dma((4, U)),
                pltpu.SemaphoreType.REGULAR, pltpu.SemaphoreType.REGULAR, pltpu.SemaphoreType.REGULAR,
            ],
            compiler_params=pltpu.CompilerParams(collective_id=0, has_side_effects=True, vmem_limit_bytes=67043328 - ROWS * D * 2),
            cost_estimate=pl.CostEstimate(flops=95_000_000_000, bytes_accessed=200_000_000, transcendentals=20_000_000),
        )(x, gain.reshape(D // 128, 128), wq, wk, wv, wo, jnp.asarray(_tables()))
        return pl.pallas_call(
            _place,
            name="place",
            out_shape=jax.ShapeDtypeStruct((ROWS, D), BF16),
            in_specs=[pl.BlockSpec(memory_space=pltpu.VMEM)],
            out_specs=any_,
            scratch_shapes=[dma((8,))],
            compiler_params=pltpu.CompilerParams(vmem_limit_bytes=2**20),
            cost_estimate=pl.CostEstimate(flops=0, bytes_accessed=42_000_000, transcendentals=0),
        )(z)

    tokens, columns = P("dp", None), P(None, "tp")
    return jax.shard_map(
        step,
        mesh=mesh,
        in_specs=(tokens, P(None), columns, columns, columns, P("tp", None)),
        out_specs=tokens,
        check_vma=False,
    )
```
